128 devices in a mesh: dp: 8 (over z, core), mp: 16 (over y, x).
Axes of the slice: x: 4, y: 4, z: 4, core: 2. Of those that a mesh axis runs over, the one named last changes fastest.
Arguments:
- patches: bfloat16 [16384, 1280], P(('dp', 'mp')), may hold values from -6 to 6
- window_ids: int32 [128, 128], P(('dp', 'mp')), may hold values from 0 to 7, never falling along the last dimension, each value on 1 to 64 neighbouring positions
- owner: int32 [4096, 1], P(('dp', 'mp')), may hold values from 0 to 7; in each aligned block of 32 rows (0 to 31, 32 to 63, ...) at most 8 rows name the same one
- slot_of_row: int32 [128, 64], P(('dp', 'mp')), may hold values from 0 to 63, each once within a row
- text_embeds: bfloat16 [8192, 8192], P(('dp', 'mp')), may hold values from -6 to 6
- vit_norm: float32 [1280], replicated, may hold values from 0.3 to 3
- vit_qkv_w: bfloat16 [1280, 1920], replicated, may hold values from -0.15625 to 0.15625
- vit_qkv_b: float32 [1920], replicated, may hold values from -12 to 12
- vit_out_w: bfloat16 [640, 1280], replicated, may hold values from -0.25 to 0.25
- merge_norm: float32 [1280], replicated, may hold values from 0.3 to 3
- merge_w1: bfloat16 [5120, 5120], P(None, 'mp'), may hold values from -0.078125 to 0.078125
- merge_b1: float32 [5120], P('mp'), may hold values from -3 to 3
- merge_w2: bfloat16 [5120, 8192], P('mp'), may hold values from -0.078125 to 0.078125
- merge_b2: float32 [8192], replicated, may hold values from -3 to 3
- llm_norm: float32 [8192], replicated, may hold values from 0.5 to 1.5
- q_w: bfloat16 [8192, 4096], P(None, 'mp'), may hold values from -0.0625 to 0.0625
- q_b: float32 [4096], P('mp'), may hold values from -12 to 12
- kv_w: bfloat16 [2, 8192, 512], P(None, None, 'mp'), may hold values from -0.0625 to 0.0625
- kv_b: float32 [2, 512], P(None, 'mp'), may hold values from -12 to 12
Outputs:
- attended: bfloat16 [8192, 4096], P('dp', 'mp')
The draws below stay inside these ranges and needn't reach their ends.
Inputs may be any that keep to these rules, and one draw needn't show every extreme that they name: `window_ids`: within each block, window numbers never fall and each window has at most 64 patches. Among the 32 merged rows of one device, no owner is named by more than 8 rows, a bound that some block reaches. `slot_of_row`: each row is a permutation of the 64 slots.
All inputs are finite; a program needn't handle non-finite values.
Results may differ from the reference program's by a relative error of at most 0.04.
Values may be sent and summed in bfloat16 or wider, within the bound.
A program may use at most 128 MiB of HBM per device.

```python
import math
import jax
import jax.numpy as jnp
import numpy as np
from jax import lax

VW = 1280
VHD = 80
VH = 8
D = 8192
HD = 128
QH = 32
KVH = 4
BLOCK = 128
ROWS_DEV = 64
MW = 5120
MR = 32
CAP = 8
SEQ = 1024
PATCHES = 16384
MERGED = 4096
TOTAL_ROWS = 8192
N_DP = 8
N_MP = 16
DEVICES = 128


def drawn_bias(key, bias_shape):
    return jnp.clip(0.5 * jax.random.normal(key, bias_shape, jnp.float32), -3.0, 3.0)


def draw_vit_qkv_b(key, part):
    noise_part = drawn_bias(jax.random.fold_in(key, 7201), (3, VH, VHD))
    return noise_part.reshape(3 * VH * VHD)


def draw_q_b(key, part):
    noise_part = drawn_bias(jax.random.fold_in(key, 7501), (QH, HD))
    return noise_part.reshape(QH * HD)


def draw_kv_b(key, part):
    noise_part = drawn_bias(jax.random.fold_in(key, 7601), (2, KVH, HD))
    return jnp.swapaxes(noise_part, 1, 2).reshape(2, KVH * HD)


def levels(key, shape, shards, least, high):
    factor_of, own = 1.0, jax.random.fold_in(key, 6)
    for axis_at, shards_of in shards:
        draws = jnp.exp(jax.random.uniform(jax.random.fold_in(own, axis_at), (shards_of,), jnp.float32, least / len(shards), high / len(shards)))
        factor_of = factor_of * jnp.repeat(draws, shape[axis_at] // shards_of).reshape([-1 if axis == axis_at else 1 for axis in range(len(shape))])
    return factor_of


def length_profile(number_of, total, limit, skew):
    loads = [(1 << 20) // math.isqrt(standing ** skew) + 1 for standing in range(2, number_of + 1)]
    spare, counts = total - limit - (number_of - 1), [1] * (number_of - 1)
    while spare > 0:
        movable = [i for i in range(number_of - 1) if counts[i] < limit]
        pool, budget = sum([loads[i] for i in movable]), spare
        for i in movable:
            extra = min(limit - counts[i], max(1, budget * loads[i] // pool), spare)
            counts[i] = counts[i] + extra
            spare = spare - extra
    return np.array([limit] + counts)


def uneven_parts(own_key, count, total, reach, skew):
    if count == 2:
        one = jax.random.randint(own_key, (), max(1, total - reach), min(reach, total - 1) + 1)
        return jnp.stack([one, total - one])
    tallies = jnp.asarray(length_profile(count, total, reach, skew), jnp.int32)
    couples = (count - 1) // 2
    donor, taker = tallies[1:1 + 2 * couples:2], tallies[2:2 + 2 * couples:2]
    room = jnp.minimum(donor - 1, reach - taker)
    passed = jax.random.randint(jax.random.fold_in(own_key, 1), (couples,), 0, 1 << 20) % (room + 1)
    tallies = tallies.at[1:1 + 2 * couples:2].set(donor - passed).at[2:2 + 2 * couples:2].set(taker + passed)
    return tallies[jax.random.permutation(jax.random.fold_in(own_key, 2), count)]


def shared_out(stream_key, own, number, rows, amount, top, limit, slope):
    ranking = jax.random.permutation(stream_key, amount)
    heavy_load, ordinary = shares(amount, rows * top, limit, slope, True), shares(amount, rows * top, limit, slope, False)
    places = jnp.arange(amount)

    def named(lengths, turn):
        used = int((lengths > 0).sum())
        fixed = max(1, used // 4)
        shifted = fixed + (places - fixed + turn * (used - fixed)) % max(1, amount - fixed)
        return jnp.zeros((amount,), jnp.int32).at[ranking[jnp.where(places < fixed, places, shifted)]].set(jnp.asarray(lengths, jnp.int32))

    lengths = jnp.where(number % 4 == 0, named(heavy_load, number // 4), named(ordinary, number - number // 4 - 1))
    mixed = jax.random.permutation(jax.random.fold_in(own, 3), amount)
    source_of, receiver = mixed[0:amount // 2 * 2:2], mixed[1:amount // 2 * 2:2]
    slack = jnp.minimum(lengths[source_of] - 1, limit - lengths[receiver]) // 2
    slack = jnp.where((source_of == ranking[0]) | (receiver == ranking[0]) | (lengths[receiver] == 0), 0, jnp.maximum(slack, 0))
    shifted = jax.random.randint(jax.random.fold_in(own, 4), (amount // 2,), 0, 1 << 20) % (slack + 1)
    lengths = lengths.at[source_of].add(-shifted).at[receiver].add(shifted)
    labels = jnp.searchsorted(jnp.cumsum(lengths), jnp.arange(rows * top), side="right").astype(jnp.int32)
    listing = labels.reshape(top, rows).T
    listing = listing[jax.random.permutation(jax.random.fold_in(own, 1), rows)]
    turn = jax.random.randint(jax.random.fold_in(own, 2), (rows, 1), 0, top)
    return jnp.take_along_axis(listing, (jnp.arange(top)[None, :] + turn) % top, axis=1)


def shares(count, total, limit, slope, full):
    portions = [(1 << 20) // math.isqrt(grade ** slope) + 1 for grade in range(1, count + 1)]
    largest = limit if full else min(limit, max(-(-total // count), total * portions[0] // sum(portions)))
    least = 1 if total - largest >= count - 1 else 0
    counts, rest = [largest] + [least] * (count - 1), total - largest - least * (count - 1)
    while rest > 0:
        candidates = [i for i in range(1, count) if counts[i] < largest] or [i for i in range(1, count) if counts[i] < limit]
        mass, left = sum([portions[i] for i in candidates]), rest
        for i in candidates:
            extra = min(limit - counts[i], max(1, left * portions[i] // mass), rest)
            counts[i] = counts[i] + extra
            rest = rest - extra
    return np.array(counts)


def centred(rng, shape, deviation, reach, cuts=(), kind=jnp.bfloat16):
    factor_of = levels(rng, shape, cuts, -0.22, 0.18) if cuts else 1.0
    array = jax.random.normal(rng, shape, jnp.float32) * deviation * factor_of
    return jnp.minimum(jnp.maximum(array, -reach), reach).astype(kind)


def setup_inputs(seed: int = 0) -> dict:
    keys = jax.random.split(jax.random.key(seed), 20)
    patches = centred(keys[0], (PATCHES, VW), 1.0, 6.0, ((0, 128),))
    window_ids = jax.vmap(lambda own: jnp.searchsorted(jnp.cumsum(uneven_parts(own, 8, BLOCK, BLOCK // 2, 2)), jnp.arange(BLOCK), side="right"))(jax.random.split(keys[1], (PATCHES // BLOCK))).reshape((PATCHES // BLOCK, BLOCK)).astype(jnp.int32)
    owner_keys = jax.random.split(jax.random.fold_in(keys[2], 1), MERGED // MR)
    owner_turns = jax.random.permutation(jax.random.fold_in(keys[2], 3), MERGED // MR)
    owner = jax.vmap(lambda own, number: shared_out(jax.random.fold_in(keys[2], 2), own, number, MR, N_DP, 1, CAP, 2))(owner_keys, owner_turns).reshape((MERGED, 1))
    slot_of_row = jax.vmap(lambda own: jax.random.permutation(own, ROWS_DEV))(jax.random.split(keys[3], DEVICES)).reshape((DEVICES, ROWS_DEV)).astype(jnp.int32)
    text_embeds = centred(keys[4], (TOTAL_ROWS, D), 1.0, 6.0, ((0, 128),))
    vit_norm = jnp.clip(jnp.exp(jax.random.uniform(keys[5], (VW,), jnp.float32, math.log(0.3), math.log(3.0))), 0.3, 3.0)
    vit_qkv_w = centred(keys[6], (VW, 3 * VH * VHD), VW ** -0.5, 0.15625)
    vit_qkv_b = draw_vit_qkv_b(jax.random.fold_in(keys[19], 71), 0)
    vit_out_w = centred(keys[8], (VH * VHD, VW), (VH * VHD) ** -0.5, 0.25)
    merge_norm = jnp.clip(jnp.exp(jax.random.uniform(keys[9], (VW,), jnp.float32, math.log(0.3), math.log(3.0))), 0.3, 3.0)
    merge_w1 = centred(keys[10], (MW, MW), MW ** -0.5, 0.078125, ((1, 16),))
    merge_b1 = centred(keys[11], (MW,), 0.5, 3.0, ((0, 16),), jnp.float32)
    merge_w2 = centred(keys[12], (MW, D), MW ** -0.5, 0.078125, ((0, 16),))
    merge_b2 = centred(keys[13], (D,), 0.5, 3.0, (), jnp.float32)
    llm_norm = jnp.clip(1.0 + 0.1 * jax.random.normal(keys[14], (D,), jnp.float32), 0.5, 1.5)
    q_w = centred(keys[15], (D, QH * HD), D ** -0.5, 0.0625, ((1, 16),))
    q_b = draw_q_b(jax.random.fold_in(keys[19], 71), 0)
    kv_w = centred(keys[17], (2, D, KVH * HD), D ** -0.5, 0.0625, ((2, 16),))
    kv_b = draw_kv_b(jax.random.fold_in(keys[19], 71), 0)
    return dict(patches=patches, window_ids=window_ids, owner=owner, slot_of_row=slot_of_row, text_embeds=text_embeds, vit_norm=vit_norm, vit_qkv_w=vit_qkv_w, vit_qkv_b=vit_qkv_b, vit_out_w=vit_out_w, merge_norm=merge_norm, merge_w1=merge_w1, merge_b1=merge_b1, merge_w2=merge_w2, merge_b2=merge_b2, llm_norm=llm_norm, q_w=q_w, q_b=q_b, kv_w=kv_w, kv_b=kv_b)


epsilon = 1e-06

def rms_norm(inputs, gain):
    inputs = inputs.astype(jnp.float32)
    return inputs * lax.rsqrt(lax.optimization_barrier(jnp.mean(inputs * inputs, axis=-1, keepdims=True)) + epsilon) * gain

def vision_block(patches, window_ids, vit_norm, vit_qkv_w, vit_qkv_b, vit_out_w, merge_norm):
    normed = rms_norm(patches, vit_norm).astype(jnp.bfloat16)
    projected = (jnp.dot(normed, vit_qkv_w, preferred_element_type=jnp.float32) + vit_qkv_b).astype(jnp.bfloat16)
    blocks = window_ids.shape[0]
    width = window_ids.shape[1]
    inner_width = vit_out_w.shape[0]
    heads = inner_width // VHD
    shaped = projected.reshape(blocks, width, 3, heads, VHD).astype(jnp.float32)
    scores = jnp.einsum('bqhd,bkhd->bhqk', shaped[:, :, 0], shaped[:, :, 1]) * VHD ** (-0.5)
    in_window = window_ids[:, None, :, None] == window_ids[:, None, None, :]
    scores = jnp.where(in_window, scores, -1e+30)
    peak = lax.optimization_barrier(jnp.max(scores, axis=-1, keepdims=True))
    weights = jnp.exp(scores - peak)
    weights = (weights / lax.optimization_barrier(jnp.sum(weights, axis=-1, keepdims=True))).astype(jnp.bfloat16)
    mixture = jnp.einsum('bhqk,bkhd->bqhd', weights.astype(jnp.float32), shaped[:, :, 2])
    mixture = mixture.astype(jnp.bfloat16).reshape(blocks * width, inner_width)
    residual = (patches.astype(jnp.float32) + jnp.dot(mixture, vit_out_w, preferred_element_type=jnp.float32)).astype(jnp.bfloat16)
    merged = rms_norm(residual, merge_norm).astype(jnp.bfloat16)
    return merged.reshape(blocks * width // 4, 4 * patches.shape[1])

def causal_heads(queries, key_heads, value_heads):
    length = queries.shape[0]
    scores = jnp.einsum('qhd,khd->hqk', queries.astype(jnp.float32), key_heads.astype(jnp.float32)) * HD ** (-0.5)
    allowed = jnp.arange(length)[:, None] >= jnp.arange(length)[None, :]
    scores = jnp.where(allowed[None], scores, -1e+30)
    peak = lax.optimization_barrier(jnp.max(scores, axis=-1, keepdims=True))
    weights = jnp.exp(scores - peak)
    weights = (weights / lax.optimization_barrier(jnp.sum(weights, axis=-1, keepdims=True))).astype(jnp.bfloat16)
    mixture = jnp.einsum('hqk,khd->qhd', weights.astype(jnp.float32), value_heads.astype(jnp.float32))
    return mixture.astype(jnp.bfloat16).reshape(length, -1)

def reference(patches, window_ids, owner, slot_of_row, text_embeds, vit_norm, vit_qkv_w, vit_qkv_b, vit_out_w, merge_norm, merge_w1, merge_b1, merge_w2, merge_b2, llm_norm, q_w, q_b, kv_w, kv_b):
    merged = vision_block(patches, window_ids, vit_norm, vit_qkv_w, vit_qkv_b, vit_out_w, merge_norm)
    hidden = jax.nn.gelu(jnp.dot(merged, merge_w1, preferred_element_type=jnp.float32) + merge_b1, approximate=False).astype(jnp.bfloat16)
    shard_width = MW // N_MP

    def add_shard(running, shard_index):
        first = shard_index * shard_width
        part_hidden = lax.dynamic_slice_in_dim(hidden, first, shard_width, 1)
        part_weight = lax.dynamic_slice_in_dim(merge_w2, first, shard_width, 0)
        partial_value = jnp.dot(part_hidden, part_weight, preferred_element_type=jnp.float32)
        rounded = lax.optimization_barrier(partial_value.astype(jnp.bfloat16))
        return (running + rounded.astype(jnp.float32), 0)
    start_sum = jnp.zeros((merged.shape[0], D), jnp.float32)
    running, unused = lax.scan(add_shard, start_sum, jnp.arange(N_MP, dtype=jnp.int32))
    embedded = (running + merge_b2).astype(jnp.bfloat16)
    devices = DEVICES
    row_ids = jnp.arange(MERGED, dtype=jnp.int32)
    sender = row_ids // MR
    sender_dp = sender // N_MP
    sender_mp = sender % N_MP
    target_group = owner[:, 0]
    onehot = (target_group[:, None] == jnp.arange(N_DP, dtype=jnp.int32)[None, :]).astype(jnp.int32)
    per_device = onehot.reshape(devices, MR, N_DP)
    earlier = (jnp.cumsum(per_device, axis=1) - per_device).reshape(MERGED, N_DP)
    rank_in = lax.optimization_barrier(jnp.sum(earlier * onehot, axis=1))
    target_device = target_group * N_MP + sender_mp
    global_slot = (target_device * ROWS_DEV + sender_dp * CAP + rank_in).astype(jnp.int32)
    buffer = jnp.zeros((TOTAL_ROWS, D), jnp.bfloat16).at[global_slot].set(embedded)
    filled = jnp.zeros((TOTAL_ROWS,), jnp.int32).at[global_slot].set(1)
    source_rows = (jnp.arange(devices, dtype=jnp.int32)[:, None] * ROWS_DEV + slot_of_row).reshape(-1).astype(jnp.int32)
    sequence = jnp.where(filled[source_rows][:, None] > 0, buffer[source_rows], text_embeds)
    llm_normed = rms_norm(sequence, llm_norm).astype(jnp.bfloat16)
    queries = (jnp.dot(llm_normed, q_w, preferred_element_type=jnp.float32) + q_b).astype(jnp.bfloat16)
    key_rows = (jnp.dot(llm_normed, kv_w[0], preferred_element_type=jnp.float32) + kv_b[0]).astype(jnp.bfloat16)
    value_rows = (jnp.dot(llm_normed, kv_w[1], preferred_element_type=jnp.float32) + kv_b[1]).astype(jnp.bfloat16)
    group_size = QH // KVH

    def one_group(inputs):
        group_queries, group_keys, group_values = inputs
        key_heads = jnp.repeat(jnp.swapaxes(group_keys, 1, 2), group_size, axis=1)
        value_heads = jnp.repeat(jnp.swapaxes(group_values, 1, 2), group_size, axis=1)
        return causal_heads(group_queries, key_heads, value_heads)
    attended = lax.map(one_group, (queries.reshape(N_DP, SEQ, QH, HD), key_rows.reshape(N_DP, SEQ, HD, KVH), value_rows.reshape(N_DP, SEQ, HD, KVH)))
    return attended.reshape(N_DP * SEQ, QH * HD)
```

```python
import jax
import jax.numpy as jnp
from jax import lax
from jax.experimental import pallas as pl
from jax.experimental.pallas import tpu as pltpu
from jax.sharding import PartitionSpec as P

VHD = 80
HD = 128
QH = 32
KVH = 4


epsilon = 1e-06


def laid_out(parts, dim):
    lengths = list(parts.shape[1:])
    lengths[dim] *= parts.shape[0]
    return jnp.moveaxis(parts, 0, dim).reshape(lengths)


def copy_for_each(x, axis):
    size = lax.axis_size(axis)
    return lax.all_to_all(jnp.broadcast_to(x[None], (size, *x.shape)), axis, 0, 0, tiled=True)


def gathered_copies(x, axis, dim):
    return laid_out(copy_for_each(x, axis), dim)


def rms_norm(inputs, gain):
    inputs = inputs.astype(jnp.float32)
    return inputs * lax.rsqrt(jnp.mean(inputs * inputs, axis=-1, keepdims=True) + epsilon) * gain


def vision_block(patches, window_ids, vit_norm, vit_qkv_w, vit_qkv_b, vit_out_w, merge_norm):
    normed = rms_norm(patches, vit_norm).astype(jnp.bfloat16)
    projected = (jnp.dot(normed, vit_qkv_w, preferred_element_type=jnp.float32) + vit_qkv_b).astype(
        jnp.bfloat16
    )
    blocks = window_ids.shape[0]
    width = window_ids.shape[1]
    inner_width = vit_out_w.shape[0]
    heads = inner_width // VHD
    shaped = projected.reshape(blocks, width, 3, heads, VHD)
    scores = jnp.einsum(
        "bqhd,bkhd->bhqk", shaped[:, :, 0], shaped[:, :, 1], preferred_element_type=jnp.float32
    ) * VHD ** (-0.5)
    in_window = window_ids[:, None, :, None] == window_ids[:, None, None, :]
    scores = jnp.where(in_window, scores, -1e30)
    peak = jnp.max(scores, axis=-1, keepdims=True)
    weights = jnp.exp(scores - peak)
    weights = (weights / jnp.sum(weights, axis=-1, keepdims=True)).astype(jnp.bfloat16)
    mixture = jnp.einsum(
        "bhqk,bkhd->bqhd", weights, shaped[:, :, 2], preferred_element_type=jnp.float32
    )
    mixture = mixture.astype(jnp.bfloat16).reshape(blocks * width, inner_width)
    residual = (
        patches.astype(jnp.float32)
        + jnp.dot(mixture, vit_out_w, preferred_element_type=jnp.float32)
    ).astype(jnp.bfloat16)
    merged = rms_norm(residual, merge_norm).astype(jnp.bfloat16)
    return merged


MESH = pl.DeviceIdType.MESH
NT = (((1,), (1,)), ((), ()))


class Copies:
    def __init__(self, send, recv, local):
        self.send, self.recv, self.local = send, recv, local
        self.n, self.m = 0, 0
        self.sent = []

    def remote(self, src, dst, dev):
        k = self.n
        self.n += 1
        c = pltpu.make_async_remote_copy(
            src_ref=src, dst_ref=dst, send_sem=self.send.at[k], recv_sem=self.recv.at[k],
            device_id=dev, device_id_type=MESH)
        c.start()
        self.sent.append(c)
        return c

    def here(self, src, dst):
        k = self.m
        self.m += 1
        c = pltpu.make_async_copy(src, dst, self.local.at[k])
        c.start()
        return c

    def drain(self):
        for c in self.sent:
            c.wait_send()
        self.sent = []


def places():
    mp, dp = lax.axis_index("mp"), lax.axis_index("dp")
    y, x = mp // 4, lax.rem(mp, 4)
    X = lambda s: (dp, y * 4 + lax.rem(x + s + 4, 4))
    Y = lambda s: (dp, lax.rem(y + s + 4, 4) * 4 + x)
    Z = lambda s: (lax.rem(dp + 2 * s + 8, 8), mp)
    other = (dp + 1 - 2 * lax.rem(dp, 2), mp)
    return dp, y, x, X, Y, Z, other


def meet(devs):
    barrier = pltpu.get_barrier_semaphore()
    for d in devs:
        pl.semaphore_signal(barrier, inc=1, device_id=d, device_id_type=MESH)
    pl.semaphore_wait(barrier, len(devs))


N1 = 104


def merger_kernel(m, w1, b1, w2, b2, qw, kvt, kvb, info,
                  e_out, wq, wkv, kb, info_out,
                  G, w1v, H, W2, KVX, PO, PR, PL, PW, RO, RN, send, recv, local):
    dp, y, x, X, Y, Z, other = places()
    md = lambda v, s: lax.rem(v + s + 4, 4)
    e = dp
    z = dp // 2
    cp = Copies(send, recv, local)
    meet([X(1), X(2), X(3), Y(1), Y(2), Y(3), Z(1), Z(-1), other])
    A, B = pl.ds(0, 2), pl.ds(2, 2)
    a1 = {s: cp.remote(m.at[A], G.at[A, y, x], X(s)) for s in (1, -1)}
    c1 = {s: cp.remote(m.at[B], G.at[B, y, x], Y(s)) for s in (1, -1)}
    a2 = {(0, s): cp.remote(m.at[A], G.at[A, y, x], Y(s)) for s in (1, -1)}
    c2 = {(0, s): cp.remote(m.at[B], G.at[B, y, x], X(s)) for s in (1, -1)}
    loc = [cp.here(m, G.at[:, y, x]), cp.here(w1, w1v)]
    cols = lambda xd: pl.ds(pl.multiple_of(2048 * xd + 256 * e, 256), 256)
    mine = pl.ds(pl.multiple_of(256 * e, 256), 256)
    wx = []
    for s in (1, 3, 2):
        xd = md(x, s)
        wx.append(cp.remote(w2.at[:, cols(xd)], W2.at[x, :, mine], X(s)))
    for s in (1, 3, 2):
        xd = md(x, s)
        wx.append(cp.remote(qw.at[cols(xd), :], wq.at[x, mine, :], X(s)))
        wx.append(cp.remote(kvt.at[:, :, cols(xd)], KVX.at[x], X(s)))
        wx.append(cp.remote(kvb, kb.at[y, x], X(s)))
        wx.append(cp.remote(info, info_out.at[x], X(s)))
    wl = [cp.here(w2.at[:, cols(x)], W2.at[x, :, mine]),
          cp.here(qw.at[cols(x), :], wq.at[x, mine, :]),
          cp.here(kvt.at[:, :, cols(x)], KVX.at[x]),
          cp.here(kvb, kb.at[y, x]),
          cp.here(info, info_out.at[x])]

    af, cf = {}, {}
    for s in (1, -1):
        a1[s].wait_recv()
        xs, j = md(x, -s), 0 if s == 1 else 1
        af[s] = cp.remote(G.at[j, y, xs], G.at[j, y, xs], X(s))
        for t in (1, -1):
            a2[(-s, t)] = cp.remote(G.at[A, y, xs], G.at[A, y, xs], Y(t))
        c1[s].wait_recv()
        ys, j = md(y, -s), 2 if s == 1 else 3
        cf[s] = cp.remote(G.at[j, ys, x], G.at[j, ys, x], Y(s))
        for t in (1, -1):
            c2[(-s, t)] = cp.remote(G.at[B, ys, x], G.at[B, ys, x], X(t))
    last = []

    def pass_on(p):
        for t in (1, -1):
            a2[(p, t)].wait_recv()
            xs, ys, j = md(x, p), md(y, -t), 0 if t == 1 else 1
            last.append(cp.remote(G.at[j, ys, xs], G.at[j, ys, xs], Y(t)))
            c2[(p, t)].wait_recv()
            ys, xs, j = md(y, p), md(x, -t), 2 if t == 1 else 3
            last.append(cp.remote(G.at[j, ys, xs], G.at[j, ys, xs], X(t)))

    pass_on(0)
    for c in wx[:3]:
        c.wait_recv()
    wl[0].wait()
    first, second = pl.ds(0, 2), pl.ds(2, 2)
    bands = lambda r: pl.ds(pl.multiple_of(256 * r, 256), 256)

    def piece(name, r, half=None):
        if name == "w2":
            h = pl.ds(0, 4) if half is None else (first, second)[half]
            return W2.at[h, :, bands(r)]
        if name == "q":
            h = pl.ds(0, 4) if half is None else (first, second)[half]
            return wq.at[h, bands(r), :]
        h = pl.ds(0, 4) if half is None else (first, second)[half]
        return wkv.at[h, :, :, bands(r)]

    zs, ds_, zf, at = {}, {}, {}, {}

    def z_start(name):
        zs[name] = {s: cp.remote(piece(name, e), piece(name, e), Z(s)) for s in (1, -1)}
        ds_[name] = [cp.remote(piece(name, e), piece(name, e), other)]

    def z_mid(name):
        zf[name] = {}
        for s in (1, -1):
            zs[name][s].wait_recv()
            r, h = lax.rem(e - 2 * s + 8, 8), 0 if s == 1 else 1
            zf[name][s] = cp.remote(piece(name, r, h), piece(name, r, h), Z(s))
            ds_[name].append(cp.remote(piece(name, r), piece(name, r), other))

    def z_end(name):
        for s in (1, -1):
            zf[name][s].wait_recv()
        r = lax.rem(e + 4, 8)
        ds_[name].append(cp.remote(piece(name, r), piece(name, r), other))

    def z_all(name):
        for c in ds_[name]:
            c.wait_recv()

    z_start("w2")
    for c in wx[3:]:
        c.wait_recv()
    for c in wl[1:]:
        c.wait()
    z_start("q")
    ky = []
    for s in (1, 2, 3):
        yd = md(y, s)
        ky.append(cp.remote(KVX.at[:, yd], wkv.at[y, :, :, mine], Y(s)))
        ky.append(cp.remote(kb.at[y], kb.at[y], Y(s)))
    kl = cp.here(KVX.at[:, y], wkv.at[y, :, :, mine])
    for s in (1, -1):
        af[s].wait_recv()
        cf[s].wait_recv()
    xf, yf = md(x, 2), md(y, 2)
    for t in (1, -1):
        a2[(2, t)] = cp.remote(G.at[A, y, xf], G.at[A, y, xf], Y(t))
        c2[(2, t)] = cp.remote(G.at[B, yf, x], G.at[B, yf, x], X(t))
    pass_on(-1)
    pass_on(1)
    z_mid("w2")
    for c in ky:
        c.wait_recv()
    kl.wait()
    z_start("kv")
    pass_on(2)
    for c in last:
        c.wait_recv()
    for c in loc:
        c.wait()
    for g in range(4):
        acc = None
        for j in range(4):
            p = lax.dot_general(w1v[:, 1280 * j:1280 * (j + 1)], G[j, g].reshape(128, 1280), NT,
                                preferred_element_type=jnp.float32)
            acc = p if acc is None else acc + p
        v = acc + b1[...]
        v = 0.5 * v * (1.0 + lax.erf(v * (0.5 ** 0.5)))
        H[x, :, 128 * g:128 * (g + 1)] = v.astype(jnp.bfloat16)
    h1 = {s: cp.remote(H.at[x], H.at[x], X(s)) for s in (1, -1)}
    z_end("w2")
    z_mid("q")
    z_mid("kv")
    h2 = []
    for s in (1, -1):
        h1[s].wait_recv()
        xs, r = md(x, -s), pl.ds(0, 160) if s == 1 else pl.ds(160, 160)
        h2.append(cp.remote(H.at[xs, r, :], H.at[xs, r, :], X(s)))
    z_all("w2")
    for c in h2:
        c.wait_recv()

    def product(g, put):
        hg = H[:, :, pl.ds(pl.multiple_of(128 * g, 128), 128)].reshape(1280, 128).T
        for n in range(4):
            cs = slice(512 * n, 512 * (n + 1))
            put(cs, jnp.dot(hg, W2[:, :, cs].reshape(1280, 512), preferred_element_type=jnp.float32))

    def to(ref):
        def put(cs, v):
            ref[:, cs] = v.astype(ref.dtype)
        return put

    product(md(y, 2), to(PO))
    lo, hi = pl.ds(0, 64), pl.ds(64, 64)
    o = {1: cp.remote(PO.at[lo], RO.at[0], Y(1)), -1: cp.remote(PO.at[hi], RO.at[1], Y(-1))}
    product(md(y, 1), to(PR))
    n1 = [cp.remote(PR.at[hi], RN.at[0, hi], Y(1))]
    product(md(y, -1), to(PL))
    n1.append(cp.remote(PL.at[lo], RN.at[1, lo], Y(-1)))
    o[1].wait_recv()
    PR[0:64, :] = (PR[0:64, :].astype(jnp.float32) + RO[0].astype(jnp.float32)).astype(jnp.bfloat16)
    n1.append(cp.remote(PR.at[lo], RN.at[0, lo], Y(1)))
    o[-1].wait_recv()
    PL[64:128, :] = (PL[64:128, :].astype(jnp.float32) + RO[1].astype(jnp.float32)).astype(jnp.bfloat16)
    n1.append(cp.remote(PL.at[hi], RN.at[1, hi], Y(-1)))
    product(y, to(PW))
    z_end("q")
    z_end("kv")
    for c in n1:
        c.wait_recv()
    total = PW[...] + RN[0].astype(jnp.float32) + RN[1].astype(jnp.float32)
    e_out[...] = (total + b2[:, pl.ds(pl.multiple_of(2048 * x, 2048), 2048)]).astype(jnp.bfloat16)
    z_all("q")
    z_all("kv")
    cp.drain()


def merger(m, w1, b1, w2, b2, qw, kvt, kvb, info):
    bf, f32 = jnp.bfloat16, jnp.float32
    V, ANY = pl.BlockSpec(memory_space=pltpu.VMEM), pl.BlockSpec(memory_space=pl.ANY)
    S = jax.ShapeDtypeStruct
    return pl.pallas_call(
        merger_kernel,
        out_shape=(S((128, 2048), bf), S((4, 2048, 256), bf), S((4, 4, 16, 2048), bf), S((4, 4, 8, 128), f32),
                   S((4, 8, 128), jnp.int32)),
        in_specs=[V, ANY, V, ANY, V, ANY, ANY, V, V],
        out_specs=[V] * 5,
        scratch_shapes=[
            pltpu.VMEM((4, 4, 4, 32, 1280), bf),
            pltpu.VMEM((320, 5120), bf),
            pltpu.VMEM((4, 320, 512), bf),
            pltpu.VMEM((4, 320, 2048), bf),
            pltpu.VMEM((4, 4, 16, 256), bf),
            pltpu.VMEM((128, 2048), bf),
            pltpu.VMEM((128, 2048), bf),
            pltpu.VMEM((128, 2048), bf),
            pltpu.VMEM((128, 2048), f32),
            pltpu.VMEM((2, 64, 2048), bf),
            pltpu.VMEM((2, 128, 2048), bf),
            pltpu.SemaphoreType.DMA((N1,)),
            pltpu.SemaphoreType.DMA((N1,)),
            pltpu.SemaphoreType.DMA((16,)),
        ],
        compiler_params=pltpu.CompilerParams(collective_id=1, has_side_effects=True, vmem_limit_bytes=60000000),
        name="merger",
    )(m, w1, b1, w2, b2, qw, kvt, kvb, info)


def prepared(merged, owner, slot_of_row, kv_w, kv_b):
    x = lax.rem(lax.axis_index("mp"), 4)
    m = merged.reshape(32, 4, 1280).transpose(1, 0, 2)
    kvt = kv_w.transpose(0, 2, 1).reshape(2, 8, 4, 8192).transpose(2, 0, 1, 3).reshape(4, 16, 8192)
    kvb = jnp.pad(kv_b.reshape(2, 8, 4).transpose(2, 0, 1).reshape(4, 16), ((0, 4), (0, 112)))
    zero = jnp.zeros((8, 128), jnp.int32)
    info = lax.dynamic_update_slice(zero, owner.reshape(1, 32), (0, 32 * x))
    info = lax.dynamic_update_slice(info, slot_of_row, (1 + x // 2, 64 * lax.rem(x, 2)))
    return m, kvt, kvb, info


def shards(
    patches,
    window_ids,
    owner,
    slot_of_row,
    text_embeds,
    vit_norm,
    vit_qkv_w,
    vit_qkv_b,
    vit_out_w,
    merge_norm,
    merge_w1,
    merge_b1,
    merge_w2,
    merge_b2,
    llm_norm,
    q_w,
    q_b,
    kv_w,
    kv_b,
):
    merged_rows = vision_block(
        patches, window_ids, vit_norm, vit_qkv_w, vit_qkv_b, vit_out_w, merge_norm
    )
    own_index = lax.axis_index("mp")
    merged = merged_rows
    m, kvt, kvb, info = prepared(merged, owner, slot_of_row, kv_w, kv_b)
    part, wq, wkv, kb, info_all = merger(
        m, merge_w1.T, merge_b1[:, None], merge_w2, merge_b2[None], q_w, kvt, kvb, info
    )
    embedded = lax.all_to_all(
        part.reshape(4, 32, 2048), "mp", 0, 0, tiled=True,
        axis_index_groups=[[4 * i + j for j in range(4)] for i in range(4)],
    ).transpose(1, 0, 2).reshape(32, 8192)
    seq_rows = text_embeds.shape[0]
    groups = lax.axis_size("dp")
    capacity = seq_rows // groups
    target_group = owner[:, 0]
    onehot = (target_group[:, None] == jnp.arange(groups, dtype=jnp.int32)[None, :]).astype(
        jnp.int32
    )
    rank_in = jnp.sum((jnp.cumsum(onehot, axis=0) - onehot) * onehot, axis=1)
    send_slot = target_group * capacity + rank_in
    selector = send_slot[None, :] == jnp.arange(seq_rows, dtype=jnp.int32)[:, None]
    buffer = jnp.dot(
        selector.astype(jnp.bfloat16), embedded, preferred_element_type=jnp.float32
    ).astype(jnp.bfloat16)
    buffer = buffer.reshape(groups, capacity, embedded.shape[1])
    marks = jnp.sum(selector.astype(jnp.int32), axis=1).reshape(groups, capacity)
    arrived, arrived_marks = (
        lax.all_to_all(buffer, "dp", split_axis=0, concat_axis=0, tiled=True),
        lax.all_to_all(marks, "dp", split_axis=0, concat_axis=0, tiled=True),
    )
    arrived = arrived.reshape(seq_rows, embedded.shape[1])
    arrived_marks = arrived_marks.reshape(seq_rows)
    chosen = slot_of_row[0]
    sequence = jnp.where(arrived_marks[chosen][:, None] > 0, arrived[chosen], text_embeds)
    llm_normed = rms_norm(sequence, llm_norm).astype(jnp.bfloat16)
    query_cols = q_w.shape[1]
    kv_cols = kv_w.shape[2]
    shard_rows = lax.all_gather(llm_normed, "mp", axis=0, tiled=True)
    projected = jnp.concatenate(
        [
            jnp.dot(shard_rows, q_w, preferred_element_type=jnp.float32),
            jnp.dot(shard_rows, kv_w[0], preferred_element_type=jnp.float32),
            jnp.dot(shard_rows, kv_w[1], preferred_element_type=jnp.float32),
        ],
        axis=1,
    )
    length = projected.shape[0]
    queries = (projected[:, :query_cols] + q_b).astype(jnp.bfloat16)
    key_rows = (projected[:, query_cols : query_cols + kv_cols] + kv_b[0]).astype(jnp.bfloat16)
    value_rows = (projected[:, query_cols + kv_cols :] + kv_b[1]).astype(jnp.bfloat16)
    stacked = jnp.stack([key_rows.T, value_rows.T])
    all_heads = gathered_copies(stacked, "mp", 1)
    heads_here = query_cols // HD
    group_size = QH // KVH
    kv_head = own_index * heads_here // group_size
    by_head = all_heads.reshape(2, HD, KVH, length)
    key_cols = lax.dynamic_index_in_dim(by_head[0], kv_head, 1, keepdims=False)
    value_cols = lax.dynamic_index_in_dim(by_head[1], kv_head, 1, keepdims=False)
    query_heads = queries.reshape(length, heads_here, HD)
    scores = jnp.einsum(
        "qhd,dk->hqk", query_heads, key_cols, preferred_element_type=jnp.float32
    ) * HD ** (-0.5)
    allowed = jnp.arange(length)[:, None] >= jnp.arange(length)[None, :]
    scores = jnp.where(allowed[None], scores, -1e30)
    peak = jnp.max(scores, axis=-1, keepdims=True)
    weights = jnp.exp(scores - peak)
    weights = (weights / jnp.sum(weights, axis=-1, keepdims=True)).astype(jnp.bfloat16)
    mixture = jnp.einsum("hqk,dk->qhd", weights, value_cols, preferred_element_type=jnp.float32)
    return mixture.astype(jnp.bfloat16).reshape(length, query_cols)


def solution(mesh):
    return jax.shard_map(
        shards,
        mesh=mesh,
        in_specs=(
            P(("dp", "mp"), None),
            P(("dp", "mp"), None),
            P(("dp", "mp"), None),
            P(("dp", "mp"), None),
            P(("dp", "mp"), None),
            P(),
            P(),
            P(),
            P(),
            P(),
            P(None, "mp"),
            P("mp"),
            P("mp", None),
            P(),
            P(),
            P(None, "mp"),
            P("mp"),
            P(None, None, "mp"),
            P(None, "mp"),
        ),
        out_specs=P("dp", "mp"),
        check_vma=False,
    )
```

```python
import jax
import jax.numpy as jnp
from jax import lax
from jax.experimental import pallas as pl
from jax.experimental.pallas import tpu as pltpu
from jax.sharding import PartitionSpec as P

VHD = 80
HD = 128
QH = 32
KVH = 4


epsilon = 1e-06


def laid_out(parts, dim):
    lengths = list(parts.shape[1:])
    lengths[dim] *= parts.shape[0]
    return jnp.moveaxis(parts, 0, dim).reshape(lengths)


def copy_for_each(x, axis):
    size = lax.axis_size(axis)
    return lax.all_to_all(jnp.broadcast_to(x[None], (size, *x.shape)), axis, 0, 0, tiled=True)


def gathered_copies(x, axis, dim):
    return laid_out(copy_for_each(x, axis), dim)


def rms_norm(inputs, gain):
    inputs = inputs.astype(jnp.float32)
    return inputs * lax.rsqrt(jnp.mean(inputs * inputs, axis=-1, keepdims=True) + epsilon) * gain


def vision_block(patches, window_ids, vit_norm, vit_qkv_w, vit_qkv_b, vit_out_w, merge_norm):
    normed = rms_norm(patches, vit_norm).astype(jnp.bfloat16)
    projected = (jnp.dot(normed, vit_qkv_w, preferred_element_type=jnp.float32) + vit_qkv_b).astype(
        jnp.bfloat16
    )
    blocks = window_ids.shape[0]
    width = window_ids.shape[1]
    inner_width = vit_out_w.shape[0]
    heads = inner_width // VHD
    shaped = projected.reshape(blocks, width, 3, heads, VHD)
    scores = jnp.einsum(
        "bqhd,bkhd->bhqk", shaped[:, :, 0], shaped[:, :, 1], preferred_element_type=jnp.float32
    ) * VHD ** (-0.5)
    in_window = window_ids[:, None, :, None] == window_ids[:, None, None, :]
    scores = jnp.where(in_window, scores, -1e30)
    peak = jnp.max(scores, axis=-1, keepdims=True)
    weights = jnp.exp(scores - peak)
    weights = (weights / jnp.sum(weights, axis=-1, keepdims=True)).astype(jnp.bfloat16)
    mixture = jnp.einsum(
        "bhqk,bkhd->bqhd", weights, shaped[:, :, 2], preferred_element_type=jnp.float32
    )
    mixture = mixture.astype(jnp.bfloat16).reshape(blocks * width, inner_width)
    residual = (
        patches.astype(jnp.float32)
        + jnp.dot(mixture, vit_out_w, preferred_element_type=jnp.float32)
    ).astype(jnp.bfloat16)
    merged = rms_norm(residual, merge_norm).astype(jnp.bfloat16)
    return merged


MESH = pl.DeviceIdType.MESH
NT = (((1,), (1,)), ((), ()))


class Copies:
    def __init__(self, send, recv, local):
        self.send, self.recv, self.local = send, recv, local
        self.n, self.m = 0, 0
        self.sent = []

    def remote(self, src, dst, dev):
        k = self.n
        self.n += 1
        c = pltpu.make_async_remote_copy(
            src_ref=src, dst_ref=dst, send_sem=self.send.at[k], recv_sem=self.recv.at[k],
            device_id=dev, device_id_type=MESH)
        c.start()
        self.sent.append(c)
        return c

    def here(self, src, dst):
        k = self.m
        self.m += 1
        c = pltpu.make_async_copy(src, dst, self.local.at[k])
        c.start()
        return c

    def drain(self):
        for c in self.sent:
            c.wait_send()
        self.sent = []


def places():
    mp, dp = lax.axis_index("mp"), lax.axis_index("dp")
    y, x = mp // 4, lax.rem(mp, 4)
    X = lambda s: (dp, y * 4 + lax.rem(x + s + 4, 4))
    Y = lambda s: (dp, lax.rem(y + s + 4, 4) * 4 + x)
    Z = lambda s: (lax.rem(dp + 2 * s + 8, 8), mp)
    other = (dp + 1 - 2 * lax.rem(dp, 2), mp)
    return dp, y, x, X, Y, Z, other


def meet(devs):
    barrier = pltpu.get_barrier_semaphore()
    for d in devs:
        pl.semaphore_signal(barrier, inc=1, device_id=d, device_id_type=MESH)
    pl.semaphore_wait(barrier, len(devs))


N1 = 104


def merger_kernel(m, w1, b1, w2, b2, qw, kvt, kvb, info,
                  e_out, wq, wkv, kb, info_out,
                  G, w1v, H, W2, KVX, PO, PR, PL, PW, RO, RN, send, recv, local):
    dp, y, x, X, Y, Z, other = places()
    md = lambda v, s: lax.rem(v + s + 4, 4)
    e = dp
    z = dp // 2
    cp = Copies(send, recv, local)
    meet([X(1), X(2), X(3), Y(1), Y(2), Y(3), Z(1), Z(-1), other])
    A, B = pl.ds(0, 2), pl.ds(2, 2)
    a1 = {s: cp.remote(m.at[A], G.at[A, y, x], X(s)) for s in (1, -1)}
    c1 = {s: cp.remote(m.at[B], G.at[B, y, x], Y(s)) for s in (1, -1)}
    a2 = {(0, s): cp.remote(m.at[A], G.at[A, y, x], Y(s)) for s in (1, -1)}
    c2 = {(0, s): cp.remote(m.at[B], G.at[B, y, x], X(s)) for s in (1, -1)}
    loc = [cp.here(m, G.at[:, y, x]), cp.here(w1, w1v)]
    cols = lambda xd: pl.ds(pl.multiple_of(2048 * xd + 256 * e, 256), 256)
    mine = pl.ds(pl.multiple_of(256 * e, 256), 256)
    wx = []
    for s in (1, 3, 2):
        xd = md(x, s)
        wx.append(cp.remote(w2.at[:, cols(xd)], W2.at[x, :, mine], X(s)))
    for s in (1, 3, 2):
        xd = md(x, s)
        wx.append(cp.remote(qw.at[cols(xd), :], wq.at[x, mine, :], X(s)))
        wx.append(cp.remote(kvt.at[:, :, cols(xd)], KVX.at[x], X(s)))
        wx.append(cp.remote(kvb, kb.at[y, x], X(s)))
        wx.append(cp.remote(info, info_out.at[x], X(s)))
    wl = [cp.here(w2.at[:, cols(x)], W2.at[x, :, mine]),
          cp.here(qw.at[cols(x), :], wq.at[x, mine, :]),
          cp.here(kvt.at[:, :, cols(x)], KVX.at[x]),
          cp.here(kvb, kb.at[y, x]),
          cp.here(info, info_out.at[x])]

    af, cf = {}, {}
    for s in (1, -1):
        a1[s].wait_recv()
        xs, j = md(x, -s), 0 if s == 1 else 1
        af[s] = cp.remote(G.at[j, y, xs], G.at[j, y, xs], X(s))
        for t in (1, -1):
            a2[(-s, t)] = cp.remote(G.at[A, y, xs], G.at[A, y, xs], Y(t))
        c1[s].wait_recv()
        ys, j = md(y, -s), 2 if s == 1 else 3
        cf[s] = cp.remote(G.at[j, ys, x], G.at[j, ys, x], Y(s))
        for t in (1, -1):
            c2[(-s, t)] = cp.remote(G.at[B, ys, x], G.at[B, ys, x], X(t))
    last = []

    def pass_on(p):
        for t in (1, -1):
            a2[(p, t)].wait_recv()
            xs, ys, j = md(x, p), md(y, -t), 0 if t == 1 else 1
            last.append(cp.remote(G.at[j, ys, xs], G.at[j, ys, xs], Y(t)))
            c2[(p, t)].wait_recv()
            ys, xs, j = md(y, p), md(x, -t), 2 if t == 1 else 3
            last.append(cp.remote(G.at[j, ys, xs], G.at[j, ys, xs], X(t)))

    pass_on(0)
    for c in wx[:3]:
        c.wait_recv()
    wl[0].wait()
    first, second = pl.ds(0, 2), pl.ds(2, 2)
    bands = lambda r: pl.ds(pl.multiple_of(256 * r, 256), 256)

    def piece(name, r, half=None):
        if name == "w2":
            h = pl.ds(0, 4) if half is None else (first, second)[half]
            return W2.at[h, :, bands(r)]
        if name == "q":
            h = pl.ds(0, 4) if half is None else (first, second)[half]
            return wq.at[h, bands(r), :]
        h = pl.ds(0, 4) if half is None else (first, second)[half]
        return wkv.at[h, :, :, bands(r)]

    zs, ds_, zf, at = {}, {}, {}, {}

    def z_start(name):
        zs[name] = {s: cp.remote(piece(name, e), piece(name, e), Z(s)) for s in (1, -1)}
        ds_[name] = [cp.remote(piece(name, e), piece(name, e), other)]

    def z_mid(name):
        zf[name] = {}
        for s in (1, -1):
            zs[name][s].wait_recv()
            r, h = lax.rem(e - 2 * s + 8, 8), 0 if s == 1 else 1
            zf[name][s] = cp.remote(piece(name, r, h), piece(name, r, h), Z(s))
            ds_[name].append(cp.remote(piece(name, r), piece(name, r), other))

    def z_end(name):
        for s in (1, -1):
            zf[name][s].wait_recv()
        r = lax.rem(e + 4, 8)
        ds_[name].append(cp.remote(piece(name, r), piece(name, r), other))

    def z_all(name):
        for c in ds_[name]:
            c.wait_recv()

    z_start("w2")
    for c in wx[3:]:
        c.wait_recv()
    for c in wl[1:]:
        c.wait()
    z_start("q")
    ky = []
    for s in (1, 2, 3):
        yd = md(y, s)
        ky.append(cp.remote(KVX.at[:, yd], wkv.at[y, :, :, mine], Y(s)))
        ky.append(cp.remote(kb.at[y], kb.at[y], Y(s)))
    kl = cp.here(KVX.at[:, y], wkv.at[y, :, :, mine])
    for s in (1, -1):
        af[s].wait_recv()
        cf[s].wait_recv()
    xf, yf = md(x, 2), md(y, 2)
    for t in (1, -1):
        a2[(2, t)] = cp.remote(G.at[A, y, xf], G.at[A, y, xf], Y(t))
        c2[(2, t)] = cp.remote(G.at[B, yf, x], G.at[B, yf, x], X(t))
    pass_on(-1)
    pass_on(1)
    z_mid("w2")
    for c in ky:
        c.wait_recv()
    kl.wait()
    z_start("kv")
    pass_on(2)
    for c in last:
        c.wait_recv()
    for c in loc:
        c.wait()
    for g in range(4):
        acc = None
        for j in range(4):
            p = lax.dot_general(w1v[:, 1280 * j:1280 * (j + 1)], G[j, g].reshape(128, 1280), NT,
                                preferred_element_type=jnp.float32)
            acc = p if acc is None else acc + p
        v = acc + b1[...]
        v = 0.5 * v * (1.0 + lax.erf(v * (0.5 ** 0.5)))
        H[x, :, 128 * g:128 * (g + 1)] = v.astype(jnp.bfloat16)
    h1 = {s: cp.remote(H.at[x], H.at[x], X(s)) for s in (1, -1)}
    z_end("w2")
    z_mid("q")
    z_mid("kv")
    h2 = []
    for s in (1, -1):
        h1[s].wait_recv()
        xs, r = md(x, -s), pl.ds(0, 160) if s == 1 else pl.ds(160, 160)
        h2.append(cp.remote(H.at[xs, r, :], H.at[xs, r, :], X(s)))
    z_all("w2")
    for c in h2:
        c.wait_recv()

    def product(g, put):
        hg = H[:, :, pl.ds(pl.multiple_of(128 * g, 128), 128)].reshape(1280, 128).T
        for n in range(4):
            cs = slice(512 * n, 512 * (n + 1))
            put(cs, jnp.dot(hg, W2[:, :, cs].reshape(1280, 512), preferred_element_type=jnp.float32))

    def to(ref):
        def put(cs, v):
            ref[:, cs] = v.astype(ref.dtype)
        return put

    product(md(y, 2), to(PO))
    lo, hi = pl.ds(0, 64), pl.ds(64, 64)
    o = {1: cp.remote(PO.at[lo], RO.at[0], Y(1)), -1: cp.remote(PO.at[hi], RO.at[1], Y(-1))}
    product(md(y, 1), to(PR))
    n1 = [cp.remote(PR.at[hi], RN.at[0, hi], Y(1))]
    product(md(y, -1), to(PL))
    n1.append(cp.remote(PL.at[lo], RN.at[1, lo], Y(-1)))
    o[1].wait_recv()
    PR[0:64, :] = (PR[0:64, :].astype(jnp.float32) + RO[0].astype(jnp.float32)).astype(jnp.bfloat16)
    n1.append(cp.remote(PR.at[lo], RN.at[0, lo], Y(1)))
    o[-1].wait_recv()
    PL[64:128, :] = (PL[64:128, :].astype(jnp.float32) + RO[1].astype(jnp.float32)).astype(jnp.bfloat16)
    n1.append(cp.remote(PL.at[hi], RN.at[1, hi], Y(-1)))
    product(y, to(PW))
    z_end("q")
    z_end("kv")
    for c in n1:
        c.wait_recv()
    total = PW[...] + RN[0].astype(jnp.float32) + RN[1].astype(jnp.float32)
    e_out[...] = (total + b2[:, pl.ds(pl.multiple_of(2048 * x, 2048), 2048)]).astype(jnp.bfloat16)
    z_all("q")
    z_all("kv")
    cp.drain()


def merger(m, w1, b1, w2, b2, qw, kvt, kvb, info):
    bf, f32 = jnp.bfloat16, jnp.float32
    V, ANY = pl.BlockSpec(memory_space=pltpu.VMEM), pl.BlockSpec(memory_space=pl.ANY)
    S = jax.ShapeDtypeStruct
    return pl.pallas_call(
        merger_kernel,
        out_shape=(S((128, 2048), bf), S((4, 2048, 256), bf), S((4, 4, 16, 2048), bf), S((4, 4, 8, 128), f32),
                   S((4, 8, 128), jnp.int32)),
        in_specs=[V, ANY, V, ANY, V, ANY, ANY, V, V],
        out_specs=[V] * 5,
        scratch_shapes=[
            pltpu.VMEM((4, 4, 4, 32, 1280), bf),
            pltpu.VMEM((320, 5120), bf),
            pltpu.VMEM((4, 320, 512), bf),
            pltpu.VMEM((4, 320, 2048), bf),
            pltpu.VMEM((4, 4, 16, 256), bf),
            pltpu.VMEM((128, 2048), bf),
            pltpu.VMEM((128, 2048), bf),
            pltpu.VMEM((128, 2048), bf),
            pltpu.VMEM((128, 2048), f32),
            pltpu.VMEM((2, 64, 2048), bf),
            pltpu.VMEM((2, 128, 2048), bf),
            pltpu.SemaphoreType.DMA((N1,)),
            pltpu.SemaphoreType.DMA((N1,)),
            pltpu.SemaphoreType.DMA((16,)),
        ],
        compiler_params=pltpu.CompilerParams(collective_id=1, has_side_effects=True, vmem_limit_bytes=60000000),
        name="merger",
    )(m, w1, b1, w2, b2, qw, kvt, kvb, info)


def prepared(merged, owner, slot_of_row, kv_w, kv_b):
    x = lax.rem(lax.axis_index("mp"), 4)
    m = merged.reshape(32, 4, 1280).transpose(1, 0, 2)
    kvt = kv_w.transpose(0, 2, 1).reshape(2, 8, 4, 8192).transpose(2, 0, 1, 3).reshape(4, 16, 8192)
    kvb = jnp.pad(kv_b.reshape(2, 8, 4).transpose(2, 0, 1).reshape(4, 16), ((0, 4), (0, 112)))
    zero = jnp.zeros((8, 128), jnp.int32)
    info = lax.dynamic_update_slice(zero, owner.reshape(1, 32), (0, 32 * x))
    info = lax.dynamic_update_slice(info, slot_of_row, (1 + x // 2, 64 * lax.rem(x, 2)))
    return m, kvt, kvb, info


N2 = 128


def language_kernel(part, info, wq, wkv, kb, text, gain, qb,
                    q_out, kv_out,
                    T, SB, R, A, SS, SY, SC, Q0, QR, QL, QO, RQO, RQN, KP, RKV, send, recv, local):
    dp, y, x, X, Y, Z, other = places()
    md = lambda v, s: lax.rem(v + s + 4, 4)
    bf, f32 = jnp.bfloat16, jnp.float32
    mp = y * 4 + x
    cp = Copies(send, recv, local)
    group = [(lax.rem(dp + s, 8), mp) for s in range(1, 8)]
    meet([X(1), X(2), X(3), Y(1), Y(2), Y(3)] + group)
    quarter = lambda v: pl.ds(pl.multiple_of(2048 * v, 2048), 2048)
    iota = lambda shape, d: lax.broadcasted_iota(jnp.int32, shape, d)

    tx = [cp.remote(text.at[:, quarter(md(x, s))], T.at[x], X(s)) for s in (1, 3, 2)]
    tl = cp.here(text.at[:, quarter(x)], T.at[x])

    tab = info[0] + info[1] + info[2] + info[3]
    own = tab[0:1, :]
    down = jnp.broadcast_to(own.astype(f32), (128, 128)).T.astype(jnp.int32)
    r0, r1 = iota((128, 128), 0), iota((128, 128), 1)
    before = (down == own) & (r0 < r1) & (r0 // 32 == r1 // 32)
    rank = jnp.sum(before.astype(jnp.int32), axis=0, keepdims=True)
    target = own * 32 + (iota((1, 128), 1) // 32) * 8 + rank
    pick = (iota((256, 128), 0) == target).astype(f32).astype(bf)
    for n in range(4):
        cs = slice(512 * n, 512 * (n + 1))
        v = jnp.dot(pick, part[:, cs], preferred_element_type=f32)
        SB[:, :, cs] = v.astype(bf).reshape(8, 32, 512)
    v = jnp.dot(pick, jnp.ones((128, 128), bf), preferred_element_type=f32)
    SB[:, :, 2048:2176] = v.astype(bf).reshape(8, 32, 128)
    hand = [cp.remote(SB.at[d[0]], R.at[dp], d) for d in group]
    hl = cp.here(SB.at[dp], R.at[dp])

    choose = []
    for i in range(2):
        s = jnp.broadcast_to(tab[1 + i:2 + i, :].astype(f32), (128, 128)).T.astype(jnp.int32)
        s = jnp.concatenate([s, s], axis=1)
        lane, row = iota((128, 256), 1), iota((128, 256), 0)
        hit = ((lane // 32) * 8 + lane % 8 == s) & ((lane % 32) // 8 == row // 64 + 2 * i)
        choose.append(hit.astype(f32).astype(bf))
    for c in tx:
        c.wait_recv()
    tl.wait()
    for c in hand:
        c.wait_recv()
    hl.wait()

    gx = gain[:, quarter(x)]
    sq = []
    yh = {}
    for i in range(2):
        seen = jnp.dot(choose[i], R[:, :, 2048:2176].reshape(256, 128), preferred_element_type=f32)
        filled = seen[:, 0:1] > 0.5
        total = jnp.zeros((128, 1), f32)
        for n in range(4):
            cs = slice(512 * n, 512 * (n + 1))
            v = jnp.dot(choose[i], R[:, :, cs].reshape(256, 512), preferred_element_type=f32)
            v = jnp.where(filled, v, T[2 * i:2 * i + 2, :, cs].reshape(128, 512).astype(f32))
            total = total + jnp.sum(v * v, axis=1, keepdims=True)
            A[y, 128 * i:128 * (i + 1), cs] = (v * gx[:, cs]).astype(bf)
        sq.append(total)
        h = pl.ds(128 * i, 128)
        if i == 0:
            yh[(1, 0)] = cp.remote(A.at[y, h], A.at[y, h], Y(1))
        else:
            yh[(-1, 1)] = cp.remote(A.at[y, h], A.at[y, h], Y(-1))
    h = [pl.ds(0, 128), pl.ds(128, 128)]
    yh[(1, 1)] = cp.remote(A.at[y, h[1]], A.at[y, h[1]], Y(1))
    yh[(-1, 0)] = cp.remote(A.at[y, h[0]], A.at[y, h[0]], Y(-1))
    SS[x] = jnp.concatenate([jnp.broadcast_to(t, (128, 128)).T[0:8, :] for t in sq], axis=1)
    sx = [cp.remote(SS.at[x], SS.at[x], X(s)) for s in (1, 2, 3)]

    def unit(g, i):
        rows = pl.ds(pl.multiple_of(256 * g + 128 * i, 128), 128)
        a = A[g, 128 * i:128 * (i + 1), :]
        prod = lambda s: jnp.dot(a, wq[md(x, s)], preferred_element_type=f32)
        lo, hi = pl.ds(pl.multiple_of(256 * g + 128 * i, 64), 64), pl.ds(pl.multiple_of(256 * g + 128 * i + 64, 64), 64)
        QO[rows, :] = prod(2).astype(bf)
        o = [cp.remote(QO.at[lo], RQO.at[0, lo], X(1)), cp.remote(QO.at[hi], RQO.at[1, hi], X(-1))]
        KP[rows, :] = lax.dot_general(a, wkv[...].reshape(256, 2048), NT, preferred_element_type=f32).astype(bf)
        slot = 2 * g + i
        k = []
        for s in (2, 1, 3):
            xd = md(x, s)
            src = pl.ds(pl.multiple_of(256 * g + 128 * i + 32 * xd, 32), 32)
            k.append(cp.remote(KP.at[src], RKV.at[x, slot], X(s)))
        QR[rows, :] = prod(1).astype(bf)
        n = [cp.remote(QR.at[hi], RQN.at[0, hi], X(1))]
        QL[rows, :] = prod(-1).astype(bf)
        n.append(cp.remote(QL.at[lo], RQN.at[1, lo], X(-1)))
        Q0[rows, :] = prod(0)
        return g, i, rows, lo, hi, slot, o, k, n

    def relay(u):
        g, i, rows, lo, hi, slot, o, k, n = u
        o[0].wait_recv()
        QR[lo, :] = (QR[lo, :].astype(f32) + RQO[0, lo, :].astype(f32)).astype(bf)
        n.append(cp.remote(QR.at[lo], RQN.at[0, lo], X(1)))
        o[1].wait_recv()
        QL[hi, :] = (QL[hi, :].astype(f32) + RQO[1, hi, :].astype(f32)).astype(bf)
        n.append(cp.remote(QL.at[hi], RQN.at[1, hi], X(-1)))

    bias = jnp.concatenate([kb[p // 4, p % 4, pl.ds(y, 1), 0:16] for p in range(16)], axis=1)

    def keys(u):
        g, i, rows, lo, hi, slot, o, k, n = u
        for c in k:
            c.wait_recv()
        m = pl.ds(pl.multiple_of(256 * g + 128 * i + 32 * x, 32), 32)
        v = KP[m, :].astype(f32)
        for s in (1, 2, 3):
            v = v + RKV[md(x, s), slot].astype(f32)
        sc = SC[m, :]
        v = v * jnp.concatenate([sc, sc], axis=1) + bias
        kv_out[m, :] = v.astype(bf)
        u[7].extend(cp.remote(kv_out.at[m], kv_out.at[m], X(s)) for s in (2, 1, 3))

    def scale(g):
        v = lax.rsqrt(SY[g] * (1.0 / 8192.0) + 1e-6)
        for i in range(2):
            SC[pl.ds(pl.multiple_of(256 * g + 128 * i, 128), 128), :] = jnp.broadcast_to(
                v[0:1, 128 * i:128 * (i + 1)], (128, 128)).T

    units = [unit(y, 0), unit(y, 1)]
    for c in sx:
        c.wait_recv()
    SY[y] = SS[0] + SS[1] + SS[2] + SS[3]
    sy = [cp.remote(SY.at[y], SY.at[y], Y(s)) for s in (1, 2, 3)]
    scale(y)
    relay(units[0])
    relay(units[1])
    keys(units[0])
    keys(units[1])
    far = {}
    up, dn, op = md(y, 1), md(y, -1), md(y, 2)
    yh[(1, 0)].wait_recv()
    far[1] = cp.remote(A.at[dn, h[0]], A.at[dn, h[0]], Y(1))
    yh[(-1, 1)].wait_recv()
    far[-1] = cp.remote(A.at[up, h[1]], A.at[up, h[1]], Y(-1))
    units.append(unit(dn, 0))
    units.append(unit(up, 1))
    for c in sy:
        c.wait_recv()
    for g in (dn, up, op):
        scale(g)
    relay(units[2])
    relay(units[3])
    keys(units[2])
    keys(units[3])
    yh[(1, 1)].wait_recv()
    units.append(unit(dn, 1))
    yh[(-1, 0)].wait_recv()
    units.append(unit(up, 0))
    relay(units[4])
    relay(units[5])
    keys(units[4])
    keys(units[5])
    far[1].wait_recv()
    units.append(unit(op, 0))
    far[-1].wait_recv()
    units.append(unit(op, 1))
    relay(units[6])
    relay(units[7])
    keys(units[6])
    keys(units[7])
    for u in units:
        rows, n, k = u[2], u[8], u[7]
        for c in n:
            c.wait_recv()
        sc = SC[rows, :]
        v = Q0[rows, :] + RQN[0, rows, :].astype(f32) + RQN[1, rows, :].astype(f32)
        q_out[rows, :] = (v * jnp.concatenate([sc, sc], axis=1) + qb[...]).astype(bf)
    for u in units:
        for c in u[7][3:]:
            c.wait_recv()
    cp.drain()


def language(part, info, wq, wkv, kb, text, gain, qb):
    bf, f32 = jnp.bfloat16, jnp.float32
    V, ANY = pl.BlockSpec(memory_space=pltpu.VMEM), pl.BlockSpec(memory_space=pl.ANY)
    S = jax.ShapeDtypeStruct
    M = pltpu.VMEM
    return pl.pallas_call(
        language_kernel,
        out_shape=(S((1024, 256), bf), S((1024, 256), bf)),
        in_specs=[V, V, V, V, V, ANY, V, V],
        out_specs=[V] * 2,
        scratch_shapes=[
            M((4, 64, 2048), bf),
            M((8, 32, 2176), bf),
            M((8, 32, 2176), bf),
            M((4, 256, 2048), bf),
            M((4, 8, 256), f32),
            M((4, 8, 256), f32),
            M((1024, 128), f32),
            M((1024, 256), f32),
            M((1024, 256), bf),
            M((1024, 256), bf),
            M((1024, 256), bf),
            M((2, 1024, 256), bf),
            M((2, 1024, 256), bf),
            M((1024, 256), bf),
            M((4, 8, 32, 256), bf),
            pltpu.SemaphoreType.DMA((N2,)),
            pltpu.SemaphoreType.DMA((N2,)),
            pltpu.SemaphoreType.DMA((4,)),
        ],
        compiler_params=pltpu.CompilerParams(collective_id=2, has_side_effects=True, vmem_limit_bytes=60000000),
        name="language",
    )(part, info, wq, wkv, kb, text, gain, qb)


def attention_kernel(q, kv, out):
    bf, f32 = jnp.bfloat16, jnp.float32
    c, d = lax.broadcasted_iota(jnp.int32, (256, 128), 0), lax.broadcasted_iota(jnp.int32, (256, 128), 1)
    spot = (d // 8) * 16 + d % 8
    keys = jnp.dot(kv[...], (c == spot).astype(f32).astype(bf), preferred_element_type=f32).astype(bf)
    values = jnp.dot(kv[...], (c == spot + 8).astype(f32).astype(bf), preferred_element_type=f32).astype(bf)
    for i in range(4):
        rows = slice(256 * i, 256 * (i + 1))
        n = 256 * (i + 1)
        for h in range(2):
            hs = slice(128 * h, 128 * (h + 1))
            s = lax.dot_general(q[rows, hs], keys[:n], NT, preferred_element_type=f32) * HD ** (-0.5)
            ok = lax.broadcasted_iota(jnp.int32, (256, n), 0) + 256 * i >= lax.broadcasted_iota(jnp.int32, (256, n), 1)
            s = jnp.where(ok, s, -1e30)
            p = jnp.exp(s - jnp.max(s, axis=1, keepdims=True))
            total = jnp.sum(p, axis=1, keepdims=True)
            m = jnp.dot(p.astype(bf), values[:n], preferred_element_type=f32)
            out[rows, hs] = (m / total).astype(bf)


def attention(q, kv):
    V = pl.BlockSpec(memory_space=pltpu.VMEM)
    return pl.pallas_call(
        attention_kernel,
        out_shape=jax.ShapeDtypeStruct((1024, 256), jnp.bfloat16),
        in_specs=[V, V],
        out_specs=V,
        compiler_params=pltpu.CompilerParams(vmem_limit_bytes=60000000),
        name="attention",
    )(q, kv)


def shards(
    patches,
    window_ids,
    owner,
    slot_of_row,
    text_embeds,
    vit_norm,
    vit_qkv_w,
    vit_qkv_b,
    vit_out_w,
    merge_norm,
    merge_w1,
    merge_b1,
    merge_w2,
    merge_b2,
    llm_norm,
    q_w,
    q_b,
    kv_w,
    kv_b,
):
    merged_rows = vision_block(
        patches, window_ids, vit_norm, vit_qkv_w, vit_qkv_b, vit_out_w, merge_norm
    )
    merged = merged_rows
    m, kvt, kvb, info = prepared(merged, owner, slot_of_row, kv_w, kv_b)
    part, wq, wkv, kb, info_all = merger(
        m, merge_w1.T, merge_b1[:, None], merge_w2, merge_b2[None], q_w, kvt, kvb, info
    )
    q, kv = language(part, info_all, wq, wkv, kb, text_embeds, llm_norm[None], q_b[None])
    return attention(q, kv)


def solution(mesh):
    return jax.shard_map(
        shards,
        mesh=mesh,
        in_specs=(
            P(("dp", "mp"), None),
            P(("dp", "mp"), None),
            P(("dp", "mp"), None),
            P(("dp", "mp"), None),
            P(("dp", "mp"), None),
            P(),
            P(),
            P(),
            P(),
            P(),
            P(None, "mp"),
            P("mp"),
            P("mp", None),
            P(),
            P(),
            P(None, "mp"),
            P("mp"),
            P(None, None, "mp"),
            P(None, "mp"),
        ),
        out_specs=P("dp", "mp"),
        check_vma=False,
    )
```

```python
import jax
import jax.numpy as jnp
from jax import lax
from jax.experimental import pallas as pl
from jax.experimental.pallas import tpu as pltpu
from jax.sharding import PartitionSpec as P

VHD = 80
HD = 128
MESH = pl.DeviceIdType.MESH
NT = (((1,), (1,)), ((), ()))


class Copies:
    def __init__(self, send, recv, local):
        self.send, self.recv, self.local = send, recv, local
        self.n, self.m = 0, 0
        self.sent = []

    def remote(self, src, dst, dev):
        k = self.n
        self.n += 1
        c = pltpu.make_async_remote_copy(
            src_ref=src, dst_ref=dst, send_sem=self.send.at[k], recv_sem=self.recv.at[k],
            device_id=dev, device_id_type=MESH)
        c.start()
        self.sent.append(c)
        return c

    def here(self, src, dst):
        k = self.m
        self.m += 1
        c = pltpu.make_async_copy(src, dst, self.local.at[k])
        c.start()
        return c

    def drain(self):
        for c in self.sent:
            c.wait_send()
        self.sent = []


def places():
    mp, dp = lax.axis_index("mp"), lax.axis_index("dp")
    y, x = mp // 4, lax.rem(mp, 4)
    X = lambda s: (dp, y * 4 + lax.rem(x + s + 4, 4))
    Y = lambda s: (dp, lax.rem(y + s + 4, 4) * 4 + x)
    Z = lambda s: (lax.rem(dp + 2 * s + 8, 8), mp)
    other = (dp + 1 - 2 * lax.rem(dp, 2), mp)
    return dp, y, x, X, Y, Z, other


def meet(devs):
    barrier = pltpu.get_barrier_semaphore()
    for d in devs:
        pl.semaphore_signal(barrier, inc=1, device_id=d, device_id_type=MESH)
    pl.semaphore_wait(barrier, len(devs))


N3 = 300


def vision(patches, ids, norm, qkv_w, qkv_b, out_w, gain):
    bf, f32 = jnp.bfloat16, jnp.float32
    iota = lambda shape, d: lax.broadcasted_iota(jnp.int32, shape, d)
    i, s = iota((128, 128), 0), iota((128, 128), 1)
    perm = (s == (i % 32) * 4 + i // 32).astype(f32).astype(bf)
    p = jnp.dot(perm, patches[...], preferred_element_type=f32)
    wide = jnp.broadcast_to(ids[...].astype(f32), (128, 128)).astype(bf)
    across = lax.dot_general(wide, perm, NT, preferred_element_type=f32)
    same = across == across.T
    normed = p * lax.rsqrt(jnp.mean(p * p, axis=1, keepdims=True) + 1e-6) * norm[...]
    qkv = (jnp.dot(normed.astype(bf), qkv_w[...], preferred_element_type=f32) + qkv_b[...]).astype(bf)
    tiles = [None] * 5
    for h in range(8):
        lo, hi = 80 * h // 128, (80 * h + 207) // 128
        lane = iota((128, 128 * (hi - lo)), 1) + 128 * lo
        here = (lane >= 80 * h) & (lane < 80 * h + 80)
        part = lambda k: qkv[:, 640 * k + 128 * lo:640 * k + 128 * hi]
        zero = jnp.zeros((), bf)
        sc = lax.dot_general(jnp.where(here, part(0), zero), part(1), NT, preferred_element_type=f32) * VHD ** (-0.5)
        sc = jnp.where(same, sc, -1e30)
        e = jnp.exp(sc - jnp.max(sc, axis=1, keepdims=True))
        w = (e / jnp.sum(e, axis=1, keepdims=True)).astype(bf)
        mix = jnp.dot(w, jnp.where(here, part(2), zero), preferred_element_type=f32)
        for t in range(lo, hi):
            v = mix[:, 128 * (t - lo):128 * (t - lo + 1)]
            tiles[t] = v if tiles[t] is None else tiles[t] + v
    mixed = jnp.concatenate(tiles, axis=1).astype(bf)
    r = (p + jnp.dot(mixed, out_w[...], preferred_element_type=f32)).astype(bf).astype(f32)
    return (r * lax.rsqrt(jnp.mean(r * r, axis=1, keepdims=True) + 1e-6) * gain[...]).astype(bf)


def whole_kernel(patches, ids, owner, slots, text, vnorm, qkv_w, qkv_b, out_w, mnorm, w1, b1, w2, b2, gain, qw, qb,
                 kvw, kvb, q_out, kv_out,
                 MS, G, QKVW, OUTW, w1v, H, HT, W2, wq, wkv, KVS, KVX, KBS, kb, INS, info, RW, RQ,
                 PC, RO, RN, T, TR, SB, R, A, SS, SY, SC, Q0, QR, QL, QO, RQO, RQN, KP, RKV, send, recv, local):
    dp, y, x, X, Y, Z, other = places()
    md = lambda v, s: lax.rem(v + s + 4, 4)
    bf, f32 = jnp.bfloat16, jnp.float32
    iota = lambda shape, d: lax.broadcasted_iota(jnp.int32, shape, d)
    e, mp = dp, y * 4 + x
    cp = Copies(send, recv, local)
    lv = [cp.here(qkv_w, QKVW), cp.here(out_w, OUTW), cp.here(w1, w1v)]
    group = [(lax.rem(dp + s, 8), mp) for s in (2, 6, 1, 3, 5, 7, 4)]
    meet([X(1), X(2), X(3), Y(1), Y(2), Y(3)] + group)
    A2, B2 = pl.ds(0, 2), pl.ds(2, 2)
    cols = lambda xd: pl.ds(pl.multiple_of(2048 * xd + 256 * e, 256), 256)
    mine = pl.ds(pl.multiple_of(256 * e, 256), 256)
    first, second = pl.ds(0, 2), pl.ds(2, 2)

    xo = md(x, 2)
    w2_half = [pl.ds(0, 160), pl.ds(160, 160)]
    q_half = lambda v, i: pl.ds(pl.multiple_of(2048 * v + 256 * e + 128 * i, 128), 128)
    w2r = [cp.remote(w2.at[w2_half[i], cols(xo)], RW.at[i], X(1 - 2 * i)) for i in range(2)]
    w2d = [cp.remote(w2.at[:, cols(md(x, s))], W2.at[x, :, mine], X(s)) for s in (1, -1)]
    qr = [cp.remote(qw.at[q_half(xo, i), :], RQ.at[i], X(1 - 2 * i)) for i in range(2)]
    qd = [cp.remote(qw.at[cols(md(x, s)), :], wq.at[x, mine, :], X(s)) for s in (1, -1)]
    wl = [cp.here(w2.at[:, cols(x)], W2.at[x, :, mine]), cp.here(qw.at[cols(x), :], wq.at[x, mine, :])]

    lv[0].wait()
    lv[1].wait()
    MS[...] = vision(patches, ids, vnorm, QKVW, qkv_b, OUTW, mnorm).reshape(4, 32, 1280)

    a1 = {s: cp.remote(MS.at[A2], G.at[A2, y, x], X(s)) for s in (1, -1)}
    c1 = {s: cp.remote(MS.at[B2], G.at[B2, y, x], Y(s)) for s in (1, -1)}
    a2 = {(0, s): cp.remote(MS.at[A2], G.at[A2, y, x], Y(s)) for s in (1, -1)}
    c2 = {(0, s): cp.remote(MS.at[B2], G.at[B2, y, x], X(s)) for s in (1, -1)}
    gl = cp.here(MS, G.at[:, y, x])
    for c in w2r:
        c.wait_recv()
    w2f = [cp.remote(RW.at[i], W2.at[md(x, 2 * i - 1), w2_half[i], mine], X(1 - 2 * i)) for i in range(2)]
    for c in w2d:
        c.wait_recv()

    i64, s64 = iota((64, 64), 0), iota((64, 64), 1)
    order = (s64 == (i64 // 8 % 2) * 32 + (i64 % 8) * 4 + i64 // 16).astype(f32).astype(bf)
    for n in range(4):
        cs = slice(2048 * n, 2048 * (n + 1))
        v = jnp.dot(order, kvw[:, :, cs].reshape(64, 2048), preferred_element_type=f32)
        KVS[:, :, cs] = v.astype(bf).reshape(4, 16, 2048)
    li, ll = iota((128, 128), 0), iota((128, 128), 1)
    rows = []
    flat = jnp.concatenate([kvb[0:1, :], kvb[1:2, :], jnp.zeros((1, 64), f32)], axis=1)
    down = jnp.broadcast_to(flat, (128, 128)).T
    for j in range(4):
        keep = (li == (ll // 8) * 32 + (ll % 8) * 4 + j) & (ll < 16)
        rows.append(jnp.sum(jnp.where(keep, down, 0.0), axis=0, keepdims=True))
    KBS[...] = jnp.concatenate(rows + [jnp.zeros((4, 128), f32)], axis=0)
    own4 = jnp.broadcast_to(jnp.concatenate([owner[...]] * 4, axis=1), (8, 128))
    slot2 = jnp.broadcast_to(jnp.concatenate([slots[...]] * 2, axis=1), (8, 128))
    t0, t1 = iota((8, 128), 0), iota((8, 128), 1)
    INS[...] = jnp.where((t0 == 0) & (t1 // 32 == x), own4,
                         jnp.where((t0 == 1 + x // 2) & (t1 // 64 == x % 2), slot2, 0))
    wx = []
    for s in (1, 3, 2):
        wx.append(cp.remote(KVS.at[:, :, cols(md(x, s))], KVX.at[x], X(s)))
        wx.append(cp.remote(KBS, kb.at[y, x], X(s)))
        wx.append(cp.remote(INS, info.at[x], X(s)))
    KVX[x] = KVS[:, :, cols(x)]
    kb[y, x] = KBS[...]
    info[x] = INS[...]

    af, cf = {}, {}
    for s in (1, -1):
        a1[s].wait_recv()
        xs, j = md(x, -s), 0 if s == 1 else 1
        af[s] = cp.remote(G.at[j, y, xs], G.at[j, y, xs], X(s))
        for t in (1, -1):
            a2[(-s, t)] = cp.remote(G.at[A2, y, xs], G.at[A2, y, xs], Y(t))
        c1[s].wait_recv()
        ys, j = md(y, -s), 2 if s == 1 else 3
        cf[s] = cp.remote(G.at[j, ys, x], G.at[j, ys, x], Y(s))
        for t in (1, -1):
            c2[(-s, t)] = cp.remote(G.at[B2, ys, x], G.at[B2, ys, x], X(t))
    last = []

    def pass_on(p):
        for t in (1, -1):
            a2[(p, t)].wait_recv()
            xs, ys, j = md(x, p), md(y, -t), 0 if t == 1 else 1
            last.append(cp.remote(G.at[j, ys, xs], G.at[j, ys, xs], Y(t)))
            c2[(p, t)].wait_recv()
            ys, xs, j = md(y, p), md(x, -t), 2 if t == 1 else 3
            last.append(cp.remote(G.at[j, ys, xs], G.at[j, ys, xs], X(t)))

    pass_on(0)
    bands = lambda r: pl.ds(pl.multiple_of(256 * r, 256), 256)

    def piece(name, r, half=None):
        h = pl.ds(0, 4) if half is None else (first, second)[half]
        if name == "w2":
            return W2.at[h, :, bands(r)]
        if name == "q":
            return wq.at[h, bands(r), :]
        return wkv.at[h, :, :, bands(r)]

    zs, ds_, zf = {}, {}, {}

    def z_start(name):
        zs[name] = {s: cp.remote(piece(name, e), piece(name, e), Z(s)) for s in (1, -1)}
        ds_[name] = [cp.remote(piece(name, e), piece(name, e), other)]

    def z_mid(name):
        zf[name] = {}
        for s in (1, -1):
            zs[name][s].wait_recv()
            r, h = lax.rem(e - 2 * s + 8, 8), 0 if s == 1 else 1
            zf[name][s] = cp.remote(piece(name, r, h), piece(name, r, h), Z(s))
            ds_[name].append(cp.remote(piece(name, r), piece(name, r), other))

    def z_end(name):
        for s in (1, -1):
            zf[name][s].wait_recv()
        r = lax.rem(e + 4, 8)
        ds_[name].append(cp.remote(piece(name, r), piece(name, r), other))

    def z_all(name):
        for c in ds_[name]:
            c.wait_recv()

    for c in w2f:
        c.wait_recv()
    wl[0].wait()
    z_start("w2")
    for c in qr:
        c.wait_recv()
    qf = [cp.remote(RQ.at[i], wq.at[md(x, 2 * i - 1), pl.ds(pl.multiple_of(256 * e + 128 * i, 128), 128), :],
                    X(1 - 2 * i)) for i in range(2)]
    for c in wx:
        c.wait_recv()
    ky = []
    for s in (1, 2, 3):
        yd = md(y, s)
        ky.append(cp.remote(KVX.at[:, yd], wkv.at[y, :, :, mine], Y(s)))
        ky.append(cp.remote(kb.at[y], kb.at[y], Y(s)))
    wkv[y, :, :, mine] = KVX[:, y]
    for s in (1, -1):
        af[s].wait_recv()
        cf[s].wait_recv()
    xf, yf = md(x, 2), md(y, 2)
    for t in (1, -1):
        a2[(2, t)] = cp.remote(G.at[A2, y, xf], G.at[A2, y, xf], Y(t))
        c2[(2, t)] = cp.remote(G.at[B2, yf, x], G.at[B2, yf, x], X(t))
    pass_on(-1)
    pass_on(1)
    for c in qd + qf:
        c.wait_recv()
    wl[1].wait()
    z_mid("w2")
    z_start("q")
    for c in ky:
        c.wait_recv()
    z_start("kv")
    pass_on(2)
    for c in last:
        c.wait_recv()
    gl.wait()
    lv[2].wait()
    wide = jnp.concatenate([b1[...], jnp.zeros((1, 64), f32)], axis=1)
    bcol = jnp.broadcast_to(wide, (128, 384)).T[0:320, :]
    bcol = jnp.concatenate([bcol, bcol], axis=1)
    for g in range(2):
        acc = None
        for j in range(4):
            p = lax.dot_general(w1v[:, 1280 * j:1280 * (j + 1)], G[j, 2 * g:2 * g + 2].reshape(256, 1280), NT,
                                preferred_element_type=f32)
            acc = p if acc is None else acc + p
        v = acc + bcol
        v = 0.5 * v * (1.0 + lax.erf(v * (0.5 ** 0.5)))
        H[x, :, 256 * g:256 * (g + 1)] = v.astype(bf)
    h1 = {s: cp.remote(H.at[x], H.at[x], X(s)) for s in (1, -1)}
    z_end("w2")
    z_mid("q")
    z_mid("kv")
    h2 = []
    for s in (1, -1):
        h1[s].wait_recv()
        xs, r = md(x, -s), pl.ds(0, 160) if s == 1 else pl.ds(160, 160)
        h2.append(cp.remote(H.at[xs, r, :], H.at[xs, r, :], X(s)))
    quarter = lambda v: pl.ds(pl.multiple_of(2048 * v, 2048), 2048)
    th = [pl.ds(0, 32), pl.ds(32, 32)]
    tr = [cp.remote(text.at[th[i], quarter(xo)], TR.at[i], X(1 - 2 * i)) for i in range(2)]
    td = [cp.remote(text.at[:, quarter(md(x, s))], T.at[x], X(s)) for s in (1, -1)]
    tl = cp.here(text.at[:, quarter(x)], T.at[x])
    tab = info[0] + info[1] + info[2] + info[3]
    own = tab[0:1, :]
    down = jnp.broadcast_to(own.astype(f32), (128, 128)).T.astype(jnp.int32)
    before = (down == own) & (li < ll) & (li // 32 == ll // 32)
    rank = jnp.sum(before.astype(jnp.int32), axis=0, keepdims=True)
    target = own * 32 + (iota((1, 128), 1) // 32) * 8 + rank
    pick = (iota((256, 128), 0) == target).astype(f32).astype(bf)
    choose = []
    for i in range(2):
        s = jnp.broadcast_to(tab[1 + i:2 + i, :].astype(f32), (128, 128)).T.astype(jnp.int32)
        s = jnp.concatenate([s, s], axis=1)
        lane, row = iota((128, 256), 1), iota((128, 256), 0)
        hit = ((lane // 32) * 8 + lane % 8 == s) & ((lane % 32) // 8 == row // 64 + 2 * i)
        choose.append(hit.astype(f32).astype(bf))
    z_all("w2")
    for c in h2:
        c.wait_recv()
    HT[...] = H[...].reshape(1280, 512).T

    lo, hi = pl.ds(0, 64), pl.ds(64, 64)
    yr, yl = md(y, 1), md(y, -1)
    ro, rn, hand, handl = {}, {}, {}, {}

    def mul(c):
        cs = slice(512 * c, 512 * (c + 1))
        v = jnp.dot(HT[...], W2[:, :, cs].reshape(1280, 512), preferred_element_type=f32)
        PC[c] = v.astype(bf).reshape(4, 128, 512)
        ro[c] = [cp.remote(PC.at[c, md(y, 2), lo], RO.at[c, 0], Y(1)),
                 cp.remote(PC.at[c, md(y, 2), hi], RO.at[c, 1], Y(-1))]
        rn[c] = [cp.remote(PC.at[c, yr, hi], RN.at[c, 0, hi], Y(1)),
                 cp.remote(PC.at[c, yl, lo], RN.at[c, 1, lo], Y(-1))]

    def relay_y(c):
        ro[c][0].wait_recv()
        PC[c, yr, 0:64, :] = (PC[c, yr, 0:64, :].astype(f32) + RO[c, 0].astype(f32)).astype(bf)
        rn[c].append(cp.remote(PC.at[c, yr, lo], RN.at[c, 0, lo], Y(1)))
        ro[c][1].wait_recv()
        PC[c, yl, 64:128, :] = (PC[c, yl, 64:128, :].astype(f32) + RO[c, 1].astype(f32)).astype(bf)
        rn[c].append(cp.remote(PC.at[c, yl, hi], RN.at[c, 1, hi], Y(-1)))

    def give(c):
        for k in rn[c]:
            k.wait_recv()
        v = PC[c, y].astype(f32) + RN[c, 0].astype(f32) + RN[c, 1].astype(f32)
        v = (v + b2[:, pl.ds(pl.multiple_of(2048 * x + 512 * c, 512), 512)]).astype(bf)
        SB[c, :, :, 0:512] = jnp.dot(pick, v, preferred_element_type=f32).astype(bf).reshape(8, 32, 512)
        w = pl.ds(0, 512)
        if c == 0:
            v = jnp.dot(pick, jnp.ones((128, 128), bf), preferred_element_type=f32)
            SB[c, :, :, 512:640] = v.astype(bf).reshape(8, 32, 128)
            w = pl.ds(0, 640)
        hand[c] = [cp.remote(SB.at[c, d[0], :, w], R.at[c, dp, :, w], d) for d in group]
        handl[c] = cp.here(SB.at[c, dp, :, w], R.at[c, dp, :, w])

    h = [pl.ds(0, 128), pl.ds(128, 128)]
    gx = gain[:, quarter(x)]
    filled, sq, yc = [None, None], [None, None], {1: [], -1: []}

    def take(c):
        cs = slice(512 * c, 512 * (c + 1))
        for k in hand[c]:
            k.wait_recv()
        handl[c].wait()
        for i in range(2):
            if c == 0:
                seen = jnp.dot(choose[i], R[0, :, :, 512:640].reshape(256, 128), preferred_element_type=f32)
                filled[i] = seen[:, 0:1] > 0.5
            v = jnp.dot(choose[i], R[c, :, :, 0:512].reshape(256, 512), preferred_element_type=f32)
            v = jnp.where(filled[i], v, T[2 * i:2 * i + 2, :, cs].reshape(128, 512).astype(f32))
            t = jnp.sum(v * v, axis=1, keepdims=True)
            sq[i] = t if c == 0 else sq[i] + t
            A[y, 128 * i:128 * (i + 1), cs] = (v * gx[:, cs]).astype(bf)
            w, s = pl.ds(512 * c, 512), 1 - 2 * i
            yc[s].append(cp.remote(A.at[y, h[i], w], A.at[y, h[i], w], Y(s)))

    mul(0)
    mul(1)
    mul(2)
    relay_y(0)
    mul(3)
    relay_y(1)
    give(0)
    for c in tr:
        c.wait_recv()
    tf = [cp.remote(TR.at[i], T.at[md(x, 2 * i - 1), th[i]], X(1 - 2 * i)) for i in range(2)]
    relay_y(2)
    give(1)
    relay_y(3)
    z_end("q")
    z_end("kv")
    for c in td + tf:
        c.wait_recv()
    tl.wait()
    take(0)
    give(2)
    take(1)
    give(3)
    take(2)
    take(3)
    yo = {1: cp.remote(A.at[y, h[1]], A.at[y, h[1]], Y(1)), -1: cp.remote(A.at[y, h[0]], A.at[y, h[0]], Y(-1))}
    SS[x] = jnp.concatenate([jnp.broadcast_to(t, (128, 128)).T[0:8, :] for t in sq], axis=1)
    sx = [cp.remote(SS.at[x], SS.at[x], X(s)) for s in (1, 2, 3)]
    z_all("q")
    z_all("kv")

    def pair(ga, ia, gb, ib):
        a = jnp.concatenate([A[ga, 128 * ia:128 * (ia + 1), :], A[gb, 128 * ib:128 * (ib + 1), :]], axis=0)
        us = []
        for g, i in ((ga, ia), (gb, ib)):
            at = lambda off, n, g=g, i=i: pl.ds(pl.multiple_of(256 * g + 128 * i + off, n), n)
            us.append(dict(g=g, i=i, rows=at(0, 128), lo=at(0, 64), hi=at(64, 64), slot=2 * g + i, at=at))
        prod = lambda s: jnp.dot(a, wq[md(x, s)], preferred_element_type=f32)

        def put(ref, v):
            v = v.astype(ref.dtype)
            for n, u in enumerate(us):
                ref[u["rows"], :] = v[128 * n:128 * (n + 1)]

        put(QO, prod(2))
        for u in us:
            u["o"] = [cp.remote(QO.at[u["lo"]], RQO.at[0, u["lo"]], X(1)),
                      cp.remote(QO.at[u["hi"]], RQO.at[1, u["hi"]], X(-1))]
        put(KP, lax.dot_general(a, wkv[...].reshape(256, 2048), NT, preferred_element_type=f32))
        for u in us:
            u["k"] = []
            for s in (2, 1, 3):
                xd = md(x, s)
                src = pl.ds(pl.multiple_of(256 * u["g"] + 128 * u["i"] + 32 * xd, 32), 32)
                u["k"].append(cp.remote(KP.at[src], RKV.at[x, u["slot"]], X(s)))
        put(QR, prod(1))
        for u in us:
            u["n"] = [cp.remote(QR.at[u["hi"]], RQN.at[0, u["hi"]], X(1))]
        put(QL, prod(-1))
        for u in us:
            u["n"].append(cp.remote(QL.at[u["lo"]], RQN.at[1, u["lo"]], X(-1)))
        put(Q0, prod(0))
        return us

    def relay(us):
        for u in us:
            lo, hi = u["lo"], u["hi"]
            u["o"][0].wait_recv()
            QR[lo, :] = (QR[lo, :].astype(f32) + RQO[0, lo, :].astype(f32)).astype(bf)
            u["n"].append(cp.remote(QR.at[lo], RQN.at[0, lo], X(1)))
            u["o"][1].wait_recv()
            QL[hi, :] = (QL[hi, :].astype(f32) + RQO[1, hi, :].astype(f32)).astype(bf)
            u["n"].append(cp.remote(QL.at[hi], RQN.at[1, hi], X(-1)))

    bias = jnp.concatenate([kb[p // 4, p % 4, pl.ds(y, 1), 0:16] for p in range(16)], axis=1)

    def keys(us):
        for u in us:
            for c in u["k"]:
                c.wait_recv()
            m = pl.ds(pl.multiple_of(256 * u["g"] + 128 * u["i"] + 32 * x, 32), 32)
            v = KP[m, :].astype(f32)
            for s in (1, 2, 3):
                v = v + RKV[md(x, s), u["slot"]].astype(f32)
            sc = SC[m, :]
            v = v * jnp.concatenate([sc, sc], axis=1) + bias
            kv_out[m, :] = v.astype(bf)
            u["f"] = [cp.remote(kv_out.at[m], kv_out.at[m], X(s)) for s in (2, 1, 3)]

    def scale(g):
        v = lax.rsqrt(SY[g] * (1.0 / 8192.0) + 1e-6)
        for i in range(2):
            SC[pl.ds(pl.multiple_of(256 * g + 128 * i, 128), 128), :] = jnp.broadcast_to(
                v[0:1, 128 * i:128 * (i + 1)], (128, 128)).T

    def finish(us):
        for u in us:
            rows = u["rows"]
            for c in u["n"]:
                c.wait_recv()
            sc = SC[rows, :]
            v = Q0[rows, :] + RQN[0, rows, :].astype(f32) + RQN[1, rows, :].astype(f32)
            q_out[rows, :] = (v * jnp.concatenate([sc, sc], axis=1) + qb[...]).astype(bf)
        for u in us:
            for c in u["f"]:
                c.wait_recv()

    u0 = pair(y, 0, y, 1)
    for c in sx:
        c.wait_recv()
    SY[y] = SS[0] + SS[1] + SS[2] + SS[3]
    sy = [cp.remote(SY.at[y], SY.at[y], Y(s)) for s in (1, 2, 3)]
    scale(y)
    relay(u0)
    keys(u0)
    up, dn, op = yr, yl, md(y, 2)
    far = {}
    for c in yc[1]:
        c.wait_recv()
    far[1] = cp.remote(A.at[dn, h[0]], A.at[dn, h[0]], Y(1))
    for c in yc[-1]:
        c.wait_recv()
    far[-1] = cp.remote(A.at[up, h[1]], A.at[up, h[1]], Y(-1))
    u1 = pair(dn, 0, up, 1)
    for c in sy:
        c.wait_recv()
    for g in (dn, up, op):
        scale(g)
    relay(u1)
    keys(u1)
    finish(u0)
    yo[1].wait_recv()
    yo[-1].wait_recv()
    u2 = pair(dn, 1, up, 0)
    relay(u2)
    keys(u2)
    finish(u1)
    finish(u2)
    far[1].wait_recv()
    far[-1].wait_recv()
    u3 = pair(op, 0, op, 1)
    relay(u3)
    keys(u3)
    finish(u3)
    cp.drain()


def whole(patches, ids, owner, slots, text, vnorm, qkv_w, qkv_b, out_w, mnorm, w1, b1, w2, b2, gain, qw, qb, kvw, kvb):
    bf, f32, i32 = jnp.bfloat16, jnp.float32, jnp.int32
    V, ANY = pl.BlockSpec(memory_space=pltpu.VMEM), pl.BlockSpec(memory_space=pl.ANY)
    S = jax.ShapeDtypeStruct
    M = pltpu.VMEM
    return pl.pallas_call(
        whole_kernel,
        out_shape=(S((1024, 256), bf), S((1024, 256), bf)),
        in_specs=[V, V, V, V, ANY, V, ANY, V, ANY, V, ANY, V, ANY, V, V, ANY, V, V, V],
        out_specs=[V] * 2,
        scratch_shapes=[
            M((4, 32, 1280), bf),
            M((4, 4, 4, 32, 1280), bf),
            M((1280, 1920), bf),
            M((640, 1280), bf),
            M((320, 5120), bf),
            M((4, 320, 512), bf),
            M((512, 1280), bf),
            M((4, 320, 2048), bf),
            M((4, 2048, 256), bf),
            M((4, 4, 16, 2048), bf),
            M((4, 16, 8192), bf),
            M((4, 4, 16, 256), bf),
            M((8, 128), f32),
            M((4, 4, 8, 128), f32),
            M((8, 128), i32),
            M((4, 8, 128), i32),
            M((2, 160, 256), bf),
            M((2, 128, 256), bf),
            M((4, 4, 128, 512), bf),
            M((4, 2, 64, 512), bf),
            M((4, 2, 128, 512), bf),
            M((4, 64, 2048), bf),
            M((2, 32, 2048), bf),
            M((4, 8, 32, 640), bf),
            M((4, 8, 32, 640), bf),
            M((4, 256, 2048), bf),
            M((4, 8, 256), f32),
            M((4, 8, 256), f32),
            M((1024, 128), f32),
            M((1024, 256), f32),
            M((1024, 256), bf),
            M((1024, 256), bf),
            M((1024, 256), bf),
            M((2, 1024, 256), bf),
            M((2, 1024, 256), bf),
            M((1024, 256), bf),
            M((4, 8, 32, 256), bf),
            pltpu.SemaphoreType.DMA((N3,)),
            pltpu.SemaphoreType.DMA((N3,)),
            pltpu.SemaphoreType.DMA((16,)),
        ],
        compiler_params=pltpu.CompilerParams(collective_id=1, has_side_effects=True, vmem_limit_bytes=64000000),
        name="whole",
    )(patches, ids, owner, slots, text, vnorm, qkv_w, qkv_b, out_w, mnorm, w1, b1, w2, b2, gain, qw, qb, kvw, kvb)


def attention_kernel(q, kv, out):
    bf, f32 = jnp.bfloat16, jnp.float32
    c, d = lax.broadcasted_iota(jnp.int32, (256, 128), 0), lax.broadcasted_iota(jnp.int32, (256, 128), 1)
    spot = (d // 8) * 16 + d % 8
    keys = jnp.dot(kv[...], (c == spot).astype(f32).astype(bf), preferred_element_type=f32).astype(bf)
    values = jnp.dot(kv[...], (c == spot + 8).astype(f32).astype(bf), preferred_element_type=f32).astype(bf)
    for i in range(4):
        rows = slice(256 * i, 256 * (i + 1))
        n = 256 * (i + 1)
        for h in range(2):
            hs = slice(128 * h, 128 * (h + 1))
            s = lax.dot_general(q[rows, hs], keys[:n], NT, preferred_element_type=f32) * HD ** (-0.5)
            ok = lax.broadcasted_iota(jnp.int32, (256, n), 0) + 256 * i >= lax.broadcasted_iota(jnp.int32, (256, n), 1)
            s = jnp.where(ok, s, -1e30)
            p = jnp.exp(s - jnp.max(s, axis=1, keepdims=True))
            total = jnp.sum(p, axis=1, keepdims=True)
            m = jnp.dot(p.astype(bf), values[:n], preferred_element_type=f32)
            out[rows, hs] = (m / total).astype(bf)


def attention(q, kv):
    V = pl.BlockSpec(memory_space=pltpu.VMEM)
    return pl.pallas_call(
        attention_kernel,
        out_shape=jax.ShapeDtypeStruct((1024, 256), jnp.bfloat16),
        in_specs=[V, V],
        out_specs=V,
        compiler_params=pltpu.CompilerParams(vmem_limit_bytes=60000000),
        name="attention",
    )(q, kv)


def shards(
    patches,
    window_ids,
    owner,
    slot_of_row,
    text_embeds,
    vit_norm,
    vit_qkv_w,
    vit_qkv_b,
    vit_out_w,
    merge_norm,
    merge_w1,
    merge_b1,
    merge_w2,
    merge_b2,
    llm_norm,
    q_w,
    q_b,
    kv_w,
    kv_b,
):
    q, kv = whole(
        patches, window_ids, owner.reshape(1, 32), slot_of_row, text_embeds, vit_norm[None], vit_qkv_w,
        vit_qkv_b[None], vit_out_w, merge_norm[None], merge_w1.T, merge_b1[None], merge_w2, merge_b2[None],
        llm_norm[None], q_w, q_b[None], kv_w.transpose(0, 2, 1), kv_b,
    )
    return attention(q, kv)


def solution(mesh):
    return jax.shard_map(
        shards,
        mesh=mesh,
        in_specs=(
            P(("dp", "mp"), None),
            P(("dp", "mp"), None),
            P(("dp", "mp"), None),
            P(("dp", "mp"), None),
            P(("dp", "mp"), None),
            P(),
            P(),
            P(),
            P(),
            P(),
            P(None, "mp"),
            P("mp"),
            P("mp", None),
            P(),
            P(),
            P(None, "mp"),
            P("mp"),
            P(None, None, "mp"),
            P(None, "mp"),
        ),
        out_specs=P("dp", "mp"),
        check_vma=False,
    )
```

```python
import jax
import jax.numpy as jnp
from jax import lax
from jax.experimental import pallas as pl
from jax.experimental.pallas import tpu as pltpu
from jax.sharding import PartitionSpec as P

VHD = 80
HD = 128
MESH = pl.DeviceIdType.MESH
NT = (((1,), (1,)), ((), ()))


class Copies:
    def __init__(self, send, recv, local):
        self.send, self.recv, self.local = send, recv, local
        self.groups, self.views, self.m, self.n = {}, {}, 0, 0
        self.sent = []

    def remote(self, src, dst, dev, group=None):
        single = group is None
        if single:
            self.n += 1
            group = self.n
        k = self.groups.setdefault(group, len(self.groups))
        c = pltpu.make_async_remote_copy(
            src_ref=src, dst_ref=dst, send_sem=self.send.at[k], recv_sem=self.recv.at[k],
            device_id=dev, device_id_type=MESH)
        c.start()
        if single:
            self.sent.append(c)
        return c

    def join(self, group, view):
        k = self.groups[group]
        self.views[k] = view
        pltpu.make_async_copy(view, view, self.recv.at[k]).wait()

    def here(self, src, dst):
        k = self.m
        self.m += 1
        c = pltpu.make_async_copy(src, dst, self.local.at[k])
        c.start()
        return c

    def drain(self):
        for c in self.sent:
            c.wait_send()
        for k, view in self.views.items():
            pltpu.make_async_copy(view, view, self.send.at[k]).wait()
        assert len(self.sent) + len(self.views) == len(self.groups)


def places():
    mp, dp = lax.axis_index("mp"), lax.axis_index("dp")
    y, x = mp // 4, lax.rem(mp, 4)
    X = lambda s: (dp, y * 4 + lax.rem(x + s + 4, 4))
    Y = lambda s: (dp, lax.rem(y + s + 4, 4) * 4 + x)
    Z = lambda s: (lax.rem(dp + 2 * s + 8, 8), mp)
    other = (dp + 1 - 2 * lax.rem(dp, 2), mp)
    return dp, y, x, X, Y, Z, other


def meet(devs):
    barrier = pltpu.get_barrier_semaphore()
    for d in devs:
        pl.semaphore_signal(barrier, inc=1, device_id=d, device_id_type=MESH)
    pl.semaphore_wait(barrier, len(devs))


N3 = 117


def vision(patches, ids, norm, qkv_w, qkv_b, out_w, gain):
    bf, f32 = jnp.bfloat16, jnp.float32
    iota = lambda shape, d: lax.broadcasted_iota(jnp.int32, shape, d)
    i, s = iota((128, 128), 0), iota((128, 128), 1)
    perm = (s == (i % 32) * 4 + i // 32).astype(f32).astype(bf)
    p = jnp.dot(perm, patches[...], preferred_element_type=f32)
    wide = jnp.broadcast_to(ids[...].astype(f32), (128, 128)).astype(bf)
    across = lax.dot_general(wide, perm, NT, preferred_element_type=f32)
    same = across == across.T
    normed = p * lax.rsqrt(jnp.mean(p * p, axis=1, keepdims=True) + 1e-6) * norm[...].reshape(1, 1280)
    qkv = (jnp.dot(normed.astype(bf), qkv_w[...], preferred_element_type=f32) + qkv_b[...].reshape(1, 1920)).astype(bf)
    tiles = [None] * 5
    for h in range(8):
        lo, hi = 80 * h // 128, (80 * h + 207) // 128
        lane = iota((128, 128 * (hi - lo)), 1) + 128 * lo
        here = (lane >= 80 * h) & (lane < 80 * h + 80)
        part = lambda k: qkv[:, 640 * k + 128 * lo:640 * k + 128 * hi]
        zero = jnp.zeros((), bf)
        sc = lax.dot_general(jnp.where(here, part(0), zero), part(1), NT, preferred_element_type=f32) * VHD ** (-0.5)
        sc = jnp.where(same, sc, -1e30)
        e = jnp.exp(sc - jnp.max(sc, axis=1, keepdims=True))
        w = (e / jnp.sum(e, axis=1, keepdims=True)).astype(bf)
        mix = jnp.dot(w, jnp.where(here, part(2), zero), preferred_element_type=f32)
        for t in range(lo, hi):
            v = mix[:, 128 * (t - lo):128 * (t - lo + 1)]
            tiles[t] = v if tiles[t] is None else tiles[t] + v
    mixed = jnp.concatenate(tiles, axis=1).astype(bf)
    r = (p + jnp.dot(mixed, out_w[...], preferred_element_type=f32)).astype(bf).astype(f32)
    return (r * lax.rsqrt(jnp.mean(r * r, axis=1, keepdims=True) + 1e-6) * gain[...].reshape(1, 1280)).astype(bf)


def whole_kernel(patches, ids, owner, slots, text, vnorm, qkv_w, qkv_b, out_w, mnorm, w1, b1, w2, b2, gain, qw, qb,
                 kvw, kvb, q_out, kv_out,
                 MS, G, QKVW, OUTW, w1v, H, HT, W2, wq, wkv, KVS, KVX, KBS, kb, INS, info, RW, RQ,
                 PC, RO, RN, T, TR, SB, R, A, SS, SY, SC, Q0, QR, QL, QO, RQO, RQN, KP, RKV, send, recv, local):
    dp, y, x, X, Y, Z, other = places()
    md = lambda v, s: lax.rem(v + s + 4, 4)
    bf, f32 = jnp.bfloat16, jnp.float32
    iota = lambda shape, d: lax.broadcasted_iota(jnp.int32, shape, d)
    e, mp = dp, y * 4 + x
    cp = Copies(send, recv, local)
    lv = [cp.here(qkv_w, QKVW), cp.here(out_w, OUTW), cp.here(w1, w1v)]
    group = [(lax.rem(dp + s, 8), mp) for s in (2, 6, 1, 3, 5, 7, 4)]
    meet([X(1), X(2), X(3), Y(1), Y(2), Y(3)] + group)
    ca, cb = pl.ds(0, 768), pl.ds(768, 512)
    sa = lambda yy, xx: G.at[:, yy, xx, :, ca]
    sb = lambda yy, xx: G.at[:, yy, xx, :, cb]
    cols = lambda xd: pl.ds(pl.multiple_of(2048 * xd + 256 * e, 256), 256)
    mine = pl.ds(pl.multiple_of(256 * e, 256), 256)
    first, second = pl.ds(0, 2), pl.ds(2, 2)

    xo = md(x, 2)
    w2_half = [pl.ds(0, 160), pl.ds(160, 160)]
    q_half = lambda v, i: pl.ds(pl.multiple_of(2048 * v + 256 * e + 128 * i, 128), 128)
    bands = lambda r: pl.ds(pl.multiple_of(256 * r, 256), 256)
    zw, zwf, dw = {}, {}, []

    def w2_start(s):
        xs = md(x, s)
        src = w2.at[:, cols(x)] if s == 0 else W2.at[xs, :, mine]
        zw[s] = {t: cp.remote(src, W2.at[xs, :, mine], Z(t)) for t in (1, -1)}
        dw.append(cp.remote(src, W2.at[xs, :, mine], other, "dw"))

    def w2_mid(s):
        xs, way = md(x, s), 1 if s in (0, 1) else -1
        for t in (1, -1):
            zw[s][t].wait_recv()
            at = W2.at[xs, :, bands(lax.rem(e - 2 * t + 8, 8))]
            if t == way:
                zwf[s] = cp.remote(at, at, Z(t))
            dw.append(cp.remote(at, at, other, "dw"))

    def w2_end(s):
        zwf[s].wait_recv()
        at = W2.at[md(x, s), :, bands(lax.rem(e + 4, 8))]
        dw.append(cp.remote(at, at, other, "dw"))

    w2r = [cp.remote(w2.at[w2_half[i], cols(xo)], RW.at[i], X(1 - 2 * i)) for i in range(2)]
    w2d = [cp.remote(w2.at[:, cols(md(x, s))], W2.at[x, :, mine], X(s)) for s in (1, -1)]
    w2_start(0)
    wl = [cp.here(w2.at[:, cols(x)], W2.at[x, :, mine]), cp.here(qw.at[cols(x), :], wq.at[x, mine, :])]

    lv[0].wait()
    lv[1].wait()
    MS[...] = vision(patches, ids, vnorm, QKVW, qkv_b, OUTW, mnorm).reshape(4, 32, 1280)

    ma, mb = MS.at[:, :, ca], MS.at[:, :, cb]
    a1 = {s: cp.remote(ma, sa(y, x), X(s)) for s in (1, -1)}
    c1 = {s: cp.remote(mb, sb(y, x), Y(s)) for s in (1, -1)}
    a2 = {(0, s): cp.remote(ma, sa(y, x), Y(s)) for s in (1, -1)}
    c2 = {(0, s): cp.remote(mb, sb(y, x), X(s)) for s in (1, -1)}
    gl = cp.here(MS, G.at[:, y, x])
    i64, s64 = iota((64, 64), 0), iota((64, 64), 1)
    order = (s64 == (i64 // 8 % 2) * 32 + (i64 % 8) * 4 + i64 // 16).astype(f32).astype(bf)
    for n in range(4):
        cs = slice(2048 * n, 2048 * (n + 1))
        v = jnp.dot(order, kvw[:, :, cs].reshape(64, 2048), preferred_element_type=f32)
        KVS[:, :, cs] = v.astype(bf).reshape(4, 16, 2048)
    li, ll = iota((128, 128), 0), iota((128, 128), 1)
    rows = []
    flat = jnp.concatenate([kvb[0:1, :], kvb[1:2, :], jnp.zeros((1, 64), f32)], axis=1)
    down = jnp.broadcast_to(flat, (128, 128)).T
    for j in range(4):
        keep = (li == (ll // 8) * 32 + (ll % 8) * 4 + j) & (ll < 16)
        rows.append(jnp.sum(jnp.where(keep, down, 0.0), axis=0, keepdims=True))
    KBS[...] = jnp.concatenate(rows + [jnp.zeros((4, 128), f32)], axis=0)
    own4 = jnp.broadcast_to(jnp.concatenate([owner[...]] * 4, axis=1), (8, 128))
    slot2 = jnp.broadcast_to(jnp.concatenate([slots[...]] * 2, axis=1), (8, 128))
    t0, t1 = iota((8, 128), 0), iota((8, 128), 1)
    INS[...] = jnp.where((t0 == 0) & (t1 // 32 == x), own4,
                         jnp.where((t0 == 1 + x // 2) & (t1 // 64 == x % 2), slot2, 0))
    KVX[x] = KVS[:, :, cols(x)]
    kb[y, x] = KBS[...]
    info[x] = INS[...]

    af, cf = {}, {}
    for s in (1, -1):
        hf = first if s == 1 else second
        a1[s].wait_recv()
        xs = md(x, -s)
        at = G.at[hf, y, xs, :, ca]
        af[s] = cp.remote(at, at, X(s))
        for t in (1, -1):
            a2[(-s, t)] = cp.remote(sa(y, xs), sa(y, xs), Y(t))
        c1[s].wait_recv()
        ys = md(y, -s)
        at = G.at[hf, ys, x, :, cb]
        cf[s] = cp.remote(at, at, Y(s))
        for t in (1, -1):
            c2[(-s, t)] = cp.remote(sb(ys, x), sb(ys, x), X(t))
    last = []

    def pass_on(p):
        for t in (1, -1):
            hf = first if t == 1 else second
            a2[(p, t)].wait_recv()
            at = G.at[hf, md(y, -t), md(x, p), :, ca]
            last.append(cp.remote(at, at, Y(t), "last"))
            c2[(p, t)].wait_recv()
            at = G.at[hf, md(y, p), md(x, -t), :, cb]
            last.append(cp.remote(at, at, X(t), "last"))

    qr = [cp.remote(qw.at[q_half(xo, i), :], RQ.at[i], X(1 - 2 * i)) for i in range(2)]
    qd = [cp.remote(qw.at[cols(md(x, s)), :], wq.at[x, mine, :], X(s), "qd") for s in (1, -1)]
    wx = []
    for t in (1, 3, 2):
        wx.append(cp.remote(KVS.at[:, :, cols(md(x, t))], KVX.at[x], X(t), "wx0"))
        wx.append(cp.remote(KBS, kb.at[y, x], X(t), "wx1"))
        wx.append(cp.remote(INS, info.at[x], X(t), "wx2"))
    for c in w2r:
        c.wait_recv()
    w2f = [cp.remote(RW.at[i], W2.at[md(x, 2 * i - 1), w2_half[i], mine], X(1 - 2 * i)) for i in range(2)]
    w2_mid(0)
    w2d[0].wait_recv()
    w2_start(-1)
    w2d[1].wait_recv()
    w2_start(1)
    pass_on(0)

    def piece(name, r, half=None):
        h = pl.ds(0, 4) if half is None else (first, second)[half]
        if name == "q":
            return wq.at[h, bands(r), :]
        return wkv.at[h, :, :, bands(r)]

    zs, ds_, zf = {}, {}, {}

    def z_start(name):
        zs[name] = {s: cp.remote(piece(name, e), piece(name, e), Z(s)) for s in (1, -1)}
        ds_[name] = [cp.remote(piece(name, e), piece(name, e), other, "d" + name)]

    def z_mid(name):
        zf[name] = {}
        for s in (1, -1):
            zs[name][s].wait_recv()
            r, h = lax.rem(e - 2 * s + 8, 8), 0 if s == 1 else 1
            zf[name][s] = cp.remote(piece(name, r, h), piece(name, r, h), Z(s))
            ds_[name].append(cp.remote(piece(name, r), piece(name, r), other, "d" + name))

    def z_end(name):
        for s in (1, -1):
            zf[name][s].wait_recv()
        r = lax.rem(e + 4, 8)
        ds_[name].append(cp.remote(piece(name, r), piece(name, r), other, "d" + name))

    def z_all(name):
        cp.join("d" + name, wq.at[:, 0:1024, :] if name == "q" else wkv.at[:, :, :, 0:1024])

    for s in (1, -1):
        af[s].wait_recv()
        cf[s].wait_recv()
    xf, yf = md(x, 2), md(y, 2)
    for t in (1, -1):
        a2[(2, t)] = cp.remote(sa(y, xf), sa(y, xf), Y(t))
        c2[(2, t)] = cp.remote(sb(yf, x), sb(yf, x), X(t))
    pass_on(-1)
    pass_on(1)
    for c in qr:
        c.wait_recv()
    qf = [cp.remote(RQ.at[i], wq.at[md(x, 2 * i - 1), pl.ds(pl.multiple_of(256 * e + 128 * i, 128), 128), :],
                    X(1 - 2 * i), "qd") for i in range(2)]
    w2_mid(-1)
    w2_mid(1)
    pass_on(2)
    for c in w2f:
        c.wait_recv()
    w2_start(2)
    cp.join("last", G.at[:, 0])
    gl.wait()
    lv[2].wait()
    wide = jnp.concatenate([b1[...].reshape(1, 320), jnp.zeros((1, 64), f32)], axis=1)
    bcol = jnp.broadcast_to(wide, (128, 384)).T[0:320, :]
    bcol = jnp.concatenate([bcol, bcol], axis=1)
    h1 = {}
    for g in range(2):
        acc = None
        for j in range(4):
            p = lax.dot_general(w1v[:, 1280 * j:1280 * (j + 1)], G[j, 2 * g:2 * g + 2].reshape(256, 1280), NT,
                                preferred_element_type=f32)
            acc = p if acc is None else acc + p
        v = acc + bcol
        v = 0.5 * v * (1.0 + lax.erf(v * (0.5 ** 0.5)))
        H[x, :, 256 * g:256 * (g + 1)] = v.astype(bf)
        hc = pl.ds(256 * g, 256)
        for s in (1, -1):
            h1[(g, s)] = cp.remote(H.at[x, :, hc], H.at[x, :, hc], X(s))
    h2 = []

    def pass_hidden(g):
        for s in (1, -1):
            h1[(g, s)].wait_recv()
            at = H.at[md(x, -s), pl.ds(0, 160) if s == 1 else pl.ds(160, 160), pl.ds(256 * g, 256)]
            h2.append(cp.remote(at, at, X(s), "h2"))

    w2_mid(2)
    cp.join("wx0", KVX.at[0:3])
    cp.join("wx1", kb.at[0, 0:3])
    cp.join("wx2", info.at[0:3])
    ky = []
    for s in (1, 2, 3):
        yd = md(y, s)
        ky.append(cp.remote(KVX.at[:, yd], wkv.at[y, :, :, mine], Y(s), "ky0"))
        ky.append(cp.remote(kb.at[y], kb.at[y], Y(s), "ky1"))
    wkv[y, :, :, mine] = KVX[:, y]
    cp.join("qd", wq.at[0, 0:768, :])
    wl[1].wait()
    z_start("q")
    pass_hidden(0)
    for s in (0, -1, 1, 2):
        w2_end(s)
    pass_hidden(1)
    quarter = lambda v: pl.ds(pl.multiple_of(2048 * v, 2048), 2048)
    th = [pl.ds(0, 32), pl.ds(32, 32)]
    tr = [cp.remote(text.at[th[i], quarter(xo)], TR.at[i], X(1 - 2 * i), "tr") for i in range(2)]
    td = [cp.remote(text.at[:, quarter(md(x, s))], T.at[x], X(s), "td") for s in (1, -1)]
    tl = cp.here(text.at[:, quarter(x)], T.at[x])
    tab = info[0] + info[1] + info[2] + info[3]
    own = tab[0:1, :]
    down = jnp.broadcast_to(own.astype(f32), (128, 128)).T.astype(jnp.int32)
    before = (down == own) & (li < ll) & (li // 32 == ll // 32)
    rank = jnp.sum(before.astype(jnp.int32), axis=0, keepdims=True)
    target = own * 32 + (iota((1, 128), 1) // 32) * 8 + rank
    pick = (iota((256, 128), 0) == target).astype(f32).astype(bf)
    choose = []
    for i in range(2):
        s = jnp.broadcast_to(tab[1 + i:2 + i, :].astype(f32), (128, 128)).T.astype(jnp.int32)
        s = jnp.concatenate([s, s], axis=1)
        lane, row = iota((128, 256), 1), iota((128, 256), 0)
        hit = ((lane // 32) * 8 + lane % 8 == s) & ((lane % 32) // 8 == row // 64 + 2 * i)
        choose.append(hit.astype(f32).astype(bf))
    cp.join("ky0", KVX.at[0:3])
    cp.join("ky1", kb.at[0:3])
    z_start("kv")
    wl[0].wait()
    cp.join("dw", W2.at[:, :, 0:1024])
    cp.join("h2", H.at[0])
    HT[...] = H[...].reshape(1280, 512).T

    lo, hi = pl.ds(0, 64), pl.ds(64, 64)
    yr, yl = md(y, 1), md(y, -1)
    ro, rn, hand, handl = {}, {}, {}, {}

    def mul(c):
        cs = slice(512 * c, 512 * (c + 1))
        v = jnp.dot(HT[...], W2[:, :, cs].reshape(1280, 512), preferred_element_type=f32)
        PC[c] = v.astype(bf).reshape(4, 128, 512)
        ro[c] = [cp.remote(PC.at[c, md(y, 2), lo], RO.at[c, 0], Y(1), ("ro", c)),
                 cp.remote(PC.at[c, md(y, 2), hi], RO.at[c, 1], Y(-1), ("ro", c))]
        rn[c] = [cp.remote(PC.at[c, yr, hi], RN.at[c, 0, hi], Y(1), ("rn", c)),
                 cp.remote(PC.at[c, yl, lo], RN.at[c, 1, lo], Y(-1), ("rn", c))]

    def relay_y(c):
        cp.join(("ro", c), RO.at[c])
        PC[c, yr, 0:64, :] = (PC[c, yr, 0:64, :].astype(f32) + RO[c, 0].astype(f32)).astype(bf)
        rn[c].append(cp.remote(PC.at[c, yr, lo], RN.at[c, 0, lo], Y(1), ("rn", c)))
        PC[c, yl, 64:128, :] = (PC[c, yl, 64:128, :].astype(f32) + RO[c, 1].astype(f32)).astype(bf)
        rn[c].append(cp.remote(PC.at[c, yl, hi], RN.at[c, 1, hi], Y(-1), ("rn", c)))

    def give(c):
        cp.join(("rn", c), RN.at[c])
        v = PC[c, y].astype(f32) + RN[c, 0].astype(f32) + RN[c, 1].astype(f32)
        v = (v + b2[:, pl.ds(pl.multiple_of(2048 * x + 512 * c, 512), 512)]).astype(bf)
        SB[c, :, :, 0:512] = jnp.dot(pick, v, preferred_element_type=f32).astype(bf).reshape(8, 32, 512)
        w = pl.ds(0, 512)
        if c == 0:
            v = jnp.dot(pick, jnp.ones((128, 128), bf), preferred_element_type=f32)
            SB[c, :, :, 512:640] = v.astype(bf).reshape(8, 32, 128)
            w = pl.ds(0, 640)
        hand[c] = [cp.remote(SB.at[c, d[0], :, w], R.at[c, dp, :, w], d, ("hand", c)) for d in group]
        handl[c] = cp.here(SB.at[c, dp, :, w], R.at[c, dp, :, w])

    h = [pl.ds(0, 128), pl.ds(128, 128)]
    gx = gain[:, quarter(x)]
    filled, sq, yc = [None, None], [None, None], {1: [], -1: []}

    def take(c):
        cs = slice(512 * c, 512 * (c + 1))
        cp.join(("hand", c), R.at[c, 0:7, :, pl.ds(0, 640 if c == 0 else 512)])
        handl[c].wait()
        for i in range(2):
            if c == 0:
                seen = jnp.dot(choose[i], R[0, :, :, 512:640].reshape(256, 128), preferred_element_type=f32)
                filled[i] = seen[:, 0:1] > 0.5
            v = jnp.dot(choose[i], R[c, :, :, 0:512].reshape(256, 512), preferred_element_type=f32)
            v = jnp.where(filled[i], v, T[2 * i:2 * i + 2, :, cs].reshape(128, 512).astype(f32))
            t = jnp.sum(v * v, axis=1, keepdims=True)
            sq[i] = t if c == 0 else sq[i] + t
            A[y, 128 * i:128 * (i + 1), cs] = (v * gx[:, cs]).astype(bf)
            w, s = pl.ds(512 * c, 512), 1 - 2 * i
            yc[s].append(cp.remote(A.at[y, h[i], w], A.at[y, h[i], w], Y(s), ("yc", s)))

    mul(0)
    mul(1)
    mul(2)
    relay_y(0)
    mul(3)
    relay_y(1)
    z_mid("q")
    give(0)
    cp.join("tr", TR)
    tf = [cp.remote(TR.at[i], T.at[md(x, 2 * i - 1), th[i]], X(1 - 2 * i), "td") for i in range(2)]
    relay_y(2)
    give(1)
    relay_y(3)
    z_mid("kv")
    give(2)
    cp.join("td", T.at[0:3])
    tl.wait()
    give(3)
    z_end("q")
    z_end("kv")
    take(0)
    take(1)
    take(2)
    take(3)
    SS[x] = jnp.concatenate([jnp.broadcast_to(t, (128, 128)).T[0:8, :] for t in sq], axis=1)
    sx = [cp.remote(SS.at[x], SS.at[x], X(s), "sx") for s in (1, 2, 3)]
    z_all("q")
    z_all("kv")

    tag = [0]

    def pair(ga, oa, gb, ob, size):
        tag[0] += 1
        a = jnp.concatenate([A[ga, oa:oa + size, :], A[gb, ob:ob + size, :]], axis=0)
        us = []
        for g, o in ((ga, oa), (gb, ob)):
            at = lambda off, n, g=g, o=o: pl.ds(pl.multiple_of(256 * g + o + off, n), n)
            us.append(dict(tag=tag[0], size=size, rows=at(0, size), lo=at(0, size // 2), hi=at(size // 2, size // 2),
                           share=lambda v, g=g, o=o: pl.ds(
                               pl.multiple_of(256 * g + o + size // 4 * v, size // 4), size // 4),
                           slot=pl.ds(pl.multiple_of(64 * g + o // 4, size // 4), size // 4)))
        prod = lambda s: jnp.dot(a, wq[md(x, s)], preferred_element_type=f32)

        def put(ref, v):
            v = v.astype(ref.dtype)
            for n, u in enumerate(us):
                ref[u["rows"], :] = v[size * n:size * (n + 1)]

        put(QO, prod(2))
        for u in us:
            u["o"] = [cp.remote(QO.at[u["lo"]], RQO.at[0, u["lo"]], X(1), ("o", u["tag"])),
                      cp.remote(QO.at[u["hi"]], RQO.at[1, u["hi"]], X(-1), ("o", u["tag"]))]
        put(KP, lax.dot_general(a, wkv[...].reshape(256, 2048), NT, preferred_element_type=f32))
        for u in us:
            u["k"] = []
            for s in (2, 1, 3):
                u["k"].append(cp.remote(KP.at[u["share"](md(x, s))], RKV.at[x, u["slot"]], X(s), ("k", u["tag"])))
        put(QR, prod(1))
        for u in us:
            u["n"] = [cp.remote(QR.at[u["hi"]], RQN.at[0, u["hi"]], X(1), ("n", u["tag"]))]
        put(QL, prod(-1))
        for u in us:
            u["n"].append(cp.remote(QL.at[u["lo"]], RQN.at[1, u["lo"]], X(-1), ("n", u["tag"])))
        put(Q0, prod(0))
        return us

    def relay(us):
        cp.join(("o", us[0]["tag"]), RQO.at[0, 0:2 * us[0]["size"]])
        for u in us:
            lo, hi = u["lo"], u["hi"]
            QR[lo, :] = (QR[lo, :].astype(f32) + RQO[0, lo, :].astype(f32)).astype(bf)
            u["n"].append(cp.remote(QR.at[lo], RQN.at[0, lo], X(1), ("n", u["tag"])))
            QL[hi, :] = (QL[hi, :].astype(f32) + RQO[1, hi, :].astype(f32)).astype(bf)
            u["n"].append(cp.remote(QL.at[hi], RQN.at[1, hi], X(-1), ("n", u["tag"])))

    bias = jnp.concatenate([kb[p // 4, p % 4, pl.ds(y, 1), 0:16] for p in range(16)], axis=1)

    def keys(us):
        cp.join(("k", us[0]["tag"]), KP.at[0:3 * us[0]["size"] // 2])
        for u in us:
            m = u["share"](x)
            v = KP[m, :].astype(f32)
            for s in (1, 2, 3):
                v = v + RKV[md(x, s), u["slot"]].astype(f32)
            sc = SC[m, :]
            v = v * jnp.concatenate([sc, sc], axis=1) + bias
            kv_out[m, :] = v.astype(bf)
            u["f"] = [cp.remote(kv_out.at[m], kv_out.at[m], X(s), ("f", u["tag"])) for s in (2, 1, 3)]

    def scale(g):
        v = lax.rsqrt(SY[g] * (1.0 / 8192.0) + 1e-6)
        for i in range(2):
            SC[pl.ds(pl.multiple_of(256 * g + 128 * i, 128), 128), :] = jnp.broadcast_to(
                v[0:1, 128 * i:128 * (i + 1)], (128, 128)).T

    def finish(us):
        cp.join(("n", us[0]["tag"]), RQN.at[0, 0:4 * us[0]["size"]])
        for u in us:
            rows = u["rows"]
            sc = SC[rows, :]
            v = Q0[rows, :] + RQN[0, rows, :].astype(f32) + RQN[1, rows, :].astype(f32)
            q_out[rows, :] = (v * jnp.concatenate([sc, sc], axis=1) + qb[...]).astype(bf)
        cp.join(("f", us[0]["tag"]), KP.at[0:3 * us[0]["size"] // 2])

    u0 = pair(y, 0, y, 128, 128)
    cp.join("sx", SS.at[0:3])
    SY[y] = SS[0] + SS[1] + SS[2] + SS[3]
    sy = [cp.remote(SY.at[y], SY.at[y], Y(s), "sy") for s in (1, 2, 3)]
    band = lambda o: pl.ds(o, 64)
    yo = {1: [cp.remote(A.at[y, band(o)], A.at[y, band(o)], Y(1)) for o in (128, 192)],
          -1: [cp.remote(A.at[y, band(o)], A.at[y, band(o)], Y(-1)) for o in (0, 64)]}
    scale(y)
    relay(u0)
    up, dn, op = yr, yl, md(y, 2)
    far = {}
    cp.join(("yc", 1), A.at[0, h[0]])
    far[1] = [cp.remote(A.at[dn, band(o)], A.at[dn, band(o)], Y(1)) for o in (0, 64)]
    cp.join(("yc", -1), A.at[0, h[0]])
    far[-1] = [cp.remote(A.at[up, band(o)], A.at[up, band(o)], Y(-1)) for o in (128, 192)]
    keys(u0)
    u1 = pair(dn, 0, up, 128, 128)
    finish(u0)
    relay(u1)
    yo[1][0].wait_recv()
    yo[-1][0].wait_recv()
    cp.join("sy", SY.at[0:3])
    for g in (dn, up, op):
        scale(g)
    u2 = pair(dn, 128, up, 0, 64)
    keys(u1)
    relay(u2)
    yo[1][1].wait_recv()
    yo[-1][1].wait_recv()
    u3 = pair(dn, 192, up, 64, 64)
    keys(u2)
    finish(u1)
    relay(u3)
    far[1][0].wait_recv()
    far[-1][0].wait_recv()
    u4 = pair(op, 0, op, 128, 64)
    keys(u3)
    finish(u2)
    relay(u4)
    far[1][1].wait_recv()
    far[-1][1].wait_recv()
    u5 = pair(op, 64, op, 192, 64)
    keys(u4)
    finish(u3)
    relay(u5)
    keys(u5)
    finish(u4)
    finish(u5)
    cp.drain()
    assert len(cp.groups) == N3, len(cp.groups)


def whole(patches, ids, owner, slots, text, vnorm, qkv_w, qkv_b, out_w, mnorm, w1, b1, w2, b2, gain, qw, qb, kvw, kvb):
    bf, f32, i32 = jnp.bfloat16, jnp.float32, jnp.int32
    V, ANY = pl.BlockSpec(memory_space=pltpu.VMEM), pl.BlockSpec(memory_space=pl.ANY)
    S = jax.ShapeDtypeStruct
    M = pltpu.VMEM
    return pl.pallas_call(
        whole_kernel,
        out_shape=(S((1024, 256), bf), S((1024, 256), bf)),
        in_specs=[V, V, V, V, ANY, V, ANY, V, ANY, V, ANY, V, ANY, V, V, ANY, V, V, V],
        out_specs=[V] * 2,
        scratch_shapes=[
            M((4, 32, 1280), bf),
            M((4, 4, 4, 32, 1280), bf),
            M((1280, 1920), bf),
            M((640, 1280), bf),
            M((320, 5120), bf),
            M((4, 320, 512), bf),
            M((512, 1280), bf),
            M((4, 320, 2048), bf),
            M((4, 2048, 256), bf),
            M((4, 4, 16, 2048), bf),
            M((4, 16, 8192), bf),
            M((4, 4, 16, 256), bf),
            M((8, 128), f32),
            M((4, 4, 8, 128), f32),
            M((8, 128), i32),
            M((4, 8, 128), i32),
            M((2, 160, 256), bf),
            M((2, 128, 256), bf),
            M((4, 4, 128, 512), bf),
            M((4, 2, 64, 512), bf),
            M((4, 2, 128, 512), bf),
            M((4, 64, 2048), bf),
            M((2, 32, 2048), bf),
            M((4, 8, 32, 640), bf),
            M((4, 8, 32, 640), bf),
            M((4, 256, 2048), bf),
            M((4, 8, 256), f32),
            M((4, 8, 256), f32),
            M((1024, 128), f32),
            M((1024, 256), f32),
            M((1024, 256), bf),
            M((1024, 256), bf),
            M((1024, 256), bf),
            M((2, 1024, 256), bf),
            M((2, 1024, 256), bf),
            M((1024, 256), bf),
            M((4, 256, 256), bf),
            pltpu.SemaphoreType.DMA((N3,)),
            pltpu.SemaphoreType.DMA((N3,)),
            pltpu.SemaphoreType.DMA((16,)),
        ],
        compiler_params=pltpu.CompilerParams(collective_id=1, has_side_effects=True, vmem_limit_bytes=64000000),
        name="whole",
    )(patches, ids, owner, slots, text, vnorm, qkv_w, qkv_b, out_w, mnorm, w1, b1, w2, b2, gain, qw, qb, kvw, kvb)


def attention_kernel(q, kv, out):
    bf, f32 = jnp.bfloat16, jnp.float32
    c, d = lax.broadcasted_iota(jnp.int32, (256, 128), 0), lax.broadcasted_iota(jnp.int32, (256, 128), 1)
    spot = (d // 8) * 16 + d % 8
    keys = jnp.dot(kv[...], (c == spot).astype(f32).astype(bf), preferred_element_type=f32).astype(bf)
    values = jnp.dot(kv[...], (c == spot + 8).astype(f32).astype(bf), preferred_element_type=f32).astype(bf)
    low = lax.broadcasted_iota(jnp.int32, (256, 256), 0) >= lax.broadcasted_iota(jnp.int32, (256, 256), 1)
    k = HD ** (-0.5) * 1.4426950408889634
    for i in range(4):
        rows = slice(256 * i, 256 * (i + 1))
        for h in range(2):
            hs = slice(128 * h, 128 * (h + 1))
            s = lax.dot_general(q[rows, hs], keys[rows], NT, preferred_element_type=f32)
            s = jnp.where(low, s, -1e30)
            top = jnp.max(s, axis=1, keepdims=True)
            if i:
                before = lax.dot_general(q[rows, hs], keys[:256 * i], NT, preferred_element_type=f32)
                top = jnp.maximum(top, jnp.max(before, axis=1, keepdims=True))
            p = jnp.exp2((s - top) * k)
            total = jnp.sum(p, axis=1, keepdims=True)
            m = jnp.dot(p.astype(bf), values[rows], preferred_element_type=f32)
            if i:
                p = jnp.exp2((before - top) * k)
                total = total + jnp.sum(p, axis=1, keepdims=True)
                m = m + jnp.dot(p.astype(bf), values[:256 * i], preferred_element_type=f32)
            out[rows, hs] = (m / total).astype(bf)


def attention(q, kv):
    V = pl.BlockSpec(memory_space=pltpu.VMEM)
    return pl.pallas_call(
        attention_kernel,
        out_shape=jax.ShapeDtypeStruct((1024, 256), jnp.bfloat16),
        in_specs=[V, V],
        out_specs=V,
        compiler_params=pltpu.CompilerParams(vmem_limit_bytes=60000000),
        name="attention",
    )(q, kv)


def shards(
    patches,
    window_ids,
    owner,
    slot_of_row,
    text_embeds,
    vit_norm,
    vit_qkv_w,
    vit_qkv_b,
    vit_out_w,
    merge_norm,
    merge_w1,
    merge_b1,
    merge_w2,
    merge_b2,
    llm_norm,
    q_w,
    q_b,
    kv_w,
    kv_b,
):
    q, kv = whole(
        patches, window_ids, owner.reshape(1, 32), slot_of_row, text_embeds, vit_norm, vit_qkv_w,
        vit_qkv_b, vit_out_w, merge_norm, merge_w1.T, merge_b1, merge_w2, merge_b2[None],
        llm_norm[None], q_w, q_b[None], kv_w.transpose(0, 2, 1), kv_b,
    )
    return attention(q, kv)


def solution(mesh):
    return jax.shard_map(
        shards,
        mesh=mesh,
        in_specs=(
            P(("dp", "mp"), None),
            P(("dp", "mp"), None),
            P(("dp", "mp"), None),
            P(("dp", "mp"), None),
            P(("dp", "mp"), None),
            P(),
            P(),
            P(),
            P(),
            P(),
            P(None, "mp"),
            P("mp"),
            P("mp", None),
            P(),
            P(),
            P(None, "mp"),
            P("mp"),
            P(None, None, "mp"),
            P(None, "mp"),
        ),
        out_specs=P("dp", "mp"),
        check_vma=False,
    )
```

```python
import jax
import jax.numpy as jnp
from jax import lax
from jax.experimental import pallas as pl
from jax.experimental.pallas import tpu as pltpu
from jax.sharding import PartitionSpec as P

VHD = 80
HD = 128
MESH = pl.DeviceIdType.MESH
NT = (((1,), (1,)), ((), ()))


class Copies:
    def __init__(self, send, recv, local):
        self.send, self.recv, self.local = send, recv, local
        self.groups, self.views, self.m, self.n = {}, {}, 0, 0
        self.sent = []

    def remote(self, src, dst, dev, group=None):
        single = group is None
        if single:
            self.n += 1
            group = self.n
        k = self.groups.setdefault(group, len(self.groups))
        c = pltpu.make_async_remote_copy(
            src_ref=src, dst_ref=dst, send_sem=self.send.at[k], recv_sem=self.recv.at[k],
            device_id=dev, device_id_type=MESH)
        c.start()
        if single:
            self.sent.append(c)
        return c

    def join(self, group, view):
        k = self.groups[group]
        self.views[k] = view
        pltpu.make_async_copy(view, view, self.recv.at[k]).wait()

    def here(self, src, dst):
        k = self.m
        self.m += 1
        c = pltpu.make_async_copy(src, dst, self.local.at[k])
        c.start()
        return c

    def drain(self):
        for c in self.sent:
            c.wait_send()
        for k, view in self.views.items():
            pltpu.make_async_copy(view, view, self.send.at[k]).wait()
        assert len(self.sent) + len(self.views) == len(self.groups)


def places():
    mp, dp = lax.axis_index("mp"), lax.axis_index("dp")
    y, x = mp // 4, lax.rem(mp, 4)
    X = lambda s: (dp, y * 4 + lax.rem(x + s + 4, 4))
    Y = lambda s: (dp, lax.rem(y + s + 4, 4) * 4 + x)
    Z = lambda s: (lax.rem(dp + 2 * s + 8, 8), mp)
    other = (dp + 1 - 2 * lax.rem(dp, 2), mp)
    return dp, y, x, X, Y, Z, other


def meet(devs):
    barrier = pltpu.get_barrier_semaphore()
    for d in devs:
        pl.semaphore_signal(barrier, inc=1, device_id=d, device_id_type=MESH)
    pl.semaphore_wait(barrier, len(devs))


N3 = 117


def vision(patches, ids, norm, qkv_w, qkv_b, out_w, gain):
    bf, f32 = jnp.bfloat16, jnp.float32
    iota = lambda shape, d: lax.broadcasted_iota(jnp.int32, shape, d)
    i, s = iota((128, 128), 0), iota((128, 128), 1)
    perm = (s == (i % 32) * 4 + i // 32).astype(f32).astype(bf)
    p = jnp.dot(perm, patches[...], preferred_element_type=f32)
    wide = jnp.broadcast_to(ids[...].astype(f32), (128, 128)).astype(bf)
    across = lax.dot_general(wide, perm, NT, preferred_element_type=f32)
    same = across == across.T
    normed = p * lax.rsqrt(jnp.mean(p * p, axis=1, keepdims=True) + 1e-6) * norm[...].reshape(1, 1280)
    qkv = (jnp.dot(normed.astype(bf), qkv_w[...], preferred_element_type=f32) + qkv_b[...].reshape(1, 1920)).astype(bf)
    tiles = [None] * 5
    for h in range(8):
        lo, hi = 80 * h // 128, (80 * h + 207) // 128
        lane = iota((128, 128 * (hi - lo)), 1) + 128 * lo
        here = (lane >= 80 * h) & (lane < 80 * h + 80)
        part = lambda k: qkv[:, 640 * k + 128 * lo:640 * k + 128 * hi]
        zero = jnp.zeros((), bf)
        sc = lax.dot_general(jnp.where(here, part(0), zero), part(1), NT, preferred_element_type=f32) * VHD ** (-0.5)
        sc = jnp.where(same, sc, -1e30)
        e = jnp.exp(sc - jnp.max(sc, axis=1, keepdims=True))
        w = (e / jnp.sum(e, axis=1, keepdims=True)).astype(bf)
        mix = jnp.dot(w, jnp.where(here, part(2), zero), preferred_element_type=f32)
        for t in range(lo, hi):
            v = mix[:, 128 * (t - lo):128 * (t - lo + 1)]
            tiles[t] = v if tiles[t] is None else tiles[t] + v
    mixed = jnp.concatenate(tiles, axis=1).astype(bf)
    r = (p + jnp.dot(mixed, out_w[...], preferred_element_type=f32)).astype(bf).astype(f32)
    return (r * lax.rsqrt(jnp.mean(r * r, axis=1, keepdims=True) + 1e-6) * gain[...].reshape(1, 1280)).astype(bf)


def whole_kernel(patches, ids, owner, slots, text, vnorm, qkv_w, qkv_b, out_w, mnorm, w1, b1, w2, b2, gain, qw, qb,
                 kvw, kvb, q_out, kv_out,
                 MS, G, QKVW, OUTW, w1v, H, HT, W2, wq, wkv, KVS, KVX, KBS, kb, INS, info, RW, RQ,
                 PC, RO, RN, T, TR, SB, R, A, SS, SY, SC, Q0, QR, QL, QO, RQO, RQN, KP, RKV, send, recv, local):
    dp, y, x, X, Y, Z, other = places()
    md = lambda v, s: lax.rem(v + s + 4, 4)
    bf, f32 = jnp.bfloat16, jnp.float32
    iota = lambda shape, d: lax.broadcasted_iota(jnp.int32, shape, d)
    e, mp = dp, y * 4 + x
    cp = Copies(send, recv, local)
    lv = [cp.here(qkv_w, QKVW), cp.here(out_w, OUTW), cp.here(w1, w1v)]
    group = [(lax.rem(dp + s, 8), mp) for s in (2, 6, 1, 3, 5, 7, 4)]
    meet([X(1), X(2), X(3), Y(1), Y(2), Y(3)] + group)
    ca, cb = pl.ds(0, 768), pl.ds(768, 512)
    sa = lambda yy, xx: G.at[:, yy, xx, :, ca]
    sb = lambda yy, xx: G.at[:, yy, xx, :, cb]
    cols = lambda xd: pl.ds(pl.multiple_of(2048 * xd + 256 * e, 256), 256)
    mine = pl.ds(pl.multiple_of(256 * e, 256), 256)
    first, second = pl.ds(0, 2), pl.ds(2, 2)

    xo = md(x, 2)
    w2_half = [pl.ds(0, 160), pl.ds(160, 160)]
    q_half = lambda v, i: pl.ds(pl.multiple_of(2048 * v + 256 * e + 128 * i, 128), 128)
    bands = lambda r: pl.ds(pl.multiple_of(256 * r, 256), 256)
    zw, zwf, dw = {}, {}, []

    def w2_start(s):
        xs = md(x, s)
        src = w2.at[:, cols(x)] if s == 0 else W2.at[xs, :, mine]
        zw[s] = {t: cp.remote(src, W2.at[xs, :, mine], Z(t)) for t in (1, -1)}
        dw.append(cp.remote(src, W2.at[xs, :, mine], other, "dw"))

    def w2_mid(s):
        xs, way = md(x, s), 1 if s in (0, 1) else -1
        for t in (1, -1):
            zw[s][t].wait_recv()
            at = W2.at[xs, :, bands(lax.rem(e - 2 * t + 8, 8))]
            if t == way:
                zwf[s] = cp.remote(at, at, Z(t))
            dw.append(cp.remote(at, at, other, "dw"))

    def w2_end(s):
        zwf[s].wait_recv()
        at = W2.at[md(x, s), :, bands(lax.rem(e + 4, 8))]
        dw.append(cp.remote(at, at, other, "dw"))

    w2r = [cp.remote(w2.at[w2_half[i], cols(xo)], RW.at[i], X(1 - 2 * i)) for i in range(2)]
    w2d = [cp.remote(w2.at[:, cols(md(x, s))], W2.at[x, :, mine], X(s)) for s in (1, -1)]
    w2_start(0)
    wl = [cp.here(w2.at[:, cols(x)], W2.at[x, :, mine]), cp.here(qw.at[cols(x), :], wq.at[x, mine, :])]

    lv[0].wait()
    lv[1].wait()
    MS[...] = vision(patches, ids, vnorm, QKVW, qkv_b, OUTW, mnorm).reshape(4, 32, 1280)

    ma, mb = MS.at[:, :, ca], MS.at[:, :, cb]
    a1 = {s: cp.remote(ma, sa(y, x), X(s)) for s in (1, -1)}
    c1 = {s: cp.remote(mb, sb(y, x), Y(s)) for s in (1, -1)}
    a2 = {(0, s): cp.remote(ma, sa(y, x), Y(s)) for s in (1, -1)}
    c2 = {(0, s): cp.remote(mb, sb(y, x), X(s)) for s in (1, -1)}
    gl = cp.here(MS, G.at[:, y, x])
    i64, s64 = iota((64, 64), 0), iota((64, 64), 1)
    order = (s64 == (i64 // 8 % 2) * 32 + (i64 % 8) * 4 + i64 // 16).astype(f32).astype(bf)
    for n in range(4):
        cs = slice(2048 * n, 2048 * (n + 1))
        v = jnp.dot(order, kvw[:, :, cs].reshape(64, 2048), preferred_element_type=f32)
        KVS[:, :, cs] = v.astype(bf).reshape(4, 16, 2048)
    li, ll = iota((128, 128), 0), iota((128, 128), 1)
    rows = []
    flat = jnp.concatenate([kvb[0:1, :], kvb[1:2, :], jnp.zeros((1, 64), f32)], axis=1)
    down = jnp.broadcast_to(flat, (128, 128)).T
    for j in range(4):
        keep = (li == (ll // 8) * 32 + (ll % 8) * 4 + j) & (ll < 16)
        rows.append(jnp.sum(jnp.where(keep, down, 0.0), axis=0, keepdims=True))
    KBS[...] = jnp.concatenate(rows + [jnp.zeros((4, 128), f32)], axis=0)
    own4 = jnp.broadcast_to(jnp.concatenate([owner[...]] * 4, axis=1), (8, 128))
    slot2 = jnp.broadcast_to(jnp.concatenate([slots[...]] * 2, axis=1), (8, 128))
    t0, t1 = iota((8, 128), 0), iota((8, 128), 1)
    INS[...] = jnp.where((t0 == 0) & (t1 // 32 == x), own4,
                         jnp.where((t0 == 1 + x // 2) & (t1 // 64 == x % 2), slot2, 0))
    KVX[x] = KVS[:, :, cols(x)]
    kb[y, x] = KBS[...]
    info[x] = INS[...]

    af, cf = {}, {}
    for s in (1, -1):
        hf = first if s == 1 else second
        a1[s].wait_recv()
        xs = md(x, -s)
        at = G.at[hf, y, xs, :, ca]
        af[s] = cp.remote(at, at, X(s))
        for t in (1, -1):
            a2[(-s, t)] = cp.remote(sa(y, xs), sa(y, xs), Y(t))
        c1[s].wait_recv()
        ys = md(y, -s)
        at = G.at[hf, ys, x, :, cb]
        cf[s] = cp.remote(at, at, Y(s))
        for t in (1, -1):
            c2[(-s, t)] = cp.remote(sb(ys, x), sb(ys, x), X(t))
    last = []

    def pass_on(p):
        for t in (1, -1):
            hf = first if t == 1 else second
            a2[(p, t)].wait_recv()
            at = G.at[hf, md(y, -t), md(x, p), :, ca]
            last.append(cp.remote(at, at, Y(t), "last"))
            c2[(p, t)].wait_recv()
            at = G.at[hf, md(y, p), md(x, -t), :, cb]
            last.append(cp.remote(at, at, X(t), "last"))

    qr = [cp.remote(qw.at[q_half(xo, i), :], RQ.at[i], X(1 - 2 * i)) for i in range(2)]
    qd = [cp.remote(qw.at[cols(md(x, s)), :], wq.at[x, mine, :], X(s), "qd") for s in (1, -1)]
    wx = []
    for t in (1, 3, 2):
        wx.append(cp.remote(KVS.at[:, :, cols(md(x, t))], KVX.at[x], X(t), "wx0"))
        wx.append(cp.remote(KBS, kb.at[y, x], X(t), "wx1"))
        wx.append(cp.remote(INS, info.at[x], X(t), "wx2"))
    for c in w2r:
        c.wait_recv()
    w2f = [cp.remote(RW.at[i], W2.at[md(x, 2 * i - 1), w2_half[i], mine], X(1 - 2 * i)) for i in range(2)]
    w2_mid(0)
    w2d[0].wait_recv()
    w2_start(-1)
    w2d[1].wait_recv()
    w2_start(1)
    pass_on(0)

    def piece(name, r, half=None):
        h = pl.ds(0, 4) if half is None else (first, second)[half]
        if name == "q":
            return wq.at[h, bands(r), :]
        return wkv.at[h, :, :, bands(r)]

    zs, ds_, zf = {}, {}, {}

    def z_start(name):
        zs[name] = {s: cp.remote(piece(name, e), piece(name, e), Z(s)) for s in (1, -1)}
        ds_[name] = [cp.remote(piece(name, e), piece(name, e), other, "d" + name)]

    def z_mid(name):
        zf[name] = {}
        for s in (1, -1):
            zs[name][s].wait_recv()
            r, h = lax.rem(e - 2 * s + 8, 8), 0 if s == 1 else 1
            zf[name][s] = cp.remote(piece(name, r, h), piece(name, r, h), Z(s))
            ds_[name].append(cp.remote(piece(name, r), piece(name, r), other, "d" + name))

    def z_end(name):
        for s in (1, -1):
            zf[name][s].wait_recv()
        r = lax.rem(e + 4, 8)
        ds_[name].append(cp.remote(piece(name, r), piece(name, r), other, "d" + name))

    def z_all(name):
        cp.join("d" + name, wq.at[:, 0:1024, :] if name == "q" else wkv.at[:, :, :, 0:1024])

    for s in (1, -1):
        af[s].wait_recv()
        cf[s].wait_recv()
    xf, yf = md(x, 2), md(y, 2)
    for t in (1, -1):
        a2[(2, t)] = cp.remote(sa(y, xf), sa(y, xf), Y(t))
        c2[(2, t)] = cp.remote(sb(yf, x), sb(yf, x), X(t))
    pass_on(-1)
    pass_on(1)
    for c in qr:
        c.wait_recv()
    qf = [cp.remote(RQ.at[i], wq.at[md(x, 2 * i - 1), pl.ds(pl.multiple_of(256 * e + 128 * i, 128), 128), :],
                    X(1 - 2 * i), "qd") for i in range(2)]
    w2_mid(-1)
    w2_mid(1)
    pass_on(2)
    for c in w2f:
        c.wait_recv()
    w2_start(2)
    cp.join("last", G.at[:, 0])
    gl.wait()
    lv[2].wait()
    wide = jnp.concatenate([b1[...].reshape(1, 320), jnp.zeros((1, 64), f32)], axis=1)
    bcol = jnp.broadcast_to(wide, (128, 384)).T[0:320, :]
    bcol = jnp.concatenate([bcol, bcol], axis=1)
    h1 = {}
    for g in range(2):
        acc = None
        for j in range(4):
            p = lax.dot_general(w1v[:, 1280 * j:1280 * (j + 1)], G[j, 2 * g:2 * g + 2].reshape(256, 1280), NT,
                                preferred_element_type=f32)
            acc = p if acc is None else acc + p
        v = acc + bcol
        v = 0.5 * v * (1.0 + lax.erf(v * (0.5 ** 0.5)))
        H[x, :, 256 * g:256 * (g + 1)] = v.astype(bf)
        hc = pl.ds(256 * g, 256)
        for s in (1, -1):
            h1[(g, s)] = cp.remote(H.at[x, :, hc], H.at[x, :, hc], X(s))
    h2 = []

    def pass_hidden(g):
        for s in (1, -1):
            h1[(g, s)].wait_recv()
            at = H.at[md(x, -s), pl.ds(0, 160) if s == 1 else pl.ds(160, 160), pl.ds(256 * g, 256)]
            h2.append(cp.remote(at, at, X(s), "h2"))

    w2_mid(2)
    cp.join("wx0", KVX.at[0:3])
    cp.join("wx1", kb.at[0, 0:3])
    cp.join("wx2", info.at[0:3])
    ky = []
    for s in (1, 2, 3):
        yd = md(y, s)
        ky.append(cp.remote(KVX.at[:, yd], wkv.at[y, :, :, mine], Y(s), "ky0"))
        ky.append(cp.remote(kb.at[y], kb.at[y], Y(s), "ky1"))
    wkv[y, :, :, mine] = KVX[:, y]
    cp.join("qd", wq.at[0, 0:768, :])
    wl[1].wait()
    z_start("q")
    pass_hidden(0)
    for s in (0, -1, 1, 2):
        w2_end(s)
    pass_hidden(1)
    quarter = lambda v: pl.ds(pl.multiple_of(2048 * v, 2048), 2048)
    th = [pl.ds(0, 32), pl.ds(32, 32)]
    tr = [cp.remote(text.at[th[i], quarter(xo)], TR.at[i], X(1 - 2 * i), "tr") for i in range(2)]
    td = [cp.remote(text.at[:, quarter(md(x, s))], T.at[x], X(s), "td") for s in (1, -1)]
    tl = cp.here(text.at[:, quarter(x)], T.at[x])
    tab = info[0] + info[1] + info[2] + info[3]
    own = tab[0:1, :]
    down = jnp.broadcast_to(own.astype(f32), (128, 128)).T.astype(jnp.int32)
    before = (down == own) & (li < ll) & (li // 32 == ll // 32)
    rank = jnp.sum(before.astype(jnp.int32), axis=0, keepdims=True)
    target = own * 32 + (iota((1, 128), 1) // 32) * 8 + rank
    pick = (iota((256, 128), 0) == target).astype(f32).astype(bf)
    choose = []
    for i in range(2):
        s = jnp.broadcast_to(tab[1 + i:2 + i, :].astype(f32), (128, 128)).T.astype(jnp.int32)
        s = jnp.concatenate([s, s], axis=1)
        lane, row = iota((128, 256), 1), iota((128, 256), 0)
        hit = ((lane // 32) * 8 + lane % 8 == s) & ((lane % 32) // 8 == row // 64 + 2 * i)
        choose.append(hit.astype(f32).astype(bf))
    cp.join("ky0", KVX.at[0:3])
    cp.join("ky1", kb.at[0:3])
    z_start("kv")
    wl[0].wait()
    cp.join("dw", W2.at[:, :, 0:1024])
    cp.join("h2", H.at[0])
    HT[...] = H[...].reshape(1280, 512).T

    lo, hi = pl.ds(0, 64), pl.ds(64, 64)
    yr, yl = md(y, 1), md(y, -1)
    ro, rn, hand, handl = {}, {}, {}, {}

    def mul(c):
        cs = slice(512 * c, 512 * (c + 1))
        v = jnp.dot(HT[...], W2[:, :, cs].reshape(1280, 512), preferred_element_type=f32)
        PC[c] = v.astype(bf).reshape(4, 128, 512)
        ro[c] = [cp.remote(PC.at[c, md(y, 2), lo], RO.at[c, 0], Y(1), ("ro", c)),
                 cp.remote(PC.at[c, md(y, 2), hi], RO.at[c, 1], Y(-1), ("ro", c))]
        rn[c] = [cp.remote(PC.at[c, yr, hi], RN.at[c, 0, hi], Y(1), ("rn", c)),
                 cp.remote(PC.at[c, yl, lo], RN.at[c, 1, lo], Y(-1), ("rn", c))]

    def relay_y(c):
        cp.join(("ro", c), RO.at[c])
        PC[c, yr, 0:64, :] = (PC[c, yr, 0:64, :].astype(f32) + RO[c, 0].astype(f32)).astype(bf)
        rn[c].append(cp.remote(PC.at[c, yr, lo], RN.at[c, 0, lo], Y(1), ("rn", c)))
        PC[c, yl, 64:128, :] = (PC[c, yl, 64:128, :].astype(f32) + RO[c, 1].astype(f32)).astype(bf)
        rn[c].append(cp.remote(PC.at[c, yl, hi], RN.at[c, 1, hi], Y(-1), ("rn", c)))

    def give(c):
        cp.join(("rn", c), RN.at[c])
        v = PC[c, y].astype(f32) + RN[c, 0].astype(f32) + RN[c, 1].astype(f32)
        v = (v + b2[:, pl.ds(pl.multiple_of(2048 * x + 512 * c, 512), 512)]).astype(bf)
        SB[c, :, :, 0:512] = jnp.dot(pick, v, preferred_element_type=f32).astype(bf).reshape(8, 32, 512)
        w = pl.ds(0, 512)
        if c == 0:
            v = jnp.dot(pick, jnp.ones((128, 128), bf), preferred_element_type=f32)
            SB[c, :, :, 512:640] = v.astype(bf).reshape(8, 32, 128)
            w = pl.ds(0, 640)
        hand[c] = [cp.remote(SB.at[c, d[0], :, w], R.at[c, dp, :, w], d, ("hand", c)) for d in group]
        handl[c] = cp.here(SB.at[c, dp, :, w], R.at[c, dp, :, w])

    h = [pl.ds(0, 128), pl.ds(128, 128)]
    gx = gain[:, quarter(x)]
    filled, sq, yc = [None, None], [None, None], {1: [], -1: []}

    def take(c):
        cs = slice(512 * c, 512 * (c + 1))
        cp.join(("hand", c), R.at[c, 0:7, :, pl.ds(0, 640 if c == 0 else 512)])
        handl[c].wait()
        for i in range(2):
            if c == 0:
                seen = jnp.dot(choose[i], R[0, :, :, 512:640].reshape(256, 128), preferred_element_type=f32)
                filled[i] = seen[:, 0:1] > 0.5
            v = jnp.dot(choose[i], R[c, :, :, 0:512].reshape(256, 512), preferred_element_type=f32)
            v = jnp.where(filled[i], v, T[2 * i:2 * i + 2, :, cs].reshape(128, 512).astype(f32))
            t = jnp.sum(v * v, axis=1, keepdims=True)
            sq[i] = t if c == 0 else sq[i] + t
            A[y, 128 * i:128 * (i + 1), cs] = (v * gx[:, cs]).astype(bf)
            w, s = pl.ds(512 * c, 512), 1 - 2 * i
            yc[s].append(cp.remote(A.at[y, h[i], w], A.at[y, h[i], w], Y(s), ("yc", s)))

    mul(0)
    mul(1)
    relay_y(0)
    mul(2)
    relay_y(1)
    mul(3)
    z_mid("q")
    give(0)
    cp.join("tr", TR)
    tf = [cp.remote(TR.at[i], T.at[md(x, 2 * i - 1), th[i]], X(1 - 2 * i), "td") for i in range(2)]
    relay_y(2)
    z_mid("kv")
    give(1)
    relay_y(3)
    give(2)
    cp.join("td", T.at[0:3])
    tl.wait()
    give(3)
    take(0)
    take(1)
    z_end("q")
    take(2)
    z_end("kv")
    take(3)
    SS[x] = jnp.concatenate([jnp.broadcast_to(t, (128, 128)).T[0:8, :] for t in sq], axis=1)
    sx = [cp.remote(SS.at[x], SS.at[x], X(s), "sx") for s in (1, 2, 3)]
    z_all("q")
    z_all("kv")

    tag = [0]

    def pair(ga, oa, gb, ob, size):
        tag[0] += 1
        a = jnp.concatenate([A[ga, oa:oa + size, :], A[gb, ob:ob + size, :]], axis=0)
        us = []
        for g, o in ((ga, oa), (gb, ob)):
            at = lambda off, n, g=g, o=o: pl.ds(pl.multiple_of(256 * g + o + off, n), n)
            us.append(dict(tag=tag[0], size=size, rows=at(0, size), lo=at(0, size // 2), hi=at(size // 2, size // 2),
                           share=lambda v, g=g, o=o: pl.ds(
                               pl.multiple_of(256 * g + o + size // 4 * v, size // 4), size // 4),
                           slot=pl.ds(pl.multiple_of(64 * g + o // 4, size // 4), size // 4)))
        prod = lambda s: jnp.dot(a, wq[md(x, s)], preferred_element_type=f32)

        def put(ref, v):
            v = v.astype(ref.dtype)
            for n, u in enumerate(us):
                ref[u["rows"], :] = v[size * n:size * (n + 1)]

        put(QO, prod(2))
        for u in us:
            u["o"] = [cp.remote(QO.at[u["lo"]], RQO.at[0, u["lo"]], X(1), ("o", u["tag"])),
                      cp.remote(QO.at[u["hi"]], RQO.at[1, u["hi"]], X(-1), ("o", u["tag"]))]
        put(KP, lax.dot_general(a, wkv[...].reshape(256, 2048), NT, preferred_element_type=f32))
        for u in us:
            u["k"] = []
            for s in (2, 1, 3):
                u["k"].append(cp.remote(KP.at[u["share"](md(x, s))], RKV.at[x, u["slot"]], X(s), ("k", u["tag"])))
        put(QR, prod(1))
        for u in us:
            u["n"] = [cp.remote(QR.at[u["hi"]], RQN.at[0, u["hi"]], X(1), ("n", u["tag"]))]
        put(QL, prod(-1))
        for u in us:
            u["n"].append(cp.remote(QL.at[u["lo"]], RQN.at[1, u["lo"]], X(-1), ("n", u["tag"])))
        put(Q0, prod(0))
        return us

    def relay(us):
        cp.join(("o", us[0]["tag"]), RQO.at[0, 0:2 * us[0]["size"]])
        for u in us:
            lo, hi = u["lo"], u["hi"]
            QR[lo, :] = (QR[lo, :].astype(f32) + RQO[0, lo, :].astype(f32)).astype(bf)
            u["n"].append(cp.remote(QR.at[lo], RQN.at[0, lo], X(1), ("n", u["tag"])))
            QL[hi, :] = (QL[hi, :].astype(f32) + RQO[1, hi, :].astype(f32)).astype(bf)
            u["n"].append(cp.remote(QL.at[hi], RQN.at[1, hi], X(-1), ("n", u["tag"])))

    bias = jnp.concatenate([kb[p // 4, p % 4, pl.ds(y, 1), 0:16] for p in range(16)], axis=1)

    def keys(us):
        cp.join(("k", us[0]["tag"]), KP.at[0:3 * us[0]["size"] // 2])
        for u in us:
            m = u["share"](x)
            v = KP[m, :].astype(f32)
            for s in (1, 2, 3):
                v = v + RKV[md(x, s), u["slot"]].astype(f32)
            sc = SC[m, :]
            v = v * jnp.concatenate([sc, sc], axis=1) + bias
            kv_out[m, :] = v.astype(bf)
            u["f"] = [cp.remote(kv_out.at[m], kv_out.at[m], X(s), ("f", u["tag"])) for s in (2, 1, 3)]

    def scale(g):
        v = lax.rsqrt(SY[g] * (1.0 / 8192.0) + 1e-6)
        for i in range(2):
            SC[pl.ds(pl.multiple_of(256 * g + 128 * i, 128), 128), :] = jnp.broadcast_to(
                v[0:1, 128 * i:128 * (i + 1)], (128, 128)).T

    def finish(us):
        cp.join(("n", us[0]["tag"]), RQN.at[0, 0:4 * us[0]["size"]])
        for u in us:
            rows = u["rows"]
            sc = SC[rows, :]
            v = Q0[rows, :] + RQN[0, rows, :].astype(f32) + RQN[1, rows, :].astype(f32)
            q_out[rows, :] = (v * jnp.concatenate([sc, sc], axis=1) + qb[...]).astype(bf)
        cp.join(("f", us[0]["tag"]), KP.at[0:3 * us[0]["size"] // 2])

    u0 = pair(y, 0, y, 128, 128)
    cp.join("sx", SS.at[0:3])
    SY[y] = SS[0] + SS[1] + SS[2] + SS[3]
    sy = [cp.remote(SY.at[y], SY.at[y], Y(s), "sy") for s in (1, 2, 3)]
    band = lambda o: pl.ds(o, 64)
    yo = {1: [cp.remote(A.at[y, band(o)], A.at[y, band(o)], Y(1)) for o in (128, 192)],
          -1: [cp.remote(A.at[y, band(o)], A.at[y, band(o)], Y(-1)) for o in (0, 64)]}
    scale(y)
    relay(u0)
    up, dn, op = yr, yl, md(y, 2)
    far = {}
    cp.join(("yc", 1), A.at[0, h[0]])
    far[1] = [cp.remote(A.at[dn, band(o)], A.at[dn, band(o)], Y(1)) for o in (0, 64)]
    cp.join(("yc", -1), A.at[0, h[0]])
    far[-1] = [cp.remote(A.at[up, band(o)], A.at[up, band(o)], Y(-1)) for o in (128, 192)]
    keys(u0)
    u1 = pair(dn, 0, up, 128, 128)
    finish(u0)
    relay(u1)
    yo[1][0].wait_recv()
    yo[-1][0].wait_recv()
    cp.join("sy", SY.at[0:3])
    for g in (dn, up, op):
        scale(g)
    u2 = pair(dn, 128, up, 0, 64)
    keys(u1)
    relay(u2)
    yo[1][1].wait_recv()
    yo[-1][1].wait_recv()
    u3 = pair(dn, 192, up, 64, 64)
    keys(u2)
    finish(u1)
    relay(u3)
    far[1][0].wait_recv()
    far[-1][0].wait_recv()
    u4 = pair(op, 0, op, 128, 64)
    keys(u3)
    finish(u2)
    far[1][1].wait_recv()
    far[-1][1].wait_recv()
    u5 = pair(op, 64, op, 192, 64)
    relay(u4)
    keys(u4)
    finish(u3)
    relay(u5)
    keys(u5)
    finish(u4)
    finish(u5)
    cp.drain()
    assert len(cp.groups) == N3, len(cp.groups)


def whole(patches, ids, owner, slots, text, vnorm, qkv_w, qkv_b, out_w, mnorm, w1, b1, w2, b2, gain, qw, qb, kvw, kvb):
    bf, f32, i32 = jnp.bfloat16, jnp.float32, jnp.int32
    V, ANY = pl.BlockSpec(memory_space=pltpu.VMEM), pl.BlockSpec(memory_space=pl.ANY)
    S = jax.ShapeDtypeStruct
    M = pltpu.VMEM
    return pl.pallas_call(
        whole_kernel,
        out_shape=(S((1024, 256), bf), S((1024, 256), bf)),
        in_specs=[V, V, V, V, ANY, V, ANY, V, ANY, V, ANY, V, ANY, V, V, ANY, V, V, V],
        out_specs=[V] * 2,
        scratch_shapes=[
            M((4, 32, 1280), bf),
            M((4, 4, 4, 32, 1280), bf),
            M((1280, 1920), bf),
            M((640, 1280), bf),
            M((320, 5120), bf),
            M((4, 320, 512), bf),
            M((512, 1280), bf),
            M((4, 320, 2048), bf),
            M((4, 2048, 256), bf),
            M((4, 4, 16, 2048), bf),
            M((4, 16, 8192), bf),
            M((4, 4, 16, 256), bf),
            M((8, 128), f32),
            M((4, 4, 8, 128), f32),
            M((8, 128), i32),
            M((4, 8, 128), i32),
            M((2, 160, 256), bf),
            M((2, 128, 256), bf),
            M((4, 4, 128, 512), bf),
            M((4, 2, 64, 512), bf),
            M((4, 2, 128, 512), bf),
            M((4, 64, 2048), bf),
            M((2, 32, 2048), bf),
            M((4, 8, 32, 640), bf),
            M((4, 8, 32, 640), bf),
            M((4, 256, 2048), bf),
            M((4, 8, 256), f32),
            M((4, 8, 256), f32),
            M((1024, 128), f32),
            M((1024, 256), f32),
            M((1024, 256), bf),
            M((1024, 256), bf),
            M((1024, 256), bf),
            M((2, 1024, 256), bf),
            M((2, 1024, 256), bf),
            M((1024, 256), bf),
            M((4, 256, 256), bf),
            pltpu.SemaphoreType.DMA((N3,)),
            pltpu.SemaphoreType.DMA((N3,)),
            pltpu.SemaphoreType.DMA((16,)),
        ],
        compiler_params=pltpu.CompilerParams(collective_id=1, has_side_effects=True, vmem_limit_bytes=64000000),
        name="whole",
    )(patches, ids, owner, slots, text, vnorm, qkv_w, qkv_b, out_w, mnorm, w1, b1, w2, b2, gain, qw, qb, kvw, kvb)


def attention_kernel(q, kv, out):
    bf, f32 = jnp.bfloat16, jnp.float32
    c, d = lax.broadcasted_iota(jnp.int32, (256, 128), 0), lax.broadcasted_iota(jnp.int32, (256, 128), 1)
    spot = (d // 8) * 16 + d % 8
    keys = jnp.dot(kv[...], (c == spot).astype(f32).astype(bf), preferred_element_type=f32).astype(bf)
    values = jnp.dot(kv[...], (c == spot + 8).astype(f32).astype(bf), preferred_element_type=f32).astype(bf)
    low = lax.broadcasted_iota(jnp.int32, (256, 256), 0) >= lax.broadcasted_iota(jnp.int32, (256, 256), 1)
    k = HD ** (-0.5) * 1.4426950408889634
    for i in range(4):
        rows = slice(256 * i, 256 * (i + 1))
        for h in range(2):
            hs = slice(128 * h, 128 * (h + 1))
            s = lax.dot_general(q[rows, hs], keys[rows], NT, preferred_element_type=f32)
            s = jnp.where(low, s, -1e30)
            top = jnp.max(s, axis=1, keepdims=True)
            if i:
                before = lax.dot_general(q[rows, hs], keys[:256 * i], NT, preferred_element_type=f32)
                top = jnp.maximum(top, jnp.max(before, axis=1, keepdims=True))
            p = jnp.exp2((s - top) * k)
            total = jnp.sum(p, axis=1, keepdims=True)
            m = jnp.dot(p.astype(bf), values[rows], preferred_element_type=f32)
            if i:
                p = jnp.exp2((before - top) * k)
                total = total + jnp.sum(p, axis=1, keepdims=True)
                m = m + jnp.dot(p.astype(bf), values[:256 * i], preferred_element_type=f32)
            out[rows, hs] = (m / total).astype(bf)


def attention(q, kv):
    V = pl.BlockSpec(memory_space=pltpu.VMEM)
    return pl.pallas_call(
        attention_kernel,
        out_shape=jax.ShapeDtypeStruct((1024, 256), jnp.bfloat16),
        in_specs=[V, V],
        out_specs=V,
        compiler_params=pltpu.CompilerParams(vmem_limit_bytes=60000000),
        name="attention",
    )(q, kv)


def shards(
    patches,
    window_ids,
    owner,
    slot_of_row,
    text_embeds,
    vit_norm,
    vit_qkv_w,
    vit_qkv_b,
    vit_out_w,
    merge_norm,
    merge_w1,
    merge_b1,
    merge_w2,
    merge_b2,
    llm_norm,
    q_w,
    q_b,
    kv_w,
    kv_b,
):
    q, kv = whole(
        patches, window_ids, owner.reshape(1, 32), slot_of_row, text_embeds, vit_norm, vit_qkv_w,
        vit_qkv_b, vit_out_w, merge_norm, merge_w1.T, merge_b1, merge_w2, merge_b2[None],
        llm_norm[None], q_w, q_b[None], kv_w.transpose(0, 2, 1), kv_b,
    )
    return attention(q, kv)


def solution(mesh):
    return jax.shard_map(
        shards,
        mesh=mesh,
        in_specs=(
            P(("dp", "mp"), None),
            P(("dp", "mp"), None),
            P(("dp", "mp"), None),
            P(("dp", "mp"), None),
            P(("dp", "mp"), None),
            P(),
            P(),
            P(),
            P(),
            P(),
            P(None, "mp"),
            P("mp"),
            P("mp", None),
            P(),
            P(),
            P(None, "mp"),
            P("mp"),
            P(None, None, "mp"),
            P(None, "mp"),
        ),
        out_specs=P("dp", "mp"),
        check_vma=False,
    )
```

```python
import jax
import jax.numpy as jnp
from jax import lax
from jax.experimental import pallas as pl
from jax.experimental.pallas import tpu as pltpu
from jax.sharding import PartitionSpec as P

VHD = 80
HD = 128
MESH = pl.DeviceIdType.MESH
NT = (((1,), (1,)), ((), ()))


class Copies:
    def __init__(self, send, recv, local):
        self.send, self.recv, self.local = send, recv, local
        self.groups, self.outs, self.views, self.m, self.n = {}, {}, {}, 0, 0

    def remote(self, src, dst, dev, group=None, out=None):
        if group is None:
            self.n += 1
            group = self.n
        if out is None:
            out = group[0] if isinstance(group, tuple) and group[0] in "o n k f ro rn".split() else group
        j = self.outs.setdefault(out, len(self.outs))
        k = self.groups.setdefault(group, len(self.groups))
        c = pltpu.make_async_remote_copy(
            src_ref=src, dst_ref=dst, send_sem=self.send.at[j], recv_sem=self.recv.at[k],
            device_id=dev, device_id_type=MESH)
        c.start()
        return c

    def join(self, group, view):
        k = self.groups[group]
        self.views[group] = view
        pltpu.make_async_copy(view, view, self.recv.at[k]).wait()

    def here(self, src, dst):
        k = self.m
        self.m += 1
        c = pltpu.make_async_copy(src, dst, self.local.at[k])
        c.start()
        return c

    def drain(self, views):
        for out, j in self.outs.items():
            view = views[out] if out in views else self.views[out]
            pltpu.make_async_copy(view, view, self.send.at[j]).wait()


def places():
    mp, dp = lax.axis_index("mp"), lax.axis_index("dp")
    y, x = mp // 4, lax.rem(mp, 4)
    X = lambda s: (dp, y * 4 + lax.rem(x + s + 4, 4))
    Y = lambda s: (dp, lax.rem(y + s + 4, 4) * 4 + x)
    Z = lambda s: (lax.rem(dp + 2 * s + 8, 8), mp)
    other = (dp + 1 - 2 * lax.rem(dp, 2), mp)
    return dp, y, x, X, Y, Z, other


def meet(devs):
    barrier = pltpu.get_barrier_semaphore()
    for d in devs:
        pl.semaphore_signal(barrier, inc=1, device_id=d, device_id_type=MESH)
    pl.semaphore_wait(barrier, len(devs))


N3 = 117
N4 = 32


def vision(patches, ids, norm, qkv_w, qkv_b, out_w, gain):
    bf, f32 = jnp.bfloat16, jnp.float32
    iota = lambda shape, d: lax.broadcasted_iota(jnp.int32, shape, d)
    i, s = iota((128, 128), 0), iota((128, 128), 1)
    perm = (s == (i % 32) * 4 + i // 32).astype(f32).astype(bf)
    p = jnp.dot(perm, patches[...], preferred_element_type=f32)
    wide = jnp.broadcast_to(ids[...].astype(f32), (128, 128)).astype(bf)
    across = lax.dot_general(wide, perm, NT, preferred_element_type=f32)
    same = across == across.T
    normed = p * lax.rsqrt(jnp.mean(p * p, axis=1, keepdims=True) + 1e-6) * norm[...].reshape(1, 1280)
    qkv = (jnp.dot(normed.astype(bf), qkv_w[...], preferred_element_type=f32) + qkv_b[...].reshape(1, 1920)).astype(bf)
    tiles = [None] * 5
    for h in range(8):
        lo, hi = 80 * h // 128, (80 * h + 207) // 128
        lane = iota((128, 128 * (hi - lo)), 1) + 128 * lo
        here = (lane >= 80 * h) & (lane < 80 * h + 80)
        part = lambda k: qkv[:, 640 * k + 128 * lo:640 * k + 128 * hi]
        zero = jnp.zeros((), bf)
        sc = lax.dot_general(jnp.where(here, part(0), zero), part(1), NT, preferred_element_type=f32) * VHD ** (-0.5)
        sc = jnp.where(same, sc, -1e30)
        e = jnp.exp(sc - jnp.max(sc, axis=1, keepdims=True))
        w = (e / jnp.sum(e, axis=1, keepdims=True)).astype(bf)
        mix = jnp.dot(w, jnp.where(here, part(2), zero), preferred_element_type=f32)
        for t in range(lo, hi):
            v = mix[:, 128 * (t - lo):128 * (t - lo + 1)]
            tiles[t] = v if tiles[t] is None else tiles[t] + v
    mixed = jnp.concatenate(tiles, axis=1).astype(bf)
    r = (p + jnp.dot(mixed, out_w[...], preferred_element_type=f32)).astype(bf).astype(f32)
    return (r * lax.rsqrt(jnp.mean(r * r, axis=1, keepdims=True) + 1e-6) * gain[...].reshape(1, 1280)).astype(bf)


def whole_kernel(patches, ids, owner, slots, text, vnorm, qkv_w, qkv_b, out_w, mnorm, w1, b1, w2, b2, gain, qw, qb,
                 kvw, kvb, q_out, kv_out,
                 MS, G, QKVW, OUTW, w1v, H, HT, W2, wq, wkv, KVS, KVX, KBS, kb, INS, info, RW, RQ,
                 PC, RO, RN, T, TR, SB, R, A, SS, SY, SC, Q0, QR, QL, QO, RQO, RQN, KP, RKV, send, recv, local):
    dp, y, x, X, Y, Z, other = places()
    md = lambda v, s: lax.rem(v + s + 4, 4)
    bf, f32 = jnp.bfloat16, jnp.float32
    iota = lambda shape, d: lax.broadcasted_iota(jnp.int32, shape, d)
    e, mp = dp, y * 4 + x
    cp = Copies(send, recv, local)
    lv = [cp.here(qkv_w, QKVW), cp.here(out_w, OUTW), cp.here(w1, w1v)]
    group = [(lax.rem(dp + s, 8), mp) for s in (2, 6, 1, 3, 5, 7, 4)]
    meet([X(1), X(2), X(3), Y(1), Y(2), Y(3)] + group)
    ca, cb = pl.ds(0, 768), pl.ds(768, 512)
    sa = lambda yy, xx: G.at[:, yy, xx, :, ca]
    sb = lambda yy, xx: G.at[:, yy, xx, :, cb]
    cols = lambda xd: pl.ds(pl.multiple_of(2048 * xd + 256 * e, 256), 256)
    mine = pl.ds(pl.multiple_of(256 * e, 256), 256)
    first, second = pl.ds(0, 2), pl.ds(2, 2)

    xo = md(x, 2)
    w2_half = [pl.ds(0, 160), pl.ds(160, 160)]
    q_half = lambda v, i: pl.ds(pl.multiple_of(2048 * v + 256 * e + 128 * i, 128), 128)
    bands = lambda r: pl.ds(pl.multiple_of(256 * r, 256), 256)
    zw, zwf, dw = {}, {}, []

    def w2_start(s):
        xs = md(x, s)
        src = w2.at[:, cols(x)] if s == 0 else W2.at[xs, :, mine]
        zw[s] = {t: cp.remote(src, W2.at[xs, :, mine], Z(t), out="w") for t in (1, -1)}
        dw.append(cp.remote(src, W2.at[xs, :, mine], other, "dw"))

    def w2_mid(s):
        xs, way = md(x, s), 1 if s in (0, 1) else -1
        for t in (1, -1):
            zw[s][t].wait_recv()
            at = W2.at[xs, :, bands(lax.rem(e - 2 * t + 8, 8))]
            if t == way:
                zwf[s] = cp.remote(at, at, Z(t), out="w")
            dw.append(cp.remote(at, at, other, "dw"))

    def w2_end(s):
        zwf[s].wait_recv()
        at = W2.at[md(x, s), :, bands(lax.rem(e + 4, 8))]
        dw.append(cp.remote(at, at, other, "dw"))

    w2r = [cp.remote(w2.at[w2_half[i], cols(xo)], RW.at[i], X(1 - 2 * i), out="w") for i in range(2)]
    w2d = [cp.remote(w2.at[:, cols(md(x, s))], W2.at[x, :, mine], X(s), out="w") for s in (1, -1)]
    w2_start(0)
    wl = [cp.here(w2.at[:, cols(x)], W2.at[x, :, mine]), cp.here(qw.at[cols(x), :], wq.at[x, mine, :])]

    lv[0].wait()
    lv[1].wait()
    MS[...] = vision(patches, ids, vnorm, QKVW, qkv_b, OUTW, mnorm).reshape(4, 32, 1280)

    ma, mb = MS.at[:, :, ca], MS.at[:, :, cb]
    a1 = {s: cp.remote(ma, sa(y, x), X(s), out="g") for s in (1, -1)}
    c1 = {s: cp.remote(mb, sb(y, x), Y(s), out="g") for s in (1, -1)}
    a2 = {(0, s): cp.remote(ma, sa(y, x), Y(s), out="g") for s in (1, -1)}
    c2 = {(0, s): cp.remote(mb, sb(y, x), X(s), out="g") for s in (1, -1)}
    gl = cp.here(MS, G.at[:, y, x])
    i64, s64 = iota((64, 64), 0), iota((64, 64), 1)
    order = (s64 == (i64 // 8 % 2) * 32 + (i64 % 8) * 4 + i64 // 16).astype(f32).astype(bf)
    for n in range(4):
        cs = slice(2048 * n, 2048 * (n + 1))
        v = jnp.dot(order, kvw[:, :, cs].reshape(64, 2048), preferred_element_type=f32)
        KVS[:, :, cs] = v.astype(bf).reshape(4, 16, 2048)
    li, ll = iota((128, 128), 0), iota((128, 128), 1)
    rows = []
    flat = jnp.concatenate([kvb[0:1, :], kvb[1:2, :], jnp.zeros((1, 64), f32)], axis=1)
    down = jnp.broadcast_to(flat, (128, 128)).T
    for j in range(4):
        keep = (li == (ll // 8) * 32 + (ll % 8) * 4 + j) & (ll < 16)
        rows.append(jnp.sum(jnp.where(keep, down, 0.0), axis=0, keepdims=True))
    KBS[...] = jnp.concatenate(rows + [jnp.zeros((4, 128), f32)], axis=0)
    own4 = jnp.broadcast_to(jnp.concatenate([owner[...]] * 4, axis=1), (8, 128))
    slot2 = jnp.broadcast_to(jnp.concatenate([slots[...]] * 2, axis=1), (8, 128))
    t0, t1 = iota((8, 128), 0), iota((8, 128), 1)
    INS[...] = jnp.where((t0 == 0) & (t1 // 32 == x), own4,
                         jnp.where((t0 == 1 + x // 2) & (t1 // 64 == x % 2), slot2, 0))
    KVX[x] = KVS[:, :, cols(x)]
    kb[y, x] = KBS[...]
    info[x] = INS[...]

    af, cf = {}, {}
    for s in (1, -1):
        hf = first if s == 1 else second
        a1[s].wait_recv()
        xs = md(x, -s)
        at = G.at[hf, y, xs, :, ca]
        af[s] = cp.remote(at, at, X(s), out="g")
        for t in (1, -1):
            a2[(-s, t)] = cp.remote(sa(y, xs), sa(y, xs), Y(t), out="g")
        c1[s].wait_recv()
        ys = md(y, -s)
        at = G.at[hf, ys, x, :, cb]
        cf[s] = cp.remote(at, at, Y(s), out="g")
        for t in (1, -1):
            c2[(-s, t)] = cp.remote(sb(ys, x), sb(ys, x), X(t), out="g")
    last = []

    def pass_on(p):
        for t in (1, -1):
            hf = first if t == 1 else second
            a2[(p, t)].wait_recv()
            at = G.at[hf, md(y, -t), md(x, p), :, ca]
            last.append(cp.remote(at, at, Y(t), "last"))
            c2[(p, t)].wait_recv()
            at = G.at[hf, md(y, p), md(x, -t), :, cb]
            last.append(cp.remote(at, at, X(t), "last"))

    qr = [cp.remote(qw.at[q_half(xo, i), :], RQ.at[i], X(1 - 2 * i), out="z") for i in range(2)]
    qd = [cp.remote(qw.at[cols(md(x, s)), :], wq.at[x, mine, :], X(s), "qd") for s in (1, -1)]
    wx = []
    for t in (1, 3, 2):
        wx.append(cp.remote(KVS.at[:, :, cols(md(x, t))], KVX.at[x], X(t), "wx0"))
        wx.append(cp.remote(KBS, kb.at[y, x], X(t), "wx1"))
        wx.append(cp.remote(INS, info.at[x], X(t), "wx2"))
    for c in w2r:
        c.wait_recv()
    w2f = [cp.remote(RW.at[i], W2.at[md(x, 2 * i - 1), w2_half[i], mine], X(1 - 2 * i), out="w") for i in range(2)]
    w2_mid(0)
    w2d[0].wait_recv()
    w2_start(-1)
    w2d[1].wait_recv()
    w2_start(1)
    pass_on(0)

    def piece(name, r, half=None):
        h = pl.ds(0, 4) if half is None else (first, second)[half]
        if name == "q":
            return wq.at[h, bands(r), :]
        return wkv.at[h, :, :, bands(r)]

    zs, ds_, zf = {}, {}, {}

    def z_start(name):
        zs[name] = {s: cp.remote(piece(name, e), piece(name, e), Z(s), out="z") for s in (1, -1)}
        ds_[name] = [cp.remote(piece(name, e), piece(name, e), other, "d" + name)]

    def z_mid(name):
        zf[name] = {}
        for s in (1, -1):
            zs[name][s].wait_recv()
            r, h = lax.rem(e - 2 * s + 8, 8), 0 if s == 1 else 1
            zf[name][s] = cp.remote(piece(name, r, h), piece(name, r, h), Z(s), out="z")
            ds_[name].append(cp.remote(piece(name, r), piece(name, r), other, "d" + name))

    def z_end(name):
        for s in (1, -1):
            zf[name][s].wait_recv()
        r = lax.rem(e + 4, 8)
        ds_[name].append(cp.remote(piece(name, r), piece(name, r), other, "d" + name))

    def z_all(name):
        cp.join("d" + name, wq.at[:, 0:1024, :] if name == "q" else wkv.at[:, :, :, 0:1024])

    for s in (1, -1):
        af[s].wait_recv()
        cf[s].wait_recv()
    xf, yf = md(x, 2), md(y, 2)
    for t in (1, -1):
        a2[(2, t)] = cp.remote(sa(y, xf), sa(y, xf), Y(t), out="g")
        c2[(2, t)] = cp.remote(sb(yf, x), sb(yf, x), X(t), out="g")
    pass_on(-1)
    pass_on(1)
    for c in qr:
        c.wait_recv()
    qf = [cp.remote(RQ.at[i], wq.at[md(x, 2 * i - 1), pl.ds(pl.multiple_of(256 * e + 128 * i, 128), 128), :],
                    X(1 - 2 * i), "qd") for i in range(2)]
    w2_mid(-1)
    w2_mid(1)
    pass_on(2)
    for c in w2f:
        c.wait_recv()
    w2_start(2)
    cp.join("last", G.at[:, 0])
    gl.wait()
    lv[2].wait()
    wide = jnp.concatenate([b1[...].reshape(1, 320), jnp.zeros((1, 64), f32)], axis=1)
    bcol = jnp.broadcast_to(wide, (128, 384)).T[0:320, :]
    bcol = jnp.concatenate([bcol, bcol], axis=1)
    h1 = {}
    for g in range(2):
        acc = None
        for j in range(4):
            p = lax.dot_general(w1v[:, 1280 * j:1280 * (j + 1)], G[j, 2 * g:2 * g + 2].reshape(256, 1280), NT,
                                preferred_element_type=f32)
            acc = p if acc is None else acc + p
        v = acc + bcol
        v = 0.5 * v * (1.0 + lax.erf(v * (0.5 ** 0.5)))
        H[x, :, 256 * g:256 * (g + 1)] = v.astype(bf)
        hc = pl.ds(256 * g, 256)
        for s in (1, -1):
            h1[(g, s)] = cp.remote(H.at[x, :, hc], H.at[x, :, hc], X(s), out="h")
    h2 = []

    def pass_hidden(g):
        for s in (1, -1):
            h1[(g, s)].wait_recv()
            at = H.at[md(x, -s), pl.ds(0, 160) if s == 1 else pl.ds(160, 160), pl.ds(256 * g, 256)]
            h2.append(cp.remote(at, at, X(s), "h2"))

    w2_mid(2)
    cp.join("wx0", KVX.at[0:3])
    cp.join("wx1", kb.at[0, 0:3])
    cp.join("wx2", info.at[0:3])
    ky = []
    for s in (1, 2, 3):
        yd = md(y, s)
        ky.append(cp.remote(KVX.at[:, yd], wkv.at[y, :, :, mine], Y(s), "ky0"))
        ky.append(cp.remote(kb.at[y], kb.at[y], Y(s), "ky1"))
    wkv[y, :, :, mine] = KVX[:, y]
    cp.join("qd", wq.at[0, 0:768, :])
    wl[1].wait()
    z_start("q")
    pass_hidden(0)
    for s in (0, -1, 1, 2):
        w2_end(s)
    pass_hidden(1)
    quarter = lambda v: pl.ds(pl.multiple_of(2048 * v, 2048), 2048)
    th = [pl.ds(0, 32), pl.ds(32, 32)]
    tr = [cp.remote(text.at[th[i], quarter(xo)], TR.at[i], X(1 - 2 * i), "tr") for i in range(2)]
    td = [cp.remote(text.at[:, quarter(md(x, s))], T.at[x], X(s), "td") for s in (1, -1)]
    tl = cp.here(text.at[:, quarter(x)], T.at[x])
    tab = info[0] + info[1] + info[2] + info[3]
    own = tab[0:1, :]
    down = jnp.broadcast_to(own.astype(f32), (128, 128)).T.astype(jnp.int32)
    before = (down == own) & (li < ll) & (li // 32 == ll // 32)
    rank = jnp.sum(before.astype(jnp.int32), axis=0, keepdims=True)
    target = own * 32 + (iota((1, 128), 1) // 32) * 8 + rank
    pick = (iota((256, 128), 0) == target).astype(f32).astype(bf)
    choose = []
    for i in range(2):
        s = jnp.broadcast_to(tab[1 + i:2 + i, :].astype(f32), (128, 128)).T.astype(jnp.int32)
        s = jnp.concatenate([s, s], axis=1)
        lane, row = iota((128, 256), 1), iota((128, 256), 0)
        hit = ((lane // 32) * 8 + lane % 8 == s) & ((lane % 32) // 8 == row // 64 + 2 * i)
        choose.append(hit.astype(f32).astype(bf))
    cp.join("ky0", KVX.at[0:3])
    cp.join("ky1", kb.at[0:3])
    z_start("kv")
    wl[0].wait()
    cp.join("dw", W2.at[:, :, 0:1024])
    cp.join("h2", H.at[0])
    HT[...] = H[...].reshape(1280, 512).T

    lo, hi = pl.ds(0, 64), pl.ds(64, 64)
    yr, yl = md(y, 1), md(y, -1)
    ro, rn, hand, handl = {}, {}, {}, {}

    def mul(c):
        cs = slice(512 * c, 512 * (c + 1))
        v = jnp.dot(HT[...], W2[:, :, cs].reshape(1280, 512), preferred_element_type=f32)
        PC[c] = v.astype(bf).reshape(4, 128, 512)
        ro[c] = [cp.remote(PC.at[c, md(y, 2), lo], RO.at[c, 0], Y(1), ("ro", c)),
                 cp.remote(PC.at[c, md(y, 2), hi], RO.at[c, 1], Y(-1), ("ro", c))]
        rn[c] = [cp.remote(PC.at[c, yr, hi], RN.at[c, 0, hi], Y(1), ("rn", c)),
                 cp.remote(PC.at[c, yl, lo], RN.at[c, 1, lo], Y(-1), ("rn", c))]

    def relay_y(c):
        cp.join(("ro", c), RO.at[c])
        PC[c, yr, 0:64, :] = (PC[c, yr, 0:64, :].astype(f32) + RO[c, 0].astype(f32)).astype(bf)
        rn[c].append(cp.remote(PC.at[c, yr, lo], RN.at[c, 0, lo], Y(1), ("rn", c)))
        PC[c, yl, 64:128, :] = (PC[c, yl, 64:128, :].astype(f32) + RO[c, 1].astype(f32)).astype(bf)
        rn[c].append(cp.remote(PC.at[c, yl, hi], RN.at[c, 1, hi], Y(-1), ("rn", c)))

    def give(c):
        cp.join(("rn", c), RN.at[c])
        v = PC[c, y].astype(f32) + RN[c, 0].astype(f32) + RN[c, 1].astype(f32)
        v = (v + b2[:, pl.ds(pl.multiple_of(2048 * x + 512 * c, 512), 512)]).astype(bf)
        SB[c, :, :, 0:512] = jnp.dot(pick, v, preferred_element_type=f32).astype(bf).reshape(8, 32, 512)
        w = pl.ds(0, 512)
        if c == 0:
            v = jnp.dot(pick, jnp.ones((128, 128), bf), preferred_element_type=f32)
            SB[c, :, :, 512:640] = v.astype(bf).reshape(8, 32, 128)
            w = pl.ds(0, 640)
        hand[c] = [cp.remote(SB.at[c, d[0], :, w], R.at[c, dp, :, w], d, ("hand", c)) for d in group]
        handl[c] = cp.here(SB.at[c, dp, :, w], R.at[c, dp, :, w])

    h = [pl.ds(0, 128), pl.ds(128, 128)]
    gx = gain[:, quarter(x)]
    filled, sq, yc = [None, None], [None, None], {1: [], -1: []}

    def take(c):
        cs = slice(512 * c, 512 * (c + 1))
        cp.join(("hand", c), R.at[c, 0:7, :, pl.ds(0, 640 if c == 0 else 512)])
        handl[c].wait()
        for i in range(2):
            if c == 0:
                seen = jnp.dot(choose[i], R[0, :, :, 512:640].reshape(256, 128), preferred_element_type=f32)
                filled[i] = seen[:, 0:1] > 0.5
            v = jnp.dot(choose[i], R[c, :, :, 0:512].reshape(256, 512), preferred_element_type=f32)
            v = jnp.where(filled[i], v, T[2 * i:2 * i + 2, :, cs].reshape(128, 512).astype(f32))
            t = jnp.sum(v * v, axis=1, keepdims=True)
            sq[i] = t if c == 0 else sq[i] + t
            A[y, 128 * i:128 * (i + 1), cs] = (v * gx[:, cs]).astype(bf)
            w, s = pl.ds(512 * c, 512), 1 - 2 * i
            yc[s].append(cp.remote(A.at[y, h[i], w], A.at[y, h[i], w], Y(s), ("yc", s)))

    mul(0)
    mul(1)
    relay_y(0)
    mul(2)
    relay_y(1)
    mul(3)
    z_mid("q")
    give(0)
    cp.join("tr", TR)
    tf = [cp.remote(TR.at[i], T.at[md(x, 2 * i - 1), th[i]], X(1 - 2 * i), "td") for i in range(2)]
    relay_y(2)
    z_mid("kv")
    give(1)
    relay_y(3)
    give(2)
    cp.join("td", T.at[0:3])
    tl.wait()
    give(3)
    take(0)
    take(1)
    z_end("q")
    take(2)
    z_end("kv")
    take(3)
    SS[x] = jnp.concatenate([jnp.broadcast_to(t, (128, 128)).T[0:8, :] for t in sq], axis=1)
    sx = [cp.remote(SS.at[x], SS.at[x], X(s), "sx") for s in (1, 2, 3)]
    z_all("q")
    z_all("kv")

    tag = [0]

    def pair(ga, oa, gb, ob, size):
        tag[0] += 1
        a = jnp.concatenate([A[ga, oa:oa + size, :], A[gb, ob:ob + size, :]], axis=0)
        us = []
        for g, o in ((ga, oa), (gb, ob)):
            at = lambda off, n, g=g, o=o: pl.ds(pl.multiple_of(256 * g + o + off, n), n)
            us.append(dict(tag=tag[0], size=size, rows=at(0, size), lo=at(0, size // 2), hi=at(size // 2, size // 2),
                           share=lambda v, g=g, o=o: pl.ds(
                               pl.multiple_of(256 * g + o + size // 4 * v, size // 4), size // 4),
                           slot=pl.ds(pl.multiple_of(64 * g + o // 4, size // 4), size // 4)))
        prod = lambda s: jnp.dot(a, wq[md(x, s)], preferred_element_type=f32)

        def put(ref, v):
            v = v.astype(ref.dtype)
            for n, u in enumerate(us):
                ref[u["rows"], :] = v[size * n:size * (n + 1)]

        put(QO, prod(2))
        for u in us:
            u["o"] = [cp.remote(QO.at[u["lo"]], RQO.at[0, u["lo"]], X(1), ("o", u["tag"])),
                      cp.remote(QO.at[u["hi"]], RQO.at[1, u["hi"]], X(-1), ("o", u["tag"]))]
        put(KP, lax.dot_general(a, wkv[...].reshape(256, 2048), NT, preferred_element_type=f32))
        for u in us:
            u["k"] = []
            for s in (2, 1, 3):
                u["k"].append(cp.remote(KP.at[u["share"](md(x, s))], RKV.at[x, u["slot"]], X(s), ("k", u["tag"])))
        put(QR, prod(1))
        for u in us:
            u["n"] = [cp.remote(QR.at[u["hi"]], RQN.at[0, u["hi"]], X(1), ("n", u["tag"]))]
        put(QL, prod(-1))
        for u in us:
            u["n"].append(cp.remote(QL.at[u["lo"]], RQN.at[1, u["lo"]], X(-1), ("n", u["tag"])))
        put(Q0, prod(0))
        return us

    def relay(us):
        cp.join(("o", us[0]["tag"]), RQO.at[0, 0:2 * us[0]["size"]])
        for u in us:
            lo, hi = u["lo"], u["hi"]
            QR[lo, :] = (QR[lo, :].astype(f32) + RQO[0, lo, :].astype(f32)).astype(bf)
            u["n"].append(cp.remote(QR.at[lo], RQN.at[0, lo], X(1), ("n", u["tag"])))
            QL[hi, :] = (QL[hi, :].astype(f32) + RQO[1, hi, :].astype(f32)).astype(bf)
            u["n"].append(cp.remote(QL.at[hi], RQN.at[1, hi], X(-1), ("n", u["tag"])))

    bias = jnp.concatenate([kb[p // 4, p % 4, pl.ds(y, 1), 0:16] for p in range(16)], axis=1)

    def keys(us):
        cp.join(("k", us[0]["tag"]), KP.at[0:3 * us[0]["size"] // 2])
        for u in us:
            m = u["share"](x)
            v = KP[m, :].astype(f32)
            for s in (1, 2, 3):
                v = v + RKV[md(x, s), u["slot"]].astype(f32)
            sc = SC[m, :]
            v = v * jnp.concatenate([sc, sc], axis=1) + bias
            kv_out[m, :] = v.astype(bf)
            u["f"] = [cp.remote(kv_out.at[m], kv_out.at[m], X(s), ("f", u["tag"])) for s in (2, 1, 3)]

    def scale(g):
        v = lax.rsqrt(SY[g] * (1.0 / 8192.0) + 1e-6)
        for i in range(2):
            SC[pl.ds(pl.multiple_of(256 * g + 128 * i, 128), 128), :] = jnp.broadcast_to(
                v[0:1, 128 * i:128 * (i + 1)], (128, 128)).T

    def finish(us):
        cp.join(("n", us[0]["tag"]), RQN.at[0, 0:4 * us[0]["size"]])
        for u in us:
            rows = u["rows"]
            sc = SC[rows, :]
            v = Q0[rows, :] + RQN[0, rows, :].astype(f32) + RQN[1, rows, :].astype(f32)
            q_out[rows, :] = (v * jnp.concatenate([sc, sc], axis=1) + qb[...]).astype(bf)
        cp.join(("f", us[0]["tag"]), KP.at[0:3 * us[0]["size"] // 2])

    u0 = pair(y, 0, y, 128, 128)
    cp.join("sx", SS.at[0:3])
    SY[y] = SS[0] + SS[1] + SS[2] + SS[3]
    sy = [cp.remote(SY.at[y], SY.at[y], Y(s), "sy") for s in (1, 2, 3)]
    band = lambda o: pl.ds(o, 64)
    yo = {1: [cp.remote(A.at[y, band(o)], A.at[y, band(o)], Y(1), out="a") for o in (128, 192)],
          -1: [cp.remote(A.at[y, band(o)], A.at[y, band(o)], Y(-1), out="a") for o in (0, 64)]}
    scale(y)
    relay(u0)
    up, dn, op = yr, yl, md(y, 2)
    far = {}
    cp.join(("yc", 1), A.at[0, h[0]])
    far[1] = [cp.remote(A.at[dn, band(o)], A.at[dn, band(o)], Y(1), out="a") for o in (0, 64)]
    cp.join(("yc", -1), A.at[0, h[0]])
    far[-1] = [cp.remote(A.at[up, band(o)], A.at[up, band(o)], Y(-1), out="a") for o in (128, 192)]
    keys(u0)
    u1 = pair(dn, 0, up, 128, 128)
    finish(u0)
    relay(u1)
    yo[1][0].wait_recv()
    yo[-1][0].wait_recv()
    cp.join("sy", SY.at[0:3])
    for g in (dn, up, op):
        scale(g)
    u2 = pair(dn, 128, up, 0, 64)
    keys(u1)
    relay(u2)
    yo[1][1].wait_recv()
    yo[-1][1].wait_recv()
    u3 = pair(dn, 192, up, 64, 64)
    keys(u2)
    finish(u1)
    relay(u3)
    far[1][0].wait_recv()
    far[-1][0].wait_recv()
    u4 = pair(op, 0, op, 128, 64)
    keys(u3)
    finish(u2)
    far[1][1].wait_recv()
    far[-1][1].wait_recv()
    u5 = pair(op, 64, op, 192, 64)
    relay(u4)
    keys(u4)
    finish(u3)
    relay(u5)
    keys(u5)
    finish(u4)
    finish(u5)
    cp.drain({"w": W2.at[:, :, 0:1024], "g": W2.at[:, :, 0:1408], "z": wq.at[:, 0:1024, :], "h": H.at[0:2],
              "a": A.at[0:2], "o": RQO.at[0], "n": RQN, "k": KP.at[0:768], "f": KP.at[0:768], "ro": RO, "rn": RN})
    assert len(cp.groups) == N3 and len(cp.outs) == N4, len(cp.outs)


def whole(patches, ids, owner, slots, text, vnorm, qkv_w, qkv_b, out_w, mnorm, w1, b1, w2, b2, gain, qw, qb, kvw, kvb):
    bf, f32, i32 = jnp.bfloat16, jnp.float32, jnp.int32
    V, ANY = pl.BlockSpec(memory_space=pltpu.VMEM), pl.BlockSpec(memory_space=pl.ANY)
    S = jax.ShapeDtypeStruct
    M = pltpu.VMEM
    return pl.pallas_call(
        whole_kernel,
        out_shape=(S((1024, 256), bf), S((1024, 256), bf)),
        in_specs=[V, V, V, V, ANY, V, ANY, V, ANY, V, ANY, V, ANY, V, V, ANY, V, V, V],
        out_specs=[V] * 2,
        scratch_shapes=[
            M((4, 32, 1280), bf),
            M((4, 4, 4, 32, 1280), bf),
            M((1280, 1920), bf),
            M((640, 1280), bf),
            M((320, 5120), bf),
            M((4, 320, 512), bf),
            M((512, 1280), bf),
            M((4, 320, 2048), bf),
            M((4, 2048, 256), bf),
            M((4, 4, 16, 2048), bf),
            M((4, 16, 8192), bf),
            M((4, 4, 16, 256), bf),
            M((8, 128), f32),
            M((4, 4, 8, 128), f32),
            M((8, 128), i32),
            M((4, 8, 128), i32),
            M((2, 160, 256), bf),
            M((2, 128, 256), bf),
            M((4, 4, 128, 512), bf),
            M((4, 2, 64, 512), bf),
            M((4, 2, 128, 512), bf),
            M((4, 64, 2048), bf),
            M((2, 32, 2048), bf),
            M((4, 8, 32, 640), bf),
            M((4, 8, 32, 640), bf),
            M((4, 256, 2048), bf),
            M((4, 8, 256), f32),
            M((4, 8, 256), f32),
            M((1024, 128), f32),
            M((1024, 256), f32),
            M((1024, 256), bf),
            M((1024, 256), bf),
            M((1024, 256), bf),
            M((2, 1024, 256), bf),
            M((2, 1024, 256), bf),
            M((1024, 256), bf),
            M((4, 256, 256), bf),
            pltpu.SemaphoreType.DMA((N4,)),
            pltpu.SemaphoreType.DMA((N3,)),
            pltpu.SemaphoreType.DMA((16,)),
        ],
        compiler_params=pltpu.CompilerParams(collective_id=1, has_side_effects=True, vmem_limit_bytes=64000000),
        name="whole",
    )(patches, ids, owner, slots, text, vnorm, qkv_w, qkv_b, out_w, mnorm, w1, b1, w2, b2, gain, qw, qb, kvw, kvb)


def attention_kernel(q, kv, out):
    bf, f32 = jnp.bfloat16, jnp.float32
    c, d = lax.broadcasted_iota(jnp.int32, (256, 128), 0), lax.broadcasted_iota(jnp.int32, (256, 128), 1)
    spot = (d // 8) * 16 + d % 8
    keys = jnp.dot(kv[...], (c == spot).astype(f32).astype(bf), preferred_element_type=f32).astype(bf)
    values = jnp.dot(kv[...], (c == spot + 8).astype(f32).astype(bf), preferred_element_type=f32).astype(bf)
    low = lax.broadcasted_iota(jnp.int32, (256, 256), 0) >= lax.broadcasted_iota(jnp.int32, (256, 256), 1)
    k = HD ** (-0.5) * 1.4426950408889634
    for i in range(4):
        rows = slice(256 * i, 256 * (i + 1))
        for h in range(2):
            hs = slice(128 * h, 128 * (h + 1))
            s = lax.dot_general(q[rows, hs], keys[rows], NT, preferred_element_type=f32)
            s = jnp.where(low, s, -1e30)
            top = jnp.max(s, axis=1, keepdims=True)
            if i:
                before = lax.dot_general(q[rows, hs], keys[:256 * i], NT, preferred_element_type=f32)
                top = jnp.maximum(top, jnp.max(before, axis=1, keepdims=True))
            p = jnp.exp2((s - top) * k)
            total = jnp.sum(p, axis=1, keepdims=True)
            m = jnp.dot(p.astype(bf), values[rows], preferred_element_type=f32)
            if i:
                p = jnp.exp2((before - top) * k)
                total = total + jnp.sum(p, axis=1, keepdims=True)
                m = m + jnp.dot(p.astype(bf), values[:256 * i], preferred_element_type=f32)
            out[rows, hs] = (m / total).astype(bf)


def attention(q, kv):
    V = pl.BlockSpec(memory_space=pltpu.VMEM)
    return pl.pallas_call(
        attention_kernel,
        out_shape=jax.ShapeDtypeStruct((1024, 256), jnp.bfloat16),
        in_specs=[V, V],
        out_specs=V,
        compiler_params=pltpu.CompilerParams(vmem_limit_bytes=60000000),
        name="attention",
    )(q, kv)


def shards(
    patches,
    window_ids,
    owner,
    slot_of_row,
    text_embeds,
    vit_norm,
    vit_qkv_w,
    vit_qkv_b,
    vit_out_w,
    merge_norm,
    merge_w1,
    merge_b1,
    merge_w2,
    merge_b2,
    llm_norm,
    q_w,
    q_b,
    kv_w,
    kv_b,
):
    q, kv = whole(
        patches, window_ids, owner.reshape(1, 32), slot_of_row, text_embeds, vit_norm, vit_qkv_w,
        vit_qkv_b, vit_out_w, merge_norm, merge_w1.T, merge_b1, merge_w2, merge_b2[None],
        llm_norm[None], q_w, q_b[None], kv_w.transpose(0, 2, 1), kv_b,
    )
    return attention(q, kv)


def solution(mesh):
    return jax.shard_map(
        shards,
        mesh=mesh,
        in_specs=(
            P(("dp", "mp"), None),
            P(("dp", "mp"), None),
            P(("dp", "mp"), None),
            P(("dp", "mp"), None),
            P(("dp", "mp"), None),
            P(),
            P(),
            P(),
            P(),
            P(),
            P(None, "mp"),
            P("mp"),
            P("mp", None),
            P(),
            P(),
            P(None, "mp"),
            P("mp"),
            P(None, None, "mp"),
            P(None, "mp"),
        ),
        out_specs=P("dp", "mp"),
        check_vma=False,
    )
```

```python
import jax
import jax.numpy as jnp
from jax import lax
from jax.experimental import pallas as pl
from jax.experimental.pallas import tpu as pltpu
from jax.sharding import PartitionSpec as P

VHD = 80
HD = 128
MESH = pl.DeviceIdType.MESH
NT = (((1,), (1,)), ((), ()))


class Copies:
    def __init__(self, send, recv, local):
        self.send, self.recv, self.local = send, recv, local
        self.groups, self.outs, self.views, self.m, self.n = {}, {}, {}, 0, 0

    def remote(self, src, dst, dev, group=None, out=None):
        if group is None:
            self.n += 1
            group = self.n
        if out is None:
            out = group[0] if isinstance(group, tuple) and group[0] in ("o", "n", "k", "f", "ro", "rn") else group
        j = self.outs.setdefault(out, len(self.outs))
        k = self.groups.setdefault(group, len(self.groups))
        c = pltpu.make_async_remote_copy(
            src_ref=src, dst_ref=dst, send_sem=self.send.at[j], recv_sem=self.recv.at[k],
            device_id=dev, device_id_type=MESH)
        c.start()
        return c

    def join(self, group, view):
        k = self.groups[group]
        self.views[group] = view
        pltpu.make_async_copy(view, view, self.recv.at[k]).wait()

    def here(self, src, dst):
        k = self.m
        self.m += 1
        c = pltpu.make_async_copy(src, dst, self.local.at[k])
        c.start()
        return c

    def drain(self, views):
        for out, j in self.outs.items():
            view = views[out] if out in views else self.views[out]
            pltpu.make_async_copy(view, view, self.send.at[j]).wait()


def places():
    mp, dp = lax.axis_index("mp"), lax.axis_index("dp")
    y, x = mp // 4, lax.rem(mp, 4)
    X = lambda s: (dp, y * 4 + lax.rem(x + s + 4, 4))
    Y = lambda s: (dp, lax.rem(y + s + 4, 4) * 4 + x)
    Z = lambda s: (lax.rem(dp + 2 * s + 8, 8), mp)
    other = (dp + 1 - 2 * lax.rem(dp, 2), mp)
    return dp, y, x, X, Y, Z, other


def meet(devs):
    barrier = pltpu.get_barrier_semaphore()
    for d in devs:
        pl.semaphore_signal(barrier, inc=1, device_id=d, device_id_type=MESH)
    pl.semaphore_wait(barrier, len(devs))


N3 = 117
N4 = 32


def vision(patches, ids, norm, qkv_w, qkv_b, out_w, gain):
    bf, f32 = jnp.bfloat16, jnp.float32
    iota = lambda shape, d: lax.broadcasted_iota(jnp.int32, shape, d)
    i, s = iota((128, 128), 0), iota((128, 128), 1)
    perm = (s == (i % 32) * 4 + i // 32).astype(f32).astype(bf)
    p = jnp.dot(perm, patches[...], preferred_element_type=f32)
    wide = jnp.broadcast_to(ids[...].astype(f32), (128, 128)).astype(bf)
    across = lax.dot_general(wide, perm, NT, preferred_element_type=f32)
    same = across == across.T
    normed = p * lax.rsqrt(jnp.mean(p * p, axis=1, keepdims=True) + 1e-6) * norm[...].reshape(1, 1280)
    qkv = (jnp.dot(normed.astype(bf), qkv_w[...], preferred_element_type=f32) + qkv_b[...].reshape(1, 1920)).astype(bf)
    tiles = [None] * 5
    for h in range(8):
        lo, hi = 80 * h // 128, (80 * h + 207) // 128
        lane = iota((128, 128 * (hi - lo)), 1) + 128 * lo
        here = (lane >= 80 * h) & (lane < 80 * h + 80)
        part = lambda k: qkv[:, 640 * k + 128 * lo:640 * k + 128 * hi]
        zero = jnp.zeros((), bf)
        sc = lax.dot_general(jnp.where(here, part(0), zero), part(1), NT, preferred_element_type=f32) * VHD ** (-0.5)
        sc = jnp.where(same, sc, -1e30)
        e = jnp.exp(sc - jnp.max(sc, axis=1, keepdims=True))
        w = (e / jnp.sum(e, axis=1, keepdims=True)).astype(bf)
        mix = jnp.dot(w, jnp.where(here, part(2), zero), preferred_element_type=f32)
        for t in range(lo, hi):
            v = mix[:, 128 * (t - lo):128 * (t - lo + 1)]
            tiles[t] = v if tiles[t] is None else tiles[t] + v
    mixed = jnp.concatenate(tiles, axis=1).astype(bf)
    r = (p + jnp.dot(mixed, out_w[...], preferred_element_type=f32)).astype(bf).astype(f32)
    return (r * lax.rsqrt(jnp.mean(r * r, axis=1, keepdims=True) + 1e-6) * gain[...].reshape(1, 1280)).astype(bf)


def whole_kernel(patches, ids, owner, slots, text, vnorm, qkv_w, qkv_b, out_w, mnorm, w1, b1, w2, b2, gain, qw, qb,
                 kvw, kvb, q_out, kv_out,
                 MS, G, QKVW, OUTW, w1v, H, HT, W2, wq, wkv, KVS, KVX, KBS, kb, INS, info, RW, RQ,
                 PC, RO, RN, T, TR, SB, R, A, SS, SY, SC, Q0, QR, QL, QO, RQO, RQN, KP, RKV, send, recv, local):
    dp, y, x, X, Y, Z, other = places()
    md = lambda v, s: lax.rem(v + s + 4, 4)
    bf, f32 = jnp.bfloat16, jnp.float32
    iota = lambda shape, d: lax.broadcasted_iota(jnp.int32, shape, d)
    e, mp = dp, y * 4 + x
    cp = Copies(send, recv, local)
    lv = [cp.here(qkv_w, QKVW), cp.here(out_w, OUTW), cp.here(w1, w1v)]
    group = [(lax.rem(dp + s, 8), mp) for s in (2, 6, 1, 3, 5, 7, 4)]
    meet([X(1), X(2), X(3), Y(1), Y(2), Y(3)] + group)
    ca, cb = pl.ds(0, 768), pl.ds(768, 512)
    sa = lambda yy, xx: G.at[:, yy, xx, :, ca]
    sb = lambda yy, xx: G.at[:, yy, xx, :, cb]
    cols = lambda xd: pl.ds(pl.multiple_of(2048 * xd + 256 * e, 256), 256)
    mine = pl.ds(pl.multiple_of(256 * e, 256), 256)
    first, second = pl.ds(0, 2), pl.ds(2, 2)

    xo = md(x, 2)
    w2_half = [pl.ds(0, 160), pl.ds(160, 160)]
    q_half = lambda v, i: pl.ds(pl.multiple_of(2048 * v + 256 * e + 128 * i, 128), 128)
    bands = lambda r: pl.ds(pl.multiple_of(256 * r, 256), 256)
    zw, zwf, dw = {}, {}, []

    def w2_start(s):
        xs = md(x, s)
        src = w2.at[:, cols(x)] if s == 0 else W2.at[xs, :, mine]
        zw[s] = {t: cp.remote(src, W2.at[xs, :, mine], Z(t), out="w") for t in (1, -1)}
        dw.append(cp.remote(src, W2.at[xs, :, mine], other, "dw"))

    def w2_mid(s):
        xs, way = md(x, s), 1 if s in (0, 1) else -1
        for t in (1, -1):
            zw[s][t].wait_recv()
            at = W2.at[xs, :, bands(lax.rem(e - 2 * t + 8, 8))]
            if t == way:
                zwf[s] = cp.remote(at, at, Z(t), out="w")
            dw.append(cp.remote(at, at, other, "dw"))

    def w2_end(s):
        zwf[s].wait_recv()
        at = W2.at[md(x, s), :, bands(lax.rem(e + 4, 8))]
        dw.append(cp.remote(at, at, other, "dw"))

    w2r = [cp.remote(w2.at[w2_half[i], cols(xo)], RW.at[i], X(1 - 2 * i), out="w") for i in range(2)]
    w2d = [cp.remote(w2.at[:, cols(md(x, s))], W2.at[x, :, mine], X(s), out="w") for s in (1, -1)]
    w2_start(0)
    wl = [cp.here(w2.at[:, cols(x)], W2.at[x, :, mine]), cp.here(qw.at[cols(x), :], wq.at[x, mine, :])]

    lv[0].wait()
    lv[1].wait()
    MS[...] = vision(patches, ids, vnorm, QKVW, qkv_b, OUTW, mnorm).reshape(4, 32, 1280)

    ma, mb = MS.at[:, :, ca], MS.at[:, :, cb]
    a1 = {s: cp.remote(ma, sa(y, x), X(s), out="g") for s in (1, -1)}
    c1 = {s: cp.remote(mb, sb(y, x), Y(s), out="g") for s in (1, -1)}
    a2 = {(0, s): cp.remote(ma, sa(y, x), Y(s), out="g") for s in (1, -1)}
    c2 = {(0, s): cp.remote(mb, sb(y, x), X(s), out="g") for s in (1, -1)}
    gl = cp.here(MS, G.at[:, y, x])
    i64, s64 = iota((64, 64), 0), iota((64, 64), 1)
    order = (s64 == (i64 // 8 % 2) * 32 + (i64 % 8) * 4 + i64 // 16).astype(f32).astype(bf)
    for n in range(4):
        cs = slice(2048 * n, 2048 * (n + 1))
        v = jnp.dot(order, kvw[:, :, cs].reshape(64, 2048), preferred_element_type=f32)
        KVS[:, :, cs] = v.astype(bf).reshape(4, 16, 2048)
    li, ll = iota((128, 128), 0), iota((128, 128), 1)
    rows = []
    flat = jnp.concatenate([kvb[0:1, :], kvb[1:2, :], jnp.zeros((1, 64), f32)], axis=1)
    down = jnp.broadcast_to(flat, (128, 128)).T
    for j in range(4):
        keep = (li == (ll // 8) * 32 + (ll % 8) * 4 + j) & (ll < 16)
        rows.append(jnp.sum(jnp.where(keep, down, 0.0), axis=0, keepdims=True))
    KBS[...] = jnp.concatenate(rows + [jnp.zeros((4, 128), f32)], axis=0)
    own4 = jnp.broadcast_to(jnp.concatenate([owner[...]] * 4, axis=1), (8, 128))
    slot2 = jnp.broadcast_to(jnp.concatenate([slots[...]] * 2, axis=1), (8, 128))
    t0, t1 = iota((8, 128), 0), iota((8, 128), 1)
    INS[...] = jnp.where((t0 == 0) & (t1 // 32 == x), own4,
                         jnp.where((t0 == 1 + x // 2) & (t1 // 64 == x % 2), slot2, 0))
    KVX[x] = KVS[:, :, cols(x)]
    kb[y, x] = KBS[...]
    info[x] = INS[...]

    af, cf = {}, {}
    for s in (1, -1):
        hf = first if s == 1 else second
        a1[s].wait_recv()
        xs = md(x, -s)
        at = G.at[hf, y, xs, :, ca]
        af[s] = cp.remote(at, at, X(s), out="g")
        for t in (1, -1):
            a2[(-s, t)] = cp.remote(sa(y, xs), sa(y, xs), Y(t), out="g")
        c1[s].wait_recv()
        ys = md(y, -s)
        at = G.at[hf, ys, x, :, cb]
        cf[s] = cp.remote(at, at, Y(s), out="g")
        for t in (1, -1):
            c2[(-s, t)] = cp.remote(sb(ys, x), sb(ys, x), X(t), out="g")
    last = []

    def pass_on(p):
        for t in (1, -1):
            hf = first if t == 1 else second
            a2[(p, t)].wait_recv()
            at = G.at[hf, md(y, -t), md(x, p), :, ca]
            last.append(cp.remote(at, at, Y(t), "last"))
            c2[(p, t)].wait_recv()
            at = G.at[hf, md(y, p), md(x, -t), :, cb]
            last.append(cp.remote(at, at, X(t), "last"))

    qr = [cp.remote(qw.at[q_half(xo, i), :], RQ.at[i], X(1 - 2 * i), out="z") for i in range(2)]
    qd = [cp.remote(qw.at[cols(md(x, s)), :], wq.at[x, mine, :], X(s), "qd") for s in (1, -1)]
    wx = []
    for t in (1, 3, 2):
        wx.append(cp.remote(KVS.at[:, :, cols(md(x, t))], KVX.at[x], X(t), "wx0"))
        wx.append(cp.remote(KBS, kb.at[y, x], X(t), "wx1"))
        wx.append(cp.remote(INS, info.at[x], X(t), "wx2"))
    for c in w2r:
        c.wait_recv()
    w2f = [cp.remote(RW.at[i], W2.at[md(x, 2 * i - 1), w2_half[i], mine], X(1 - 2 * i), out="w") for i in range(2)]
    w2_mid(0)
    w2d[0].wait_recv()
    w2_start(-1)
    w2d[1].wait_recv()
    w2_start(1)
    pass_on(0)

    def piece(name, r, half=None):
        h = pl.ds(0, 4) if half is None else (first, second)[half]
        if name == "q":
            return wq.at[h, bands(r), :]
        return wkv.at[h, :, :, bands(r)]

    zs, ds_, zf = {}, {}, {}

    def z_start(name):
        zs[name] = {s: cp.remote(piece(name, e), piece(name, e), Z(s), out="z") for s in (1, -1)}
        ds_[name] = [cp.remote(piece(name, e), piece(name, e), other, "d" + name)]

    def z_mid(name):
        zf[name] = {}
        for s in (1, -1):
            zs[name][s].wait_recv()
            r, h = lax.rem(e - 2 * s + 8, 8), 0 if s == 1 else 1
            zf[name][s] = cp.remote(piece(name, r, h), piece(name, r, h), Z(s), out="z")
            ds_[name].append(cp.remote(piece(name, r), piece(name, r), other, "d" + name))

    def z_end(name):
        for s in (1, -1):
            zf[name][s].wait_recv()
        r = lax.rem(e + 4, 8)
        ds_[name].append(cp.remote(piece(name, r), piece(name, r), other, "d" + name))

    def z_all(name):
        cp.join("d" + name, wq.at[:, 0:1024, :] if name == "q" else wkv.at[:, :, :, 0:1024])

    for s in (1, -1):
        af[s].wait_recv()
        cf[s].wait_recv()
    xf, yf = md(x, 2), md(y, 2)
    for t in (1, -1):
        a2[(2, t)] = cp.remote(sa(y, xf), sa(y, xf), Y(t), out="g")
        c2[(2, t)] = cp.remote(sb(yf, x), sb(yf, x), X(t), out="g")
    pass_on(-1)
    pass_on(1)
    for c in qr:
        c.wait_recv()
    qf = [cp.remote(RQ.at[i], wq.at[md(x, 2 * i - 1), pl.ds(pl.multiple_of(256 * e + 128 * i, 128), 128), :],
                    X(1 - 2 * i), "qd") for i in range(2)]
    w2_mid(-1)
    w2_mid(1)
    pass_on(2)
    for c in w2f:
        c.wait_recv()
    w2_start(2)
    cp.join("last", G.at[:, 0])
    gl.wait()
    lv[2].wait()
    wide = jnp.concatenate([b1[...].reshape(1, 320), jnp.zeros((1, 64), f32)], axis=1)
    bcol = jnp.broadcast_to(wide, (128, 384)).T[0:320, :]
    bcol = jnp.concatenate([bcol, bcol], axis=1)
    h1 = {}
    for g in range(2):
        acc = None
        for j in range(4):
            p = lax.dot_general(w1v[:, 1280 * j:1280 * (j + 1)], G[j, 2 * g:2 * g + 2].reshape(256, 1280), NT,
                                preferred_element_type=f32)
            acc = p if acc is None else acc + p
        v = acc + bcol
        v = 0.5 * v * (1.0 + lax.erf(v * (0.5 ** 0.5)))
        H[x, :, 256 * g:256 * (g + 1)] = v.astype(bf)
        hc = pl.ds(256 * g, 256)
        for s in (1, -1):
            h1[(g, s)] = cp.remote(H.at[x, :, hc], H.at[x, :, hc], X(s), out="h")
    h2 = []

    def pass_hidden(g):
        for s in (1, -1):
            h1[(g, s)].wait_recv()
            at = H.at[md(x, -s), pl.ds(0, 160) if s == 1 else pl.ds(160, 160), pl.ds(256 * g, 256)]
            h2.append(cp.remote(at, at, X(s), "h2"))

    w2_mid(2)
    cp.join("wx0", KVX.at[0:3])
    cp.join("wx1", kb.at[0, 0:3])
    cp.join("wx2", info.at[0:3])
    ky = []
    for s in (1, 2, 3):
        yd = md(y, s)
        ky.append(cp.remote(KVX.at[:, yd], wkv.at[y, :, :, mine], Y(s), "ky0"))
        ky.append(cp.remote(kb.at[y], kb.at[y], Y(s), "ky1"))
    wkv[y, :, :, mine] = KVX[:, y]
    cp.join("qd", wq.at[0, 0:768, :])
    wl[1].wait()
    z_start("q")
    pass_hidden(0)
    for s in (0, -1, 1, 2):
        w2_end(s)
    pass_hidden(1)
    quarter = lambda v: pl.ds(pl.multiple_of(2048 * v, 2048), 2048)
    th = [pl.ds(0, 32), pl.ds(32, 32)]
    tr = [cp.remote(text.at[th[i], quarter(xo)], TR.at[i], X(1 - 2 * i), "tr") for i in range(2)]
    td = [cp.remote(text.at[:, quarter(md(x, s))], T.at[x], X(s), "td") for s in (1, -1)]
    tl = cp.here(text.at[:, quarter(x)], T.at[x])
    tab = info[0] + info[1] + info[2] + info[3]
    own = tab[0:1, :]
    down = jnp.broadcast_to(own.astype(f32), (128, 128)).T.astype(jnp.int32)
    before = (down == own) & (li < ll) & (li // 32 == ll // 32)
    rank = jnp.sum(before.astype(jnp.int32), axis=0, keepdims=True)
    target = own * 32 + (iota((1, 128), 1) // 32) * 8 + rank
    pick = (iota((256, 128), 0) == target).astype(f32).astype(bf)
    choose = []
    for i in range(2):
        s = jnp.broadcast_to(tab[1 + i:2 + i, :].astype(f32), (128, 128)).T.astype(jnp.int32)
        s = jnp.concatenate([s, s], axis=1)
        lane, row = iota((128, 256), 1), iota((128, 256), 0)
        hit = ((lane // 32) * 8 + lane % 8 == s) & ((lane % 32) // 8 == row // 64 + 2 * i)
        choose.append(hit.astype(f32).astype(bf))
    cp.join("ky0", KVX.at[0:3])
    cp.join("ky1", kb.at[0:3])
    z_start("kv")
    wl[0].wait()
    cp.join("dw", W2.at[:, :, 0:1024])
    cp.join("h2", H.at[0])
    HT[...] = H[...].reshape(1280, 512).T

    lo, hi = pl.ds(0, 64), pl.ds(64, 64)
    yr, yl = md(y, 1), md(y, -1)
    ro, rn, hand, handl = {}, {}, {}, {}

    def mul(c):
        cs = slice(512 * c, 512 * (c + 1))
        v = jnp.dot(HT[...], W2[:, :, cs].reshape(1280, 512), preferred_element_type=f32)
        PC[c] = v.astype(bf).reshape(4, 128, 512)
        ro[c] = [cp.remote(PC.at[c, md(y, 2), lo], RO.at[c, 0], Y(1), ("ro", c)),
                 cp.remote(PC.at[c, md(y, 2), hi], RO.at[c, 1], Y(-1), ("ro", c))]
        rn[c] = [cp.remote(PC.at[c, yr, hi], RN.at[c, 0, hi], Y(1), ("rn", c)),
                 cp.remote(PC.at[c, yl, lo], RN.at[c, 1, lo], Y(-1), ("rn", c))]

    def relay_y(c):
        cp.join(("ro", c), RO.at[c])
        PC[c, yr, 0:64, :] = (PC[c, yr, 0:64, :].astype(f32) + RO[c, 0].astype(f32)).astype(bf)
        rn[c].append(cp.remote(PC.at[c, yr, lo], RN.at[c, 0, lo], Y(1), ("rn", c)))
        PC[c, yl, 64:128, :] = (PC[c, yl, 64:128, :].astype(f32) + RO[c, 1].astype(f32)).astype(bf)
        rn[c].append(cp.remote(PC.at[c, yl, hi], RN.at[c, 1, hi], Y(-1), ("rn", c)))

    def give(c):
        cp.join(("rn", c), RN.at[c])
        v = PC[c, y].astype(f32) + RN[c, 0].astype(f32) + RN[c, 1].astype(f32)
        v = (v + b2[:, pl.ds(pl.multiple_of(2048 * x + 512 * c, 512), 512)]).astype(bf)
        SB[c, :, :, 0:512] = jnp.dot(pick, v, preferred_element_type=f32).astype(bf).reshape(8, 32, 512)
        w = pl.ds(0, 512)
        if c == 0:
            v = jnp.dot(pick, jnp.ones((128, 128), bf), preferred_element_type=f32)
            SB[c, :, :, 512:640] = v.astype(bf).reshape(8, 32, 128)
            w = pl.ds(0, 640)
        hand[c] = [cp.remote(SB.at[c, d[0], :, w], R.at[c, dp, :, w], d, ("hand", c)) for d in group]
        handl[c] = cp.here(SB.at[c, dp, :, w], R.at[c, dp, :, w])

    h = [pl.ds(0, 128), pl.ds(128, 128)]
    gx = gain[:, quarter(x)]
    filled, sq, yc = [None, None], [None, None], {1: [], -1: []}

    def take(c):
        cs = slice(512 * c, 512 * (c + 1))
        cp.join(("hand", c), R.at[c, 0:7, :, pl.ds(0, 640 if c == 0 else 512)])
        handl[c].wait()
        for i in range(2):
            if c == 0:
                seen = jnp.dot(choose[i], R[0, :, :, 512:640].reshape(256, 128), preferred_element_type=f32)
                filled[i] = seen[:, 0:1] > 0.5
            v = jnp.dot(choose[i], R[c, :, :, 0:512].reshape(256, 512), preferred_element_type=f32)
            v = jnp.where(filled[i], v, T[2 * i:2 * i + 2, :, cs].reshape(128, 512).astype(f32))
            t = jnp.sum(v * v, axis=1, keepdims=True)
            sq[i] = t if c == 0 else sq[i] + t
            A[y, 128 * i:128 * (i + 1), cs] = (v * gx[:, cs]).astype(bf)
            w, s = pl.ds(512 * c, 512), 1 - 2 * i
            yc[s].append(cp.remote(A.at[y, h[i], w], A.at[y, h[i], w], Y(s), ("yc", s)))

    mul(0)
    mul(1)
    relay_y(0)
    mul(2)
    relay_y(1)
    mul(3)
    z_mid("q")
    give(0)
    cp.join("tr", TR)
    tf = [cp.remote(TR.at[i], T.at[md(x, 2 * i - 1), th[i]], X(1 - 2 * i), "td") for i in range(2)]
    relay_y(2)
    z_mid("kv")
    give(1)
    relay_y(3)
    give(2)
    cp.join("td", T.at[0:3])
    tl.wait()
    give(3)
    take(0)
    take(1)
    z_end("q")
    take(2)
    z_end("kv")
    take(3)
    SS[x] = jnp.concatenate([jnp.broadcast_to(t, (128, 128)).T[0:8, :] for t in sq], axis=1)
    sx = [cp.remote(SS.at[x], SS.at[x], X(s), "sx") for s in (1, 2, 3)]
    z_all("q")
    z_all("kv")

    tag = [0]

    def pair(ga, oa, gb, ob, size):
        tag[0] += 1
        a = jnp.concatenate([A[ga, oa:oa + size, :], A[gb, ob:ob + size, :]], axis=0)
        us = []
        for g, o in ((ga, oa), (gb, ob)):
            at = lambda off, n, g=g, o=o: pl.ds(pl.multiple_of(256 * g + o + off, n), n)
            us.append(dict(tag=tag[0], size=size, rows=at(0, size), lo=at(0, size // 2), hi=at(size // 2, size // 2),
                           share=lambda v, g=g, o=o: pl.ds(
                               pl.multiple_of(256 * g + o + size // 4 * v, size // 4), size // 4),
                           slot=pl.ds(pl.multiple_of(64 * g + o // 4, size // 4), size // 4)))
        prod = lambda s: jnp.dot(a, wq[md(x, s)], preferred_element_type=f32)

        def put(ref, v):
            v = v.astype(ref.dtype)
            for n, u in enumerate(us):
                ref[u["rows"], :] = v[size * n:size * (n + 1)]

        put(QO, prod(2))
        for u in us:
            u["o"] = [cp.remote(QO.at[u["lo"]], RQO.at[0, u["lo"]], X(1), ("o", u["tag"])),
                      cp.remote(QO.at[u["hi"]], RQO.at[1, u["hi"]], X(-1), ("o", u["tag"]))]
        put(KP, lax.dot_general(a, wkv[...].reshape(256, 2048), NT, preferred_element_type=f32))
        for u in us:
            u["k"] = []
            for s in (2, 1, 3):
                u["k"].append(cp.remote(KP.at[u["share"](md(x, s))], RKV.at[x, u["slot"]], X(s), ("k", u["tag"])))
        put(QR, prod(1))
        for u in us:
            u["n"] = [cp.remote(QR.at[u["hi"]], RQN.at[0, u["hi"]], X(1), ("n", u["tag"]))]
        put(QL, prod(-1))
        for u in us:
            u["n"].append(cp.remote(QL.at[u["lo"]], RQN.at[1, u["lo"]], X(-1), ("n", u["tag"])))
        put(Q0, prod(0))
        return us

    def relay(us):
        cp.join(("o", us[0]["tag"]), RQO.at[0, 0:2 * us[0]["size"]])
        for u in us:
            lo, hi = u["lo"], u["hi"]
            QR[lo, :] = (QR[lo, :].astype(f32) + RQO[0, lo, :].astype(f32)).astype(bf)
            u["n"].append(cp.remote(QR.at[lo], RQN.at[0, lo], X(1), ("n", u["tag"])))
            QL[hi, :] = (QL[hi, :].astype(f32) + RQO[1, hi, :].astype(f32)).astype(bf)
            u["n"].append(cp.remote(QL.at[hi], RQN.at[1, hi], X(-1), ("n", u["tag"])))

    bias = jnp.concatenate([kb[p // 4, p % 4, pl.ds(y, 1), 0:16] for p in range(16)], axis=1)

    def keys(us):
        cp.join(("k", us[0]["tag"]), KP.at[0:3 * us[0]["size"] // 2])
        for u in us:
            m = u["share"](x)
            v = KP[m, :].astype(f32)
            for s in (1, 2, 3):
                v = v + RKV[md(x, s), u["slot"]].astype(f32)
            sc = SC[m, :]
            v = v * jnp.concatenate([sc, sc], axis=1) + bias
            kv_out[m, :] = v.astype(bf)
            u["f"] = [cp.remote(kv_out.at[m], kv_out.at[m], X(s), ("f", u["tag"])) for s in (2, 1, 3)]

    def scale(g):
        v = lax.rsqrt(SY[g] * (1.0 / 8192.0) + 1e-6)
        for i in range(2):
            SC[pl.ds(pl.multiple_of(256 * g + 128 * i, 128), 128), :] = jnp.broadcast_to(
                v[0:1, 128 * i:128 * (i + 1)], (128, 128)).T

    def finish(us):
        cp.join(("n", us[0]["tag"]), RQN.at[0, 0:4 * us[0]["size"]])
        for u in us:
            rows = u["rows"]
            sc = SC[rows, :]
            v = Q0[rows, :] + RQN[0, rows, :].astype(f32) + RQN[1, rows, :].astype(f32)
            q_out[rows, :] = (v * jnp.concatenate([sc, sc], axis=1) + qb[...]).astype(bf)
        cp.join(("f", us[0]["tag"]), KP.at[0:3 * us[0]["size"] // 2])

    u0 = pair(y, 0, y, 128, 128)
    cp.join("sx", SS.at[0:3])
    SY[y] = SS[0] + SS[1] + SS[2] + SS[3]
    sy = [cp.remote(SY.at[y], SY.at[y], Y(s), "sy") for s in (1, 2, 3)]
    band = lambda o: pl.ds(o, 64)
    yo = {1: [cp.remote(A.at[y, band(o)], A.at[y, band(o)], Y(1), out="a") for o in (128, 192)],
          -1: [cp.remote(A.at[y, band(o)], A.at[y, band(o)], Y(-1), out="a") for o in (0, 64)]}
    scale(y)
    relay(u0)
    up, dn, op = yr, yl, md(y, 2)
    far = {}
    cp.join(("yc", 1), A.at[0, h[0]])
    far[1] = [cp.remote(A.at[dn, band(o)], A.at[dn, band(o)], Y(1), out="a") for o in (0, 64)]
    cp.join(("yc", -1), A.at[0, h[0]])
    far[-1] = [cp.remote(A.at[up, band(o)], A.at[up, band(o)], Y(-1), out="a") for o in (128, 192)]
    keys(u0)
    u1 = pair(dn, 0, up, 128, 128)
    finish(u0)
    relay(u1)
    yo[1][0].wait_recv()
    yo[-1][0].wait_recv()
    cp.join("sy", SY.at[0:3])
    for g in (dn, up, op):
        scale(g)
    u2 = pair(dn, 128, up, 0, 64)
    keys(u1)
    relay(u2)
    yo[1][1].wait_recv()
    yo[-1][1].wait_recv()
    u3 = pair(dn, 192, up, 64, 64)
    keys(u2)
    finish(u1)
    relay(u3)
    far[1][0].wait_recv()
    far[-1][0].wait_recv()
    u4 = pair(op, 0, op, 128, 64)
    keys(u3)
    finish(u2)
    far[1][1].wait_recv()
    far[-1][1].wait_recv()
    u5 = pair(op, 64, op, 192, 64)
    relay(u4)
    keys(u4)
    finish(u3)
    relay(u5)
    keys(u5)
    finish(u4)
    finish(u5)
    cp.drain({"w": W2.at[:, :, 0:1024], "g": W2.at[:, :, 0:1408], "z": wq.at[:, 0:1024, :], "h": H.at[0:2],
              "a": A.at[0:2], "o": RQO.at[0], "n": RQN, "k": KP.at[0:768], "f": KP.at[0:768], "ro": RO, "rn": RN})
    assert len(cp.groups) == N3 and len(cp.outs) == N4, len(cp.outs)


def whole(patches, ids, owner, slots, text, vnorm, qkv_w, qkv_b, out_w, mnorm, w1, b1, w2, b2, gain, qw, qb, kvw, kvb):
    bf, f32, i32 = jnp.bfloat16, jnp.float32, jnp.int32
    V, ANY = pl.BlockSpec(memory_space=pltpu.VMEM), pl.BlockSpec(memory_space=pl.ANY)
    S = jax.ShapeDtypeStruct
    M = pltpu.VMEM
    return pl.pallas_call(
        whole_kernel,
        out_shape=(S((1024, 256), bf), S((1024, 256), bf)),
        in_specs=[V, V, V, V, ANY, V, ANY, V, ANY, V, ANY, V, ANY, V, V, ANY, V, V, V],
        out_specs=[V] * 2,
        scratch_shapes=[
            M((4, 32, 1280), bf),
            M((4, 4, 4, 32, 1280), bf),
            M((1280, 1920), bf),
            M((640, 1280), bf),
            M((320, 5120), bf),
            M((4, 320, 512), bf),
            M((512, 1280), bf),
            M((4, 320, 2048), bf),
            M((4, 2048, 256), bf),
            M((4, 4, 16, 2048), bf),
            M((4, 16, 8192), bf),
            M((4, 4, 16, 256), bf),
            M((8, 128), f32),
            M((4, 4, 8, 128), f32),
            M((8, 128), i32),
            M((4, 8, 128), i32),
            M((2, 160, 256), bf),
            M((2, 128, 256), bf),
            M((4, 4, 128, 512), bf),
            M((4, 2, 64, 512), bf),
            M((4, 2, 128, 512), bf),
            M((4, 64, 2048), bf),
            M((2, 32, 2048), bf),
            M((4, 8, 32, 640), bf),
            M((4, 8, 32, 640), bf),
            M((4, 256, 2048), bf),
            M((4, 8, 256), f32),
            M((4, 8, 256), f32),
            M((1024, 128), f32),
            M((1024, 256), f32),
            M((1024, 256), bf),
            M((1024, 256), bf),
            M((1024, 256), bf),
            M((2, 1024, 256), bf),
            M((2, 1024, 256), bf),
            M((1024, 256), bf),
            M((4, 256, 256), bf),
            pltpu.SemaphoreType.DMA((N4,)),
            pltpu.SemaphoreType.DMA((N3,)),
            pltpu.SemaphoreType.DMA((16,)),
        ],
        compiler_params=pltpu.CompilerParams(collective_id=1, has_side_effects=True, vmem_limit_bytes=64000000),
        name="whole",
    )(patches, ids, owner, slots, text, vnorm, qkv_w, qkv_b, out_w, mnorm, w1, b1, w2, b2, gain, qw, qb, kvw, kvb)


def attention_kernel(q, kv, out):
    bf, f32 = jnp.bfloat16, jnp.float32
    c, d = lax.broadcasted_iota(jnp.int32, (256, 128), 0), lax.broadcasted_iota(jnp.int32, (256, 128), 1)
    spot = (d // 8) * 16 + d % 8
    keys = jnp.dot(kv[...], (c == spot).astype(f32).astype(bf), preferred_element_type=f32).astype(bf)
    values = jnp.dot(kv[...], (c == spot + 8).astype(f32).astype(bf), preferred_element_type=f32).astype(bf)
    low = lax.broadcasted_iota(jnp.int32, (256, 256), 0) >= lax.broadcasted_iota(jnp.int32, (256, 256), 1)
    k = HD ** (-0.5) * 1.4426950408889634
    for i in range(4):
        rows = slice(256 * i, 256 * (i + 1))
        for h in range(2):
            hs = slice(128 * h, 128 * (h + 1))
            s = lax.dot_general(q[rows, hs], keys[rows], NT, preferred_element_type=f32)
            s = jnp.where(low, s, -1e30)
            top = jnp.max(s, axis=1, keepdims=True)
            if i:
                before = lax.dot_general(q[rows, hs], keys[:256 * i], NT, preferred_element_type=f32)
                top = jnp.maximum(top, jnp.max(before, axis=1, keepdims=True))
            p = jnp.exp2((s - top) * k)
            total = jnp.sum(p, axis=1, keepdims=True)
            m = jnp.dot(p.astype(bf), values[rows], preferred_element_type=f32)
            if i:
                p = jnp.exp2((before - top) * k)
                total = total + jnp.sum(p, axis=1, keepdims=True)
                m = m + jnp.dot(p.astype(bf), values[:256 * i], preferred_element_type=f32)
            out[rows, hs] = (m / total).astype(bf)


def attention(q, kv):
    V = pl.BlockSpec(memory_space=pltpu.VMEM)
    return pl.pallas_call(
        attention_kernel,
        out_shape=jax.ShapeDtypeStruct((1024, 256), jnp.bfloat16),
        in_specs=[V, V],
        out_specs=V,
        compiler_params=pltpu.CompilerParams(vmem_limit_bytes=60000000),
        name="attention",
    )(q, kv)


def shards(
    patches,
    window_ids,
    owner,
    slot_of_row,
    text_embeds,
    vit_norm,
    vit_qkv_w,
    vit_qkv_b,
    vit_out_w,
    merge_norm,
    merge_w1,
    merge_b1,
    merge_w2,
    merge_b2,
    llm_norm,
    q_w,
    q_b,
    kv_w,
    kv_b,
):
    q, kv = whole(
        patches, window_ids, owner.reshape(1, 32), slot_of_row, text_embeds, vit_norm, vit_qkv_w,
        vit_qkv_b, vit_out_w, merge_norm, merge_w1.T, merge_b1, merge_w2, merge_b2[None],
        llm_norm[None], q_w, q_b[None], kv_w.transpose(0, 2, 1), kv_b,
    )
    return attention(q, kv)


def solution(mesh):
    return jax.shard_map(
        shards,
        mesh=mesh,
        in_specs=(
            P(("dp", "mp"), None),
            P(("dp", "mp"), None),
            P(("dp", "mp"), None),
            P(("dp", "mp"), None),
            P(("dp", "mp"), None),
            P(),
            P(),
            P(),
            P(),
            P(),
            P(None, "mp"),
            P("mp"),
            P("mp", None),
            P(),
            P(),
            P(None, "mp"),
            P("mp"),
            P(None, None, "mp"),
            P(None, "mp"),
        ),
        out_specs=P("dp", "mp"),
        check_vma=False,
    )
```
